128 devices in a mesh: row: 16 (over z_hi, y, core), col: 8 (over x, z_lo).
Axes of the slice: x: 4, y: 4, z: 4 (z_hi: 2, z_lo: 2; z = z_hi * 2 + z_lo), core: 2. Of those that a mesh axis runs over, the one named last changes fastest.
Arguments:
- tokens: bfloat16 [16384, 2048], P(('row', 'col')), may hold values from -30 to 30
- ln1_gain: float32 [2048], replicated, may hold values from 0.25 to 1.75
- qkv_weight: bfloat16 [2048, 16, 3, 128], P('row', 'col'), may hold values from -4 to 4
- out_weight: bfloat16 [2048, 2048], P('col', 'row'), may hold values from -0.125 to 0.125
- ln2_gain: float32 [2048], replicated, may hold values from 0.25 to 1.75
- ffn_in: bfloat16 [2048, 8192], P('row', 'col'), may hold values from -0.125 to 0.125
- ffn_out: bfloat16 [8192, 2048], P('col', 'row'), may hold values from -0.0625 to 0.0625
- expert_ids: int32 [16384, 1], P(('row', 'col')), may hold values from 0 to 63; in each aligned block of 128 rows (0 to 127, 128 to 255, ...) at most 4 rows name the same one
- expert_in: bfloat16 [128, 2048, 2048], P(('row', 'col')), may hold values from -0.125 to 0.125
- expert_out: bfloat16 [128, 2048, 2048], P(('row', 'col')), may hold values from -0.09375 to 0.09375
Outputs:
- block_out: bfloat16 [16384, 2048], P(('row', 'col'))
The draws below stay inside these ranges and needn't reach their ends.
Inputs may be any that keep to these rules, and one draw needn't show every extreme that they name: `expert_ids`: among the tokens of one device no expert is named more than 4 times, and in every draw some expert is named exactly 4 times by the tokens of some device.
All inputs are finite; a program needn't handle non-finite values.
Results may differ from the reference program's by a relative error of at most 0.013.
Values may be sent and summed in bfloat16 or wider, within the bound.
A program may use at most 128 MiB of HBM per device.

```python
import math
import jax
import jax.numpy as jnp
import numpy as np
from jax import lax

D = 2048
HEADS = 16
DH = 128
FF = 8192
FFE = 4096
TOK_DEV = 128
SEQ = 1024
TOKENS = 16384
EXPERTS = 64
CAP = 4
FF_BLOCK = 1024
HALF = 2048
N_ROW = 16
N_COL = 8


def draw_tokens(key, part):
    first_key = jax.random.fold_in(jax.random.fold_in(key, 11), 0)
    base_values = jax.random.normal(first_key, (TOKENS, D), jnp.float32)
    return jnp.clip(base_values, -30.0, 30.0).astype(jnp.bfloat16)


def draw_qkv_weight(key, part):
    first_key = jax.random.fold_in(jax.random.fold_in(key, 23), 0)
    base_values = jax.random.normal(first_key, (D, HEADS, 3, DH), jnp.float32) * D ** (-0.5)
    factors = jnp.array([2.0, 1.0, 1.0], jnp.float32)[None, None, :, None]
    base_values = base_values * factors
    return jnp.clip(base_values, -4.0, 4.0).astype(jnp.bfloat16)


def block_scale(key, dims, shards, low, high):
    gain, own = 1.0, jax.random.fold_in(key, 6)
    for dim, blocks in shards:
        draws = jnp.exp(jax.random.uniform(jax.random.fold_in(own, dim), (blocks,), jnp.float32, low / len(shards), high / len(shards)))
        gain = gain * jnp.repeat(draws, dims[dim] // blocks).reshape([-1 if axis == dim else 1 for axis in range(len(dims))])
    return gain


def assign_block(key, own, number, rows, count, top, reach, slope):
    ranking = jax.random.permutation(key, count)
    crowded, common = portions_of(count, rows * top, reach, slope, True), portions_of(count, rows * top, reach, slope, False)
    places = jnp.arange(count)

    def named(lengths, offset_by):
        used = int((lengths > 0).sum())
        fixed = max(1, used // 4)
        passed = fixed + (places - fixed + offset_by * (used - fixed)) % max(1, count - fixed)
        return jnp.zeros((count,), jnp.int32).at[ranking[jnp.where(places < fixed, places, passed)]].set(jnp.asarray(lengths, jnp.int32))

    lengths = jnp.where(number % 4 == 0, named(crowded, number // 4), named(common, number - number // 4 - 1))
    mixed = jax.random.permutation(jax.random.fold_in(own, 3), count)
    giver, receiver = mixed[0:count // 2 * 2:2], mixed[1:count // 2 * 2:2]
    margin = jnp.minimum(lengths[giver] - 1, reach - lengths[receiver]) // 2
    margin = jnp.where((giver == ranking[0]) | (receiver == ranking[0]) | (lengths[receiver] == 0), 0, jnp.maximum(margin, 0))
    passed = jax.random.randint(jax.random.fold_in(own, 4), (count // 2,), 0, 1 << 20) % (margin + 1)
    lengths = lengths.at[giver].add(-passed).at[receiver].add(passed)
    members = jnp.searchsorted(jnp.cumsum(lengths), jnp.arange(rows * top), side="right").astype(jnp.int32)
    grid = members.reshape(top, rows).T
    grid = grid[jax.random.permutation(jax.random.fold_in(own, 1), rows)]
    offset_by = jax.random.randint(jax.random.fold_in(own, 2), (rows, 1), 0, top)
    return jnp.take_along_axis(grid, (jnp.arange(top)[None, :] + offset_by) % top, axis=1)


def portions_of(count, total, limit, skew, full):
    weights = [(1 << 20) // math.isqrt(rank ** skew) + 1 for rank in range(1, count + 1)]
    largest = limit if full else min(limit, max(-(-total // count), total * weights[0] // sum(weights)))
    least = 1 if total - largest >= count - 1 else 0
    holding, rest = [largest] + [least] * (count - 1), total - largest - least * (count - 1)
    while rest > 0:
        candidates = [i for i in range(1, count) if holding[i] < largest] or [i for i in range(1, count) if holding[i] < limit]
        whole, remaining = sum([weights[i] for i in candidates]), rest
        for i in candidates:
            extra = min(limit - holding[i], max(1, remaining * weights[i] // whole), rest)
            holding[i] = holding[i] + extra
            rest = rest - extra
    return np.array(holding)


def normal_values(own_key, dims, width, bound, pieces=(), held_as=jnp.bfloat16):
    factor_of = block_scale(own_key, dims, pieces, -0.22, 0.18) if pieces else 1.0
    values = jax.random.normal(own_key, dims, jnp.float32) * width * factor_of
    return jnp.minimum(jnp.maximum(values, -bound), bound).astype(held_as)


def setup_inputs(seed: int = 0) -> dict:
    key_list = jax.random.split(jax.random.key(seed), 11)
    tokens = draw_tokens(jax.random.fold_in(key_list[10], 71), 0)
    ln1_gain = jnp.clip(1.0 + 0.15 * jax.random.normal(key_list[1], (D,), jnp.float32), 0.25, 1.75)
    qkv_weight = draw_qkv_weight(jax.random.fold_in(key_list[10], 71), 0)
    out_weight = normal_values(key_list[3], (HEADS * DH, D), (HEADS * DH) ** -0.5, 0.125, ((0, 8), (1, 16)))
    ln2_gain = jnp.clip(1.0 + 0.15 * jax.random.normal(key_list[4], (D,), jnp.float32), 0.25, 1.75)
    ffn_in = normal_values(key_list[5], (D, FF), D ** -0.5, 0.125, ((0, 16), (1, 8)))
    ffn_out = normal_values(key_list[6], (FF, D), FF ** -0.5, 0.0625, ((0, 8), (1, 16)))
    expert_ids_keys = jax.random.split(jax.random.fold_in(key_list[7], 1), TOKENS // TOK_DEV)
    expert_ids_turns = jax.random.permutation(jax.random.fold_in(key_list[7], 3), TOKENS // TOK_DEV)
    expert_ids = jax.vmap(lambda own, number: assign_block(jax.random.fold_in(key_list[7], 2), own, number, TOK_DEV, EXPERTS, 1, CAP, 2))(expert_ids_keys, expert_ids_turns).reshape((TOKENS, 1))
    expert_in = normal_values(key_list[8], (EXPERTS * 2, D, HALF), D ** -0.5, 0.125, ((0, 128),))
    expert_out = normal_values(key_list[9], (EXPERTS * 2, HALF, D), FFE ** -0.5, 0.09375, ((0, 128),))
    return {"tokens": tokens, "ln1_gain": ln1_gain, "qkv_weight": qkv_weight, "out_weight": out_weight, "ln2_gain": ln2_gain, "ffn_in": ffn_in, "ffn_out": ffn_out, "expert_ids": expert_ids, "expert_in": expert_in, "expert_out": expert_out}


def layer_norm(row_data, gain_vector):
    row_data = row_data.astype(jnp.float32)
    centered = row_data - lax.optimization_barrier(jnp.mean(row_data, axis=-1, keepdims=True))
    spread = lax.optimization_barrier(jnp.mean(centered * centered, axis=-1, keepdims=True))
    return centered * lax.rsqrt(spread + 1e-06) * gain_vector

def attend_head(queries, key_rows, value_rows):
    scores = jnp.dot(queries, key_rows.T, preferred_element_type=jnp.float32) * DH ** (-0.5)
    row_max = lax.optimization_barrier(jnp.max(scores, axis=-1, keepdims=True))
    weights = jnp.exp(scores - row_max)
    probabilities = (weights / lax.optimization_barrier(jnp.sum(weights, axis=-1, keepdims=True))).astype(jnp.bfloat16)
    return jnp.dot(probabilities, value_rows, preferred_element_type=jnp.float32).astype(jnp.bfloat16)

def image_block(image_rows, ln1_gain, qkv_weight, out_weight, ln2_gain, ffn_in, ffn_out):
    normed = layer_norm(image_rows, ln1_gain).astype(jnp.bfloat16)
    projected = jnp.dot(normed, qkv_weight.reshape(D, HEADS * 3 * DH), preferred_element_type=jnp.float32)
    projected = projected.astype(jnp.bfloat16).reshape(SEQ, HEADS, 3, DH)
    by_head = jnp.transpose(projected, (1, 2, 0, 3))
    attended = lax.map(lambda head_item: attend_head(head_item[0], head_item[1], head_item[2]), by_head)
    attended = jnp.transpose(attended, (1, 0, 2)).reshape(SEQ, HEADS * DH)
    mixed_heads = jnp.dot(attended, out_weight, preferred_element_type=jnp.float32)
    hidden_state = (image_rows.astype(jnp.float32) + mixed_heads).astype(jnp.bfloat16)
    normed_two = layer_norm(hidden_state, ln2_gain).astype(jnp.bfloat16)
    inner_sum = jnp.dot(normed_two, ffn_in, preferred_element_type=jnp.float32)
    hidden_units = jax.nn.gelu(inner_sum, approximate=False).astype(jnp.bfloat16)
    dense_sum = jnp.zeros((SEQ, D), jnp.float32)
    for column_block in range(N_COL):
        lower_edge = column_block * FF_BLOCK
        part_sum = jnp.dot(hidden_units[:, lower_edge:lower_edge + FF_BLOCK], ffn_out[lower_edge:lower_edge + FF_BLOCK], preferred_element_type=jnp.float32)
        rounded = lax.optimization_barrier(part_sum.astype(jnp.bfloat16))
        dense_sum = dense_sum + rounded.astype(jnp.float32)
    return (hidden_state, normed_two, dense_sum)

def reference(tokens, ln1_gain, qkv_weight, out_weight, ln2_gain, ffn_in, ffn_out, expert_ids, expert_in, expert_out):
    device_count = N_ROW * N_COL
    images = tokens.reshape(TOKENS // SEQ, SEQ, D)

    def one_image(image_rows):
        return image_block(image_rows, ln1_gain, qkv_weight, out_weight, ln2_gain, ffn_in, ffn_out)
    hidden_state, normed_two, dense_sum = lax.map(one_image, images)
    hidden_state = hidden_state.reshape(TOKENS, D)
    normed_two = normed_two.reshape(TOKENS, D)
    dense_sum = dense_sum.reshape(TOKENS, D)
    chosen = expert_ids[:, 0].astype(jnp.int32)
    by_device = chosen.reshape(device_count, TOK_DEV)
    one_hot = (by_device[:, :, None] == jnp.arange(EXPERTS, dtype=jnp.int32)[None, None, :]).astype(jnp.int32)
    earlier = jnp.cumsum(one_hot, axis=1) - one_hot
    local_slot = lax.optimization_barrier(jnp.sum(earlier * one_hot, axis=2))
    global_slot = (local_slot + CAP * jnp.arange(device_count, dtype=jnp.int32)[:, None]).reshape(TOKENS).astype(jnp.int32)
    buffers = jnp.zeros((EXPERTS, device_count * CAP, D), normed_two.dtype).at[chosen, global_slot].set(normed_two)
    paired_in = expert_in.reshape(EXPERTS, 2, D, HALF)
    paired_out = expert_out.reshape(EXPERTS, 2, HALF, D)

    def run_expert(operands):
        buffer_rows, weights_in, weights_out = operands
        whole_in = jnp.concatenate((weights_in[0], weights_in[1]), axis=1)
        whole_out = jnp.concatenate((weights_out[0], weights_out[1]), axis=0)
        inner_units = jax.nn.gelu(jnp.dot(buffer_rows, whole_in, preferred_element_type=jnp.float32), approximate=False).astype(jnp.bfloat16)
        return jnp.dot(inner_units, whole_out, preferred_element_type=jnp.float32).astype(jnp.bfloat16)
    results = lax.map(run_expert, (buffers, paired_in, paired_out))
    expert_rows = results[chosen, global_slot]
    block_out = hidden_state.astype(jnp.float32) + dense_sum + expert_rows.astype(jnp.float32)
    return block_out.astype(jnp.bfloat16)
```

```python
import functools
import heapq
import jax
import jax.numpy as jnp
from jax import lax
from jax.experimental import pallas as pl
from jax.experimental.pallas import tpu as pltpu
from jax.sharding import PartitionSpec as P

MESH = pl.DeviceIdType.MESH
SPLIT = 32


class Net:
    def __init__(self, send, recv):
        row, col = lax.axis_index("row"), lax.axis_index("col")
        self.row, self.col = row, col
        self.high, self.y, self.core = row // 8, lax.rem(row // 2, 4), lax.rem(row, 2)
        self.x, self.low = col // 2, lax.rem(col, 2)
        self.send, self.recv = send, recv
        self.count = 0
        self.finish = []
        self.queue = []
        self.serial = 0

    def row_of(self, high, y, core):
        return high * 8 + lax.rem(y + 8, 4) * 2 + core

    def col_of(self, x, low):
        return lax.rem(x + 8, 4) * 2 + low

    def peer(self, name):
        high, y, core, x, low = self.high, self.y, self.core, self.x, self.low
        at = {
            "x+": (high, y, core, x + 1, low),
            "x-": (high, y, core, x - 1, low),
            "z": (high, y, core, x, 1 - low),
            "y+": (high, y + 1, core, x, low),
            "y-": (high, y - 1, core, x, low),
            "h": (1 - high, y, core, x, low),
            "c": (high, y, 1 - core, x, low),
        }[name]
        return self.row_of(*at[:3]), self.col_of(*at[3:])

    def greet(self, names):
        barrier = pltpu.get_barrier_semaphore()
        for name in names:
            pl.semaphore_signal(barrier, inc=1, device_id=self.peer(name), device_id_type=MESH)
        pl.semaphore_wait(barrier, len(names))

    def copy(self, src, dst, arriving, name):
        k = self.count
        self.count += 1
        make = lambda target: pltpu.make_async_remote_copy(
            src, target, self.send.at[k], self.recv.at[k], device_id=self.peer(name), device_id_type=MESH
        )
        out, arrival = make(dst), make(arriving)
        out.start()
        self.finish.append(out)
        return arrival

    def at(self, time, action):
        heapq.heappush(self.queue, (time, self.serial, action))
        self.serial += 1

    def when(self, time, arrival, action=None):
        def run():
            arrival.wait_recv()
            if action is not None:
                action()

        self.at(time, run)

    def run(self):
        while self.queue:
            heapq.heappop(self.queue)[2]()
        for out in self.finish:
            out.wait_send()


def rows_of(ref, start, size, step=16):
    return ref.at[pl.ds(pl.multiple_of(start, step), size)]


def spread(net, src, out):
    size = src.shape[0]
    a, half_a, half_b = SPLIT, SPLIT // 2, (size - SPLIT) // 2
    b = size - a
    x, low = net.x, net.low

    def part(dx, other, start, rows):
        plane = 1 - low if other else low
        return rows_of(out, net.col_of(x + dx, plane) * size + start, rows)

    def own(start, rows):
        return src.at[pl.ds(start, rows)]

    def from_a(side):
        step = 1 if side == "x-" else -1
        at = -step
        forward = "x+" if step > 0 else "x-"
        start = 0 if step > 0 else half_a
        got = part(at, 0, start, half_a)
        far = net.copy(got, got, part(at - step, 0, start, half_a), forward)
        net.when(6.0, far, lambda: to_z(part(2, 0, start, half_a), part(2, 1, start, half_a)))
        to_z(part(at, 0, 0, a), part(at, 1, 0, a))

    def to_z(got, arriving):
        net.when(27.0, net.copy(got, got, arriving, "z"))

    def from_b(side, other):
        step = 1 if side == "x-" else -1
        start = a if step > 0 else a + half_b
        got = part(-step, other, start, half_b)
        forward = "x+" if step > 0 else "x-"
        net.when(27.0, net.copy(got, got, part(-2 * step, other, start, half_b), forward))

    def from_z():
        got = part(0, 1, a, b)
        for side, forward in (("x-", "x+"), ("x+", "x-")):
            dx = -1 if side == "x-" else 1
            arrival = net.copy(got, got, part(dx, 1, a, b), forward)
            net.when(20.0, arrival, lambda side=side: from_b(side, 1))

    arrival = net.copy(own(a, b), part(0, 0, a, b), part(0, 1, a, b), "z")
    net.when(9.0, arrival, from_z)
    for side, forward in (("x-", "x+"), ("x+", "x-")):
        dx = -1 if side == "x-" else 1
        arrival = net.copy(own(0, a), part(0, 0, 0, a), part(dx, 0, 0, a), forward)
        net.when(4.0, arrival, lambda side=side: from_a(side))
    for side, forward in (("x-", "x+"), ("x+", "x-")):
        dx = -1 if side == "x-" else 1
        arrival = net.copy(own(a, b), part(0, 0, a, b), part(dx, 0, a, b), forward)
        net.when(12.0, arrival, lambda side=side: from_b(side, 0))
    to_z_own = net.copy(own(0, a), part(0, 0, 0, a), part(0, 1, 0, a), "z")
    net.when(27.0, to_z_own)
    out[pl.ds(pl.multiple_of(net.col * size, size), size), :] = src[...]


def spread_small(net, src, out):
    size = src.shape[0]
    x, low = net.x, net.low

    def part(dx, other):
        plane = 1 - low if other else low
        return rows_of(out, net.col_of(x + dx, plane) * size, size, 8)

    def onward(other):
        got = part(-1, other)
        net.when(27.0, net.copy(got, got, part(-2, other), "x+"))

    def around(other, got):
        arrival = net.copy(got, part(0, other), part(-1, other), "x+")
        net.when(5.0 + other, arrival, lambda: onward(other))
        net.when(27.0, net.copy(got, part(0, other), part(1, other), "x-"))

    around(0, src)
    arrival = net.copy(src, part(0, 0), part(0, 1), "z")
    net.when(3.0, arrival, lambda: around(1, part(0, 1)))
    out[pl.ds(pl.multiple_of(net.col * size, size), size), :] = src[...]


def gather(net, src, out, axis, early, late):
    depth, width = src.shape
    high, y, core = net.high, net.y, net.core
    middle = depth // 2

    def part(dy, other, core, half=None):
        index = net.row_of(1 - high if other else high, y + dy, core)
        start, size = (0, depth) if half is None else (half * middle, middle)
        if axis == 0:
            return rows_of(out, index * depth + start, size)
        return out.at[pl.ds(start, size), pl.ds(pl.multiple_of(index * width, width), width)]

    def to_core(dy, other, half=None):
        got = part(dy, other, core, half)
        net.when(late, net.copy(got, got, part(dy, other, 1 - core, half), "c"))

    def from_y(dy, other):
        got = part(dy, other, core, 0 if dy < 0 else 1)
        forward = "y+" if dy < 0 else "y-"
        half = 0 if dy < 0 else 1
        arrival = net.copy(got, got, part(2, other, core, half), forward)
        net.when(late - 1, arrival, lambda: to_core(2, other, half))
        to_core(dy, other)

    def around(other, got, time):
        for dy, forward in ((-1, "y+"), (1, "y-")):
            arrival = net.copy(got, part(0, other, core), part(dy, other, core), forward)
            net.when(time, arrival, lambda dy=dy: from_y(dy, other))

    around(0, src, early + 0.5)
    mine = part(0, 0, core)
    arrival = net.copy(src, mine, part(0, 1, core), "h")

    def from_high():
        around(1, part(0, 1, core), early + 0.6 * (late - early))
        to_core(0, 1)

    net.when(early + 0.3 * (late - early), arrival, from_high)
    net.when(late, net.copy(src, mine, part(0, 0, 1 - core), "c"))
    index = net.row
    if axis == 0:
        out[pl.ds(pl.multiple_of(index * depth, depth), depth), :] = src[...]
    else:
        out[:, pl.ds(pl.multiple_of(index * width, width), width)] = src[...]


def reduce_scatter(net, src, out, scratch):
    from_z, sums, far_a, near_a, acc_a, far_b, near_b, acc_b, plane, last = scratch
    size = out.shape[0]
    a = SPLIT
    b = size - a
    x, low = net.x, net.low

    def rows(dx, other, start, count):
        index = net.col_of(x + dx, 1 - low if other else low)
        return pl.ds(pl.multiple_of(index * size + start, 16), count)

    def ring(block, start, count, far, near, acc, times, done):
        half = count // 2
        halves = {"x+": (0, half), "x-": (half, half)}
        waiting = [4]

        def arrived():
            waiting[0] -= 1
            if waiting[0] == 0:
                done()

        for index, forward in ((0, "x+"), (1, "x-")):
            first = halves[forward][0]
            arrival = net.copy(block(2, first, half), far.at[index], far.at[index], forward)

            def add(index=index, forward=forward, first=first):
                term = block(1 if forward == "x+" else -1, first, half)
                acc[index] = far[index] + term[...]
                dst = near.at[index, pl.ds(first, half)]
                net.when(times[2], net.copy(acc.at[index], dst, dst, forward), arrived)

            net.when(times[0], arrival, add)
        for index, forward in ((0, "x+"), (1, "x-")):
            first = half - halves[forward][0]
            dst = near.at[index, pl.ds(first, half)]
            term = block(1 if forward == "x+" else -1, first, half)
            net.when(times[1], net.copy(term, dst, dst, forward), arrived)

    def block_b(other):
        return lambda dx, first, count: src.at[rows(dx, other, a + first, count)]

    def block_a(dx, first, count):
        return sums.at[pl.ds((dx % 4) * a + first, count)]

    arrivals = []
    for k in (2, 1, 3, 0):
        arrivals.append((k, net.copy(
            src.at[rows(k, 1, 0, a)], from_z.at[pl.ds(k * a, a)], from_z.at[pl.ds(k * a, a)], "z"
        )))

    def plane_done():
        index = rows(0, 1, a, b)
        total = near_b[0, 0].astype(jnp.float32) + near_b[0, 1].astype(jnp.float32)
        plane[...] = (total + src[index, :].astype(jnp.float32)).astype(plane.dtype)
        net.when(31.0, net.copy(plane, last, last, "z"), finish_b)

    def finish_b():
        out[pl.ds(a, b), :] = out[pl.ds(a, b), :] + last[...].astype(jnp.float32)

    def own_done():
        total = near_b[1, 0].astype(jnp.float32) + near_b[1, 1].astype(jnp.float32)
        out[pl.ds(a, b), :] = total + src[rows(0, 0, a, b), :].astype(jnp.float32)

    def a_done():
        total = near_a[0].astype(jnp.float32) + near_a[1].astype(jnp.float32)
        out[pl.ds(0, a), :] = total + sums[pl.ds(0, a), :].astype(jnp.float32)

    def start_a():
        for k, arrival in arrivals:
            arrival.wait_recv()
            sums[pl.ds(k * a, a), :] = from_z[pl.ds(k * a, a), :] + src[rows(k, 0, 0, a), :]
        ring(block_a, 0, a, far_a, near_a, acc_a, (26.0, 29.0, 29.5), a_done)

    ring(block_b(1), a, b, far_b.at[0], near_b.at[0], acc_b.at[0], (5.0, 18.0, 18.5), plane_done)
    ring(block_b(0), a, b, far_b.at[1], near_b.at[1], acc_b.at[1], (9.0, 27.0, 27.5), own_done)
    net.at(13.0, start_a)


def scatter_scratch(size, width, dtype):
    a = SPLIT
    b = size - a
    shapes = [(4 * a, width), (4 * a, width), (2, a // 2, width), (2, a, width), (2, a // 2, width)]
    shapes += [(2, 2, b // 2, width), (2, 2, b, width), (2, 2, b // 2, width), (b, width), (b, width)]
    return [pltpu.VMEM(shape, dtype) for shape in shapes]


def comm_body(spreads, smalls, gathers, sums, *refs):
    count = spreads + smalls + len(gathers) + sums
    ins, outs, rest = refs[:count], refs[count : 2 * count], refs[2 * count :]
    scratch, (send, recv) = rest[:-2], rest[-2:]
    net = Net(send, recv)
    names = []
    if spreads or smalls or sums:
        names += ["x+", "x-", "z"]
    if gathers:
        names += ["y+", "y-", "h", "c"]
    net.greet(names)
    k = 0
    for _ in range(sums):
        reduce_scatter(net, ins[k], outs[k], scratch)
        k += 1
    for _ in range(spreads):
        spread(net, ins[k], outs[k])
        k += 1
    for _ in range(smalls):
        spread_small(net, ins[k], outs[k])
        k += 1
    for axis, early, late in gathers:
        gather(net, ins[k], outs[k], axis, early, late)
        k += 1
    net.run()


def exchange(name, collective_id, sums=(), spreads=(), smalls=(), gathers=()):
    row_total = lax.axis_size("row")
    col_total = lax.axis_size("col")
    arrays, shapes, scratch, copies = [], [], [], 0
    for array in sums:
        size = array.shape[0] // col_total
        arrays.append(array)
        shapes.append(jax.ShapeDtypeStruct((size, array.shape[1]), jnp.float32))
        scratch += scatter_scratch(size, array.shape[1], array.dtype)
        copies += 24
    for array in spreads:
        arrays.append(array)
        shapes.append(jax.ShapeDtypeStruct((array.shape[0] * col_total, array.shape[1]), array.dtype))
        copies += 20
    for array in smalls:
        arrays.append(array)
        shapes.append(jax.ShapeDtypeStruct((array.shape[0] * col_total, array.shape[1]), array.dtype))
        copies += 8
    for array, axis, _, _ in gathers:
        depth, width = array.shape
        arrays.append(array)
        shape = (depth * row_total, width) if axis == 0 else (depth, width * row_total)
        shapes.append(jax.ShapeDtypeStruct(shape, array.dtype))
        copies += 20
    return pl.pallas_call(
        functools.partial(comm_body, len(spreads), len(smalls), [g[1:] for g in gathers], len(sums)),
        out_shape=shapes,
        in_specs=[pl.BlockSpec(memory_space=pltpu.VMEM)] * len(arrays),
        out_specs=[pl.BlockSpec(memory_space=pltpu.VMEM)] * len(arrays),
        scratch_shapes=scratch + [pltpu.SemaphoreType.DMA((copies,)), pltpu.SemaphoreType.DMA((copies,))],
        compiler_params=pltpu.CompilerParams(
            collective_id=collective_id, has_side_effects=True, vmem_limit_bytes=40 * 2**20
        ),
        name=name,
    )(*arrays)


def shuffle_body(sign, row_total, source, out, stage, send, recv, local):
    row = lax.axis_index("row")
    col = lax.axis_index("col")
    barrier = pltpu.get_barrier_semaphore()
    for step in range(1, row_total):
        pl.semaphore_signal(
            barrier, inc=1, device_id=(lax.rem(row + step, row_total), col), device_id_type=MESH
        )
    load = pltpu.make_async_copy(source, stage, local.at[0])
    load.start()
    pl.semaphore_wait(barrier, row_total - 1)
    load.wait()
    copies = []
    for step in range(1, row_total):
        to = lax.rem(row + (step if sign > 0 else row_total - step), row_total)
        copy = pltpu.make_async_remote_copy(
            stage.at[step], out.at[step], send.at[step - 1], recv.at[step - 1], device_id=(to, col), device_id_type=MESH
        )
        copy.start()
        copies.append(copy)
    own = pltpu.make_async_copy(stage.at[0], out.at[0], local.at[1])
    own.start()
    for copy in copies:
        copy.wait()
    own.wait()


def shuffle(name, collective_id, array, sign):
    row_total = lax.axis_size("row")
    return pl.pallas_call(
        functools.partial(shuffle_body, sign, row_total),
        out_shape=jax.ShapeDtypeStruct(array.shape, array.dtype),
        in_specs=[pl.BlockSpec(memory_space=pl.ANY)],
        out_specs=pl.BlockSpec(memory_space=pl.ANY),
        scratch_shapes=[
            pltpu.VMEM(array.shape, array.dtype),
            pltpu.SemaphoreType.DMA((row_total - 1,)),
            pltpu.SemaphoreType.DMA((row_total - 1,)),
            pltpu.SemaphoreType.DMA((2,)),
        ],
        compiler_params=pltpu.CompilerParams(
            collective_id=collective_id, has_side_effects=True, vmem_limit_bytes=24 * 2**20
        ),
        name=name,
    )(array)


def up_body(x_ref, w_ref, o_ref):
    inner = jnp.dot(x_ref[...], w_ref[...], preferred_element_type=jnp.float32)
    o_ref[...] = (inner * (1.0 + lax.erf(inner * (0.5**0.5))) * 0.5).astype(o_ref.dtype)


def up_gelu(x, w):
    rows, depth = x.shape
    width = w.shape[1]
    tile = min(width, 256)
    return pl.pallas_call(
        up_body,
        grid=(width // tile,),
        out_shape=jax.ShapeDtypeStruct((rows, width), jnp.bfloat16),
        in_specs=[
            pl.BlockSpec((rows, depth), lambda j: (0, 0)),
            pl.BlockSpec((depth, tile), lambda j: (0, j)),
        ],
        out_specs=pl.BlockSpec((rows, tile), lambda j: (0, j)),
        compiler_params=pltpu.CompilerParams(vmem_limit_bytes=32 * 2**20),
        cost_estimate=pl.CostEstimate(
            flops=2 * rows * depth * width,
            bytes_accessed=2 * (rows * depth + depth * width + rows * width),
            transcendentals=0,
        ),
        name="up_gelu",
    )(x, w)


def layer_norm(row_data, gain_vector):
    row_data = row_data.astype(jnp.float32)
    centered = row_data - jnp.mean(row_data, axis=-1, keepdims=True)
    spread = jnp.mean(centered * centered, axis=-1, keepdims=True)
    return centered * lax.rsqrt(spread + 1e-06) * gain_vector


def matmul(a, b):
    return jnp.dot(a, b, preferred_element_type=jnp.float32)


def shards(
    tokens,
    ln1_gain,
    qkv_weight,
    out_weight,
    ln2_gain,
    ffn_in,
    ffn_out,
    expert_ids,
    expert_in,
    expert_out,
):
    tok_count, model_width = tokens.shape
    row_total = lax.axis_size("row")
    col_total = lax.axis_size("col")
    row_index = lax.axis_index("row")
    col_index = lax.axis_index("col")
    expert_count = row_total * col_total // 2
    capacity = max(2, 2 * tok_count // expert_count)
    head_count, head_dim = qkv_weight.shape[1], qkv_weight.shape[3]
    seq_len = tok_count * col_total

    ids_block = jnp.broadcast_to(expert_ids[:, 0][None, :], (8, tok_count))
    image_rows, ids_all, qkv_whole, out_whole = exchange(
        "enter",
        0,
        spreads=(tokens,),
        smalls=(ids_block,),
        gathers=((qkv_weight.reshape(qkv_weight.shape[0], -1), 0, 3.0, 14.0), (out_weight, 1, 13.0, 19.0)),
    )
    normed = layer_norm(image_rows, ln1_gain).astype(jnp.bfloat16)
    projected = matmul(normed, qkv_whole).astype(jnp.bfloat16)
    projected = projected.reshape(seq_len, head_count, 3, head_dim)
    queries, keys, values = projected[:, :, 0], projected[:, :, 1], projected[:, :, 2]
    scores = jnp.einsum("qhd,khd->hqk", queries, keys, preferred_element_type=jnp.float32)
    scores = scores * (head_dim ** (-0.5))
    weights = jnp.exp(scores - jnp.max(scores, axis=-1, keepdims=True))
    probabilities = (weights / jnp.sum(weights, axis=-1, keepdims=True)).astype(jnp.bfloat16)
    attended = jnp.einsum("hqk,khd->qhd", probabilities, values, preferred_element_type=jnp.float32)
    attended = attended.astype(jnp.bfloat16).reshape(seq_len, head_count * head_dim)
    head_terms = matmul(attended, out_whole).astype(jnp.bfloat16)
    mixed_heads, up_whole = exchange("heads", 1, sums=(head_terms,), gathers=((ffn_in, 0, 5.0, 19.0),))
    hidden_mine = (tokens.astype(jnp.float32) + mixed_heads).astype(jnp.bfloat16)
    normed_mine = layer_norm(hidden_mine, ln2_gain).astype(jnp.bfloat16)

    normed_image, down_whole = exchange(
        "norms", 2, spreads=(normed_mine,), gathers=((ffn_out, 1, 5.0, 19.0),)
    )

    ids_rows = ids_all.reshape(col_total, 8, tok_count)[:, 0]
    expert_range = jnp.arange(expert_count, dtype=jnp.int32)
    one_hot = (ids_rows[:, :, None] == expert_range).astype(jnp.int32)
    earlier = jnp.cumsum(one_hot, axis=1) - one_hot
    slot_index = jnp.sum(earlier * one_hot, axis=2)
    block_index = jnp.arange(col_total, dtype=jnp.int32)[:, None]
    home_row = 2 * ids_rows // col_total
    mine = (2 * ids_rows % col_total) // 2 == col_index // 2
    step = (home_row - row_index + row_total) % row_total
    position = (step * col_total + block_index) * capacity + slot_index
    position = jnp.where(mine, position, -1).reshape(seq_len)
    slot_count = row_total * col_total * capacity
    slots = jnp.arange(slot_count, dtype=jnp.int32)
    placing = (slots[:, None] == position[None, :]).astype(jnp.bfloat16)
    picking = (position[:, None] == slots[None, :]).astype(jnp.bfloat16)

    table = matmul(placing, normed_image).astype(jnp.bfloat16)
    table = table.reshape(row_total, col_total * capacity, model_width)
    expert_rows = shuffle("dispatch", 3, table, 1)
    expert_units = up_gelu(expert_rows.reshape(slot_count, model_width), expert_in[0])
    partial_out = matmul(expert_units, expert_out[0]).astype(jnp.bfloat16)
    partial_out = partial_out.reshape(row_total, col_total * capacity, model_width)
    returned = shuffle("collect", 4, partial_out, -1)

    hidden_units = up_gelu(normed_image, up_whole)
    rows_two = returned.reshape(slot_count, model_width)
    partial = matmul(hidden_units, down_whole) + matmul(picking, rows_two)
    (total,) = exchange("leave", 5, sums=(partial.astype(jnp.bfloat16),))
    return (hidden_mine.astype(jnp.float32) + total).astype(jnp.bfloat16)


def solution(mesh):
    in_specs = (
        P(("row", "col"), None),
        P(),
        P("row", "col", None, None),
        P("col", "row"),
        P(),
        P("row", "col"),
        P("col", "row"),
        P(("row", "col"), None),
        P(("row", "col"), None, None),
        P(("row", "col"), None, None),
    )
    out_specs = P(("row", "col"), None)
    return jax.shard_map(shards, mesh=mesh, in_specs=in_specs, out_specs=out_specs, check_vma=False)
```

```python
import functools
import heapq
import jax
import jax.numpy as jnp
from jax import lax
from jax.experimental import pallas as pl
from jax.experimental.pallas import tpu as pltpu
from jax.sharding import PartitionSpec as P

MESH = pl.DeviceIdType.MESH
SPLIT = 32


class Net:
    def __init__(self, send, recv):
        row, col = lax.axis_index("row"), lax.axis_index("col")
        self.row, self.col = row, col
        self.high, self.y, self.core = row // 8, lax.rem(row // 2, 4), lax.rem(row, 2)
        self.x, self.low = col // 2, lax.rem(col, 2)
        self.send, self.recv = send, recv
        self.count = 0
        self.finish = []
        self.queue = []
        self.serial = 0

    def row_of(self, high, y, core):
        return high * 8 + lax.rem(y + 8, 4) * 2 + core

    def col_of(self, x, low):
        return lax.rem(x + 8, 4) * 2 + low

    def peer(self, name):
        high, y, core, x, low = self.high, self.y, self.core, self.x, self.low
        at = {
            "x+": (high, y, core, x + 1, low),
            "x-": (high, y, core, x - 1, low),
            "z": (high, y, core, x, 1 - low),
            "y+": (high, y + 1, core, x, low),
            "y-": (high, y - 1, core, x, low),
            "w": (1 - high, y, core, x, 1 - low),
            "c": (high, y, 1 - core, x, low),
            "y+c": (high, y + 1, 1 - core, x, low),
            "y-c": (high, y - 1, 1 - core, x, low),
        }[name]
        return self.row_of(*at[:3]), self.col_of(*at[3:])

    def greet(self, names):
        barrier = pltpu.get_barrier_semaphore()
        for name in names:
            pl.semaphore_signal(barrier, inc=1, device_id=self.peer(name), device_id_type=MESH)
        pl.semaphore_wait(barrier, len(names))

    def copy(self, src, dst, arriving, name):
        k = self.count
        self.count += 1
        make = lambda target: pltpu.make_async_remote_copy(
            src, target, self.send.at[k], self.recv.at[k], device_id=self.peer(name), device_id_type=MESH
        )
        out, arrival = make(dst), make(arriving)
        out.start()
        self.finish.append(out)
        return arrival

    def at(self, time, action):
        heapq.heappush(self.queue, (time, self.serial, action))
        self.serial += 1

    def when(self, time, arrival, action=None):
        def run():
            arrival.wait_recv()
            if action is not None:
                action()

        self.at(time, run)

    def run(self):
        while self.queue:
            heapq.heappop(self.queue)[2]()
        for out in self.finish:
            out.wait_send()


def rows_of(ref, start, size, step=16):
    return ref.at[pl.ds(pl.multiple_of(start, step), size)]


def spread(net, src, out):
    size = src.shape[0]
    a, half_a, half_b = SPLIT, SPLIT // 2, (size - SPLIT) // 2
    b = size - a
    x, low = net.x, net.low

    def part(dx, other, start, rows):
        plane = 1 - low if other else low
        return rows_of(out, net.col_of(x + dx, plane) * size + start, rows)

    def own(start, rows):
        return src.at[pl.ds(start, rows)]

    def from_a(side):
        step = 1 if side == "x-" else -1
        at = -step
        forward = "x+" if step > 0 else "x-"
        start = 0 if step > 0 else half_a
        got = part(at, 0, start, half_a)
        far = net.copy(got, got, part(at - step, 0, start, half_a), forward)
        net.when(6.0, far, lambda: to_z(part(2, 0, start, half_a), part(2, 1, start, half_a)))
        to_z(part(at, 0, 0, a), part(at, 1, 0, a))

    def to_z(got, arriving):
        net.when(27.0, net.copy(got, got, arriving, "z"))

    def from_b(side, other):
        step = 1 if side == "x-" else -1
        start = a if step > 0 else a + half_b
        got = part(-step, other, start, half_b)
        forward = "x+" if step > 0 else "x-"
        net.when(27.0, net.copy(got, got, part(-2 * step, other, start, half_b), forward))

    def from_z():
        got = part(0, 1, a, b)
        for side, forward in (("x-", "x+"), ("x+", "x-")):
            dx = -1 if side == "x-" else 1
            arrival = net.copy(got, got, part(dx, 1, a, b), forward)
            net.when(20.0, arrival, lambda side=side: from_b(side, 1))

    arrival = net.copy(own(a, b), part(0, 0, a, b), part(0, 1, a, b), "z")
    net.when(9.0, arrival, from_z)
    for side, forward in (("x-", "x+"), ("x+", "x-")):
        dx = -1 if side == "x-" else 1
        arrival = net.copy(own(0, a), part(0, 0, 0, a), part(dx, 0, 0, a), forward)
        net.when(4.0, arrival, lambda side=side: from_a(side))
    for side, forward in (("x-", "x+"), ("x+", "x-")):
        dx = -1 if side == "x-" else 1
        arrival = net.copy(own(a, b), part(0, 0, a, b), part(dx, 0, a, b), forward)
        net.when(12.0, arrival, lambda side=side: from_b(side, 0))
    to_z_own = net.copy(own(0, a), part(0, 0, 0, a), part(0, 1, 0, a), "z")
    net.when(27.0, to_z_own)
    out[pl.ds(pl.multiple_of(net.col * size, size), size), :] = src[...]


def spread_small(net, src, out):
    size = src.shape[0]
    x, low = net.x, net.low

    def part(dx, other):
        plane = 1 - low if other else low
        return rows_of(out, net.col_of(x + dx, plane) * size, size, 8)

    def onward(other):
        got = part(-1, other)
        net.when(27.0, net.copy(got, got, part(-2, other), "x+"))

    def around(other, got):
        arrival = net.copy(got, part(0, other), part(-1, other), "x+")
        net.when(5.0 + other, arrival, lambda: onward(other))
        net.when(27.0, net.copy(got, part(0, other), part(1, other), "x-"))

    around(0, src)
    arrival = net.copy(src, part(0, 0), part(0, 1), "z")
    net.when(3.0, arrival, lambda: around(1, part(0, 1)))
    out[pl.ds(pl.multiple_of(net.col * size, size), size), :] = src[...]


def gather(net, src, out, relay, axis, early, late):
    depth, width = src.shape
    high, y, core = net.high, net.y, net.core
    middle = depth // 2

    def part(dy, other, core, half=None):
        index = net.row_of(1 - high if other else high, y + dy, core)
        start, size = (0, depth) if half is None else (half * middle, middle)
        if axis == 0:
            return rows_of(out, index * depth + start, size)
        return out.at[pl.ds(start, size), pl.ds(pl.multiple_of(index * width, width), width)]

    def to_core(dy, other, half=None):
        got = part(dy, other, core, half)
        net.when(late, net.copy(got, got, part(dy, other, 1 - core, half), "c"))

    def from_y(dy, other):
        got = part(dy, other, core, 0 if dy < 0 else 1)
        forward = "y+" if dy < 0 else "y-"
        half = 0 if dy < 0 else 1
        arrival = net.copy(got, got, part(2, other, core, half), forward)
        net.when(late - 1, arrival, lambda: to_core(2, other, half))
        to_core(dy, other)

    def around(other, got, time):
        for dy, forward in ((-1, "y+"), (1, "y-")):
            arrival = net.copy(got, part(0, other, core), part(dy, other, core), forward)
            net.when(time, arrival, lambda dy=dy: from_y(dy, other))

    around(0, src, early + 0.5)
    span = late - early
    waiting = [2]

    def arrived():
        waiting[0] -= 1
        if waiting[0] == 0:
            around(1, part(0, 1, core), early + 0.6 * span)
            to_core(0, 1)

    for half, first, second in ((0, "z", "w"), (1, "w", "z")):
        arrival = net.copy(src.at[pl.ds(half * middle, middle)], relay.at[half], relay.at[half], first)

        def onward(half=half, second=second):
            got = relay.at[half]
            arrival = net.copy(got, part(0, half, core, half), part(0, 1, core, half), second)
            net.when(early + 0.45 * span, arrival, arrived)

        net.when(early + 0.2 * span, arrival, onward)
    mine = part(0, 0, core)
    net.when(late, net.copy(src, mine, part(0, 0, 1 - core), "c"))
    index = net.row
    if axis == 0:
        out[pl.ds(pl.multiple_of(index * depth, depth), depth), :] = src[...]
    else:
        out[:, pl.ds(pl.multiple_of(index * width, width), width)] = src[...]


def reduce_scatter(net, src, out, scratch):
    from_z, sums, far_a, near_a, acc_a, far_b, near_b, acc_b, plane, last = scratch
    size = out.shape[0]
    a = SPLIT
    b = size - a
    x, low = net.x, net.low

    def rows(dx, other, start, count):
        index = net.col_of(x + dx, 1 - low if other else low)
        return pl.ds(pl.multiple_of(index * size + start, 16), count)

    def ring(block, start, count, far, near, acc, times, done):
        half = count // 2
        halves = {"x+": (0, half), "x-": (half, half)}
        waiting = [4]

        def arrived():
            waiting[0] -= 1
            if waiting[0] == 0:
                done()

        for index, forward in ((0, "x+"), (1, "x-")):
            first = halves[forward][0]
            arrival = net.copy(block(2, first, half), far.at[index], far.at[index], forward)

            def add(index=index, forward=forward, first=first):
                term = block(1 if forward == "x+" else -1, first, half)
                acc[index] = far[index] + term[...]
                dst = near.at[index, pl.ds(first, half)]
                net.when(times[2], net.copy(acc.at[index], dst, dst, forward), arrived)

            net.when(times[0], arrival, add)
        for index, forward in ((0, "x+"), (1, "x-")):
            first = half - halves[forward][0]
            dst = near.at[index, pl.ds(first, half)]
            term = block(1 if forward == "x+" else -1, first, half)
            net.when(times[1], net.copy(term, dst, dst, forward), arrived)

    def block_b(other):
        return lambda dx, first, count: src.at[rows(dx, other, a + first, count)]

    def block_a(dx, first, count):
        return sums.at[pl.ds((dx % 4) * a + first, count)]

    arrivals = []
    for k in (2, 1, 3, 0):
        arrivals.append((k, net.copy(
            src.at[rows(k, 1, 0, a)], from_z.at[pl.ds(k * a, a)], from_z.at[pl.ds(k * a, a)], "z"
        )))

    def plane_done():
        index = rows(0, 1, a, b)
        total = near_b[0, 0].astype(jnp.float32) + near_b[0, 1].astype(jnp.float32)
        plane[...] = (total + src[index, :].astype(jnp.float32)).astype(plane.dtype)
        net.when(31.0, net.copy(plane, last, last, "z"), finish_b)

    def finish_b():
        out[pl.ds(a, b), :] = out[pl.ds(a, b), :] + last[...].astype(jnp.float32)

    def own_done():
        total = near_b[1, 0].astype(jnp.float32) + near_b[1, 1].astype(jnp.float32)
        out[pl.ds(a, b), :] = total + src[rows(0, 0, a, b), :].astype(jnp.float32)

    def a_done():
        total = near_a[0].astype(jnp.float32) + near_a[1].astype(jnp.float32)
        out[pl.ds(0, a), :] = total + sums[pl.ds(0, a), :].astype(jnp.float32)

    def start_a():
        for k, arrival in arrivals:
            arrival.wait_recv()
            sums[pl.ds(k * a, a), :] = from_z[pl.ds(k * a, a), :] + src[rows(k, 0, 0, a), :]
        ring(block_a, 0, a, far_a, near_a, acc_a, (26.0, 29.0, 29.5), a_done)

    ring(block_b(1), a, b, far_b.at[0], near_b.at[0], acc_b.at[0], (5.0, 18.0, 18.5), plane_done)
    ring(block_b(0), a, b, far_b.at[1], near_b.at[1], acc_b.at[1], (9.0, 27.0, 27.5), own_done)
    net.at(13.0, start_a)


def scatter_scratch(size, width, dtype):
    a = SPLIT
    b = size - a
    shapes = [(4 * a, width), (4 * a, width), (2, a // 2, width), (2, a, width), (2, a // 2, width)]
    shapes += [(2, 2, b // 2, width), (2, 2, b, width), (2, 2, b // 2, width), (b, width), (b, width)]
    return [pltpu.VMEM(shape, dtype) for shape in shapes]


def comm_body(spreads, smalls, gathers, sums, *refs):
    count = spreads + smalls + len(gathers) + sums
    ins, outs, rest = refs[:count], refs[count : 2 * count], refs[2 * count :]
    scratch, (send, recv) = rest[:-2], rest[-2:]
    net = Net(send, recv)
    names = []
    if spreads or smalls or sums:
        names += ["x+", "x-", "z"]
    if gathers:
        names += ["y+", "y-", "w", "c"] + ([] if names else ["z"])
    net.greet(names)
    relays = list(scratch[10 * sums :])
    k = 0
    for _ in range(sums):
        reduce_scatter(net, ins[k], outs[k], scratch[:10])
        k += 1
    for _ in range(spreads):
        spread(net, ins[k], outs[k])
        k += 1
    for _ in range(smalls):
        spread_small(net, ins[k], outs[k])
        k += 1
    for axis, early, late in gathers:
        gather(net, ins[k], outs[k], relays.pop(0), axis, early, late)
        k += 1
    net.run()


def exchange(name, collective_id, sums=(), spreads=(), smalls=(), gathers=()):
    row_total = lax.axis_size("row")
    col_total = lax.axis_size("col")
    arrays, shapes, scratch, copies = [], [], [], 0
    for array in sums:
        size = array.shape[0] // col_total
        arrays.append(array)
        shapes.append(jax.ShapeDtypeStruct((size, array.shape[1]), jnp.float32))
        scratch += scatter_scratch(size, array.shape[1], array.dtype)
        copies += 24
    for array in spreads:
        arrays.append(array)
        shapes.append(jax.ShapeDtypeStruct((array.shape[0] * col_total, array.shape[1]), array.dtype))
        copies += 20
    for array in smalls:
        arrays.append(array)
        shapes.append(jax.ShapeDtypeStruct((array.shape[0] * col_total, array.shape[1]), array.dtype))
        copies += 8
    for array, axis, _, _ in gathers:
        depth, width = array.shape
        arrays.append(array)
        shape = (depth * row_total, width) if axis == 0 else (depth, width * row_total)
        shapes.append(jax.ShapeDtypeStruct(shape, array.dtype))
        scratch.append(pltpu.VMEM((2, depth // 2, width), array.dtype))
        copies += 22
    return pl.pallas_call(
        functools.partial(comm_body, len(spreads), len(smalls), [g[1:] for g in gathers], len(sums)),
        out_shape=shapes,
        in_specs=[pl.BlockSpec(memory_space=pltpu.VMEM)] * len(arrays),
        out_specs=[pl.BlockSpec(memory_space=pltpu.VMEM)] * len(arrays),
        scratch_shapes=scratch + [pltpu.SemaphoreType.DMA((copies,)), pltpu.SemaphoreType.DMA((copies,))],
        compiler_params=pltpu.CompilerParams(
            collective_id=collective_id, has_side_effects=True, vmem_limit_bytes=40 * 2**20
        ),
        name=name,
    )(*arrays)


def y_exchange(net, src, dst, relay, times, ready=None, arrived=None):
    core = net.core
    half = src.shape[2] // 2
    tell = arrived or (lambda d: None)

    def opposite():
        for index, forward in ((0, "y+"), (1, "y-")):
            rows = pl.ds(index * half, half)
            arrival = net.copy(src.at[2, :, rows], relay.at[index], relay.at[index], forward)

            def onward(index=index, forward=forward, rows=rows):
                for c, name in ((core, forward), (1 - core, forward + "c")):
                    arrival = net.copy(relay.at[index, c], dst.at[2, core, rows], dst.at[2, c, rows], name)
                    net.when(times[3], arrival, lambda: tell(2))

            net.when(times[1], arrival, onward)

    def beside(d):
        forward = "y+" if d == 1 else "y-"
        for c, name in ((core, forward), (1 - core, forward + "c")):
            arrival = net.copy(src.at[d, c], dst.at[4 - d, core], dst.at[4 - d, c], name)
            net.when(times[2], arrival, lambda: tell(4 - d))

    def here():
        net.when(times[2], net.copy(src.at[0, 1 - core], dst.at[0, core], dst.at[0, 1 - core], "c"), lambda: tell(0))
        dst[0, core] = src[0, core]

    steps = {2: opposite, 1: lambda: beside(1), 3: lambda: beside(3), 0: here}
    if ready is None:
        for d in (2, 1, 3, 0):
            steps[d]()
    else:
        ready(steps)


def dispatch_body(x_ref, w_ref, table, hidden, out, far, relay, send, recv):
    net = Net(send, recv)
    net.greet(["y+", "y-", "y+c", "y-c", "c", "z", "w"])
    low = net.low
    half = table.shape[3] // 2
    mine, theirs = pl.ds(pl.multiple_of(low * half, half), half), pl.ds(pl.multiple_of((1 - low) * half, half), half)

    def ready(steps):
        for k, d in enumerate((2, 1, 3, 0)):
            arrival = net.copy(table.at[1, d, :, mine], far.at[d, :, mine], far.at[d, :, theirs], "w")

            def onward(k=k, d=d):
                arrival = net.copy(far.at[d, :, theirs], far.at[d, :, theirs], far.at[d, :, mine], "z")
                net.when(7.0 + 2.5 * k, arrival, steps[d])

            net.when(3.5 + 2.5 * k, arrival, onward)

    y_exchange(net, table.at[0], out.at[0], relay.at[0], (0.0, 5.0, 12.0, 16.0))
    y_exchange(net, far, out.at[1], relay.at[1], (0.0, 17.0, 24.0, 25.0), ready)
    up_tasks(net, x_ref, w_ref, hidden, 1.0, 1.2)
    net.run()


def up_tasks(net, x_ref, w_ref, out, start, every):
    rows, width = out.shape
    tile = min(256, rows)
    span = min(256, width)

    def piece(j):
        columns = pl.ds(j * span, span)

        @pl.loop(0, rows // tile)
        def _(i):
            at = pl.ds(pl.multiple_of(i * tile, tile), tile)
            inner = jnp.dot(x_ref[at, :], w_ref[:, columns], preferred_element_type=jnp.float32)
            out[at, columns] = (inner * (1.0 + lax.erf(inner * (0.5**0.5))) * 0.5).astype(out.dtype)

    for j in range(width // span):
        net.at(start + every * j, lambda j=j: piece(j))


def down_tasks(net, x_ref, w_ref, out, start, every):
    rows, width = out.shape
    tile = min(256, rows)
    span = min(512, width)

    def piece(j):
        columns = pl.ds(j * span, span)

        @pl.loop(0, rows // tile)
        def _(i):
            at = pl.ds(pl.multiple_of(i * tile, tile), tile)
            product = jnp.dot(x_ref[at, :], w_ref[:, columns], preferred_element_type=jnp.float32)
            out[at, columns] = product.astype(out.dtype)

    for j in range(width // span):
        net.at(start + every * j, lambda j=j: piece(j))


def collect_body(x_ref, w_ref, parts, dense, near, across, far, other, total, relay, send, recv):
    net = Net(send, recv)
    net.greet(["y+", "y-", "y+c", "y-c", "c", "z", "w"])
    low = net.low
    half = parts.shape[3] // 2
    mine, theirs = pl.ds(pl.multiple_of(low * half, half), half), pl.ds(pl.multiple_of((1 - low) * half, half), half)
    left = {0: 1, 1: 2, 2: 4, 3: 2}
    after = {0: 9.0, 1: 13.0, 3: 15.0, 2: 18.0}

    def arrived(d):
        left[d] -= 1
        if left[d]:
            return

        def add():
            total[d] = far[d, :, theirs] + other[d]
            net.when(27.0, net.copy(total.at[d], across.at[d], across.at[d], "w"))

        net.when(after[d], net.copy(far.at[d, :, mine], other.at[d], other.at[d], "z"), add)

    y_exchange(net, parts.at[1], far, relay.at[1], (0.0, 5.0, 9.0, 14.0), None, arrived)
    y_exchange(net, parts.at[0], near, relay.at[0], (0.0, 14.5, 22.0, 25.0))
    down_tasks(net, x_ref, w_ref, dense, 0.5, 2.0)
    net.run()


def expert_call(name, body, collective_id, arrays, shapes, scratch):
    copies = 40
    return pl.pallas_call(
        body,
        out_shape=[jax.ShapeDtypeStruct(shape, jnp.bfloat16) for shape in shapes],
        in_specs=[pl.BlockSpec(memory_space=pltpu.VMEM)] * len(arrays),
        out_specs=[pl.BlockSpec(memory_space=pltpu.VMEM)] * len(shapes),
        scratch_shapes=[pltpu.VMEM(shape, jnp.bfloat16) for shape in scratch]
        + [pltpu.SemaphoreType.DMA((copies,)), pltpu.SemaphoreType.DMA((copies,))],
        compiler_params=pltpu.CompilerParams(
            collective_id=collective_id, has_side_effects=True, vmem_limit_bytes=48 * 2**20
        ),
        name=name,
    )(*arrays)


def up_body(x_ref, w_ref, o_ref):
    inner = jnp.dot(x_ref[...], w_ref[...], preferred_element_type=jnp.float32)
    o_ref[...] = (inner * (1.0 + lax.erf(inner * (0.5**0.5))) * 0.5).astype(o_ref.dtype)


def up_gelu(x, w):
    rows, depth = x.shape
    width = w.shape[1]
    tile = min(width, 256)
    return pl.pallas_call(
        up_body,
        grid=(width // tile,),
        out_shape=jax.ShapeDtypeStruct((rows, width), jnp.bfloat16),
        in_specs=[
            pl.BlockSpec((rows, depth), lambda j: (0, 0)),
            pl.BlockSpec((depth, tile), lambda j: (0, j)),
        ],
        out_specs=pl.BlockSpec((rows, tile), lambda j: (0, j)),
        compiler_params=pltpu.CompilerParams(vmem_limit_bytes=32 * 2**20),
        cost_estimate=pl.CostEstimate(
            flops=2 * rows * depth * width,
            bytes_accessed=2 * (rows * depth + depth * width + rows * width),
            transcendentals=0,
        ),
        name="up_gelu",
    )(x, w)


def layer_norm(row_data, gain_vector):
    row_data = row_data.astype(jnp.float32)
    centered = row_data - jnp.mean(row_data, axis=-1, keepdims=True)
    spread = jnp.mean(centered * centered, axis=-1, keepdims=True)
    return centered * lax.rsqrt(spread + 1e-06) * gain_vector


def matmul(a, b):
    return jnp.dot(a, b, preferred_element_type=jnp.float32)


def shards(
    tokens,
    ln1_gain,
    qkv_weight,
    out_weight,
    ln2_gain,
    ffn_in,
    ffn_out,
    expert_ids,
    expert_in,
    expert_out,
):
    tok_count, model_width = tokens.shape
    row_total = lax.axis_size("row")
    col_total = lax.axis_size("col")
    row_index = lax.axis_index("row")
    col_index = lax.axis_index("col")
    expert_count = row_total * col_total // 2
    capacity = max(2, 2 * tok_count // expert_count)
    head_count, head_dim = qkv_weight.shape[1], qkv_weight.shape[3]
    seq_len = tok_count * col_total

    ids_block = jnp.broadcast_to(expert_ids[:, 0][None, :], (8, tok_count))
    image_rows, ids_all, qkv_whole, out_whole = exchange(
        "enter",
        0,
        spreads=(tokens,),
        smalls=(ids_block,),
        gathers=((qkv_weight.reshape(qkv_weight.shape[0], -1), 0, 3.0, 14.0), (out_weight, 1, 13.0, 19.0)),
    )
    normed = layer_norm(image_rows, ln1_gain).astype(jnp.bfloat16)
    projected = matmul(normed, qkv_whole).astype(jnp.bfloat16)
    projected = projected.reshape(seq_len, head_count, 3, head_dim)
    queries, keys, values = projected[:, :, 0], projected[:, :, 1], projected[:, :, 2]
    scores = jnp.einsum("qhd,khd->hqk", queries, keys, preferred_element_type=jnp.float32)
    scores = scores * (head_dim ** (-0.5))
    weights = jnp.exp(scores - jnp.max(scores, axis=-1, keepdims=True))
    probabilities = (weights / jnp.sum(weights, axis=-1, keepdims=True)).astype(jnp.bfloat16)
    attended = jnp.einsum("hqk,khd->qhd", probabilities, values, preferred_element_type=jnp.float32)
    attended = attended.astype(jnp.bfloat16).reshape(seq_len, head_count * head_dim)
    head_terms = matmul(attended, out_whole).astype(jnp.bfloat16)
    mixed_heads, up_whole = exchange("heads", 1, sums=(head_terms,), gathers=((ffn_in, 0, 5.0, 19.0),))
    hidden_mine = (tokens.astype(jnp.float32) + mixed_heads).astype(jnp.bfloat16)
    normed_mine = layer_norm(hidden_mine, ln2_gain).astype(jnp.bfloat16)

    normed_image, down_whole = exchange(
        "norms", 2, spreads=(normed_mine,), gathers=((ffn_out, 1, 5.0, 19.0),)
    )

    ids_rows = ids_all.reshape(col_total, 8, tok_count)[:, 0]
    expert_range = jnp.arange(expert_count, dtype=jnp.int32)
    one_hot = (ids_rows[:, :, None] == expert_range).astype(jnp.int32)
    earlier = jnp.cumsum(one_hot, axis=1) - one_hot
    slot_index = jnp.sum(earlier * one_hot, axis=2)
    block_index = jnp.arange(col_total, dtype=jnp.int32)[:, None]
    home_row = 2 * ids_rows // col_total
    mine = (2 * ids_rows % col_total) // 2 == col_index // 2
    other = (home_row // 8 != row_index // 8).astype(jnp.int32)
    step = (home_row // 2 - row_index // 2 + 8) % 4
    chunk = step * 2 + home_row % 2
    place = block_index * capacity + slot_index
    rows = col_total * capacity
    position = jnp.where(mine, (other * 8 + chunk) * rows + place, -1).reshape(seq_len)
    slot_count = row_total * rows
    slots = jnp.arange(slot_count, dtype=jnp.int32)
    placing = (slots[:, None] == position[None, :]).astype(jnp.bfloat16)
    half = rows // 2
    crossed = jnp.where(place // half == col_index % 2, 8 * rows + chunk * half + place % half, -1)
    source = jnp.where(mine, jnp.where(other == 1, crossed, chunk * rows + place), -1).reshape(seq_len)
    returned_slots = jnp.arange(8 * (rows + half), dtype=jnp.int32)
    picking = (source[:, None] == returned_slots[None, :]).astype(jnp.bfloat16)

    table = matmul(placing, normed_image).astype(jnp.bfloat16)
    table = table.reshape(2, 4, 2, rows, model_width)
    full, part = (4, 2, rows, model_width), (4, 2, half, model_width)
    relays = (2, 2, 2, half, model_width)
    hidden_units, expert_rows = expert_call(
        "dispatch",
        dispatch_body,
        3,
        (normed_image, up_whole, table),
        ((seq_len, up_whole.shape[1]), table.shape),
        (full, relays),
    )
    expert_units = up_gelu(expert_rows.reshape(slot_count, model_width), expert_in[0])
    partial_out = matmul(expert_units, expert_out[0]).astype(jnp.bfloat16).reshape(table.shape)
    dense, near, across = expert_call(
        "collect",
        collect_body,
        4,
        (hidden_units, down_whole, partial_out),
        ((seq_len, model_width), full, part),
        (full, part, part, relays),
    )
    rows_two = jnp.concatenate((near.reshape(-1, model_width), across.reshape(-1, model_width)))
    partial = dense.astype(jnp.float32) + matmul(picking, rows_two)
    (total,) = exchange("leave", 5, sums=(partial.astype(jnp.bfloat16),))
    return (hidden_mine.astype(jnp.float32) + total).astype(jnp.bfloat16)


def solution(mesh):
    in_specs = (
        P(("row", "col"), None),
        P(),
        P("row", "col", None, None),
        P("col", "row"),
        P(),
        P("row", "col"),
        P("col", "row"),
        P(("row", "col"), None),
        P(("row", "col"), None, None),
        P(("row", "col"), None, None),
    )
    out_specs = P(("row", "col"), None)
    return jax.shard_map(shards, mesh=mesh, in_specs=in_specs, out_specs=out_specs, check_vma=False)
```

```python
import functools
import heapq
import math
import jax
import jax.numpy as jnp
from jax import lax
from jax.experimental import pallas as pl
from jax.experimental.pallas import tpu as pltpu
from jax.sharding import PartitionSpec as P

MESH = pl.DeviceIdType.MESH
SPLIT = 32


class Net:
    def __init__(self, send, recv):
        row, col = lax.axis_index("row"), lax.axis_index("col")
        self.row, self.col = row, col
        self.high, self.y, self.core = row // 8, lax.rem(row // 2, 4), lax.rem(row, 2)
        self.x, self.low = col // 2, lax.rem(col, 2)
        self.send, self.recv = send, recv
        self.count = 0
        self.finish = []
        self.queue = []
        self.serial = 0
        self.now = 0.0
        self.free = {}
        self.spare = []

    def row_of(self, high, y, core):
        return high * 8 + lax.rem(y + 8, 4) * 2 + core

    def col_of(self, x, low):
        return lax.rem(x + 8, 4) * 2 + low

    def peer(self, name):
        high, y, core, x, low = self.high, self.y, self.core, self.x, self.low
        at = {
            "x+": (high, y, core, x + 1, low),
            "x-": (high, y, core, x - 1, low),
            "z": (high, y, core, x, 1 - low),
            "y+": (high, y + 1, core, x, low),
            "y-": (high, y - 1, core, x, low),
            "w": (1 - high, y, core, x, 1 - low),
            "c": (high, y, 1 - core, x, low),
            "y+c": (high, y + 1, 1 - core, x, low),
            "y-c": (high, y - 1, 1 - core, x, low),
        }[name]
        return self.row_of(*at[:3]), self.col_of(*at[3:])

    def greet(self, names):
        barrier = pltpu.get_barrier_semaphore()
        for name in names:
            pl.semaphore_signal(barrier, inc=1, device_id=self.peer(name), device_id_type=MESH)
        pl.semaphore_wait(barrier, len(names))

    def copy(self, src, dst, arriving, name):
        k = self.count
        self.count += 1
        make = lambda target: pltpu.make_async_remote_copy(
            src, target, self.send.at[k], self.recv.at[k], device_id=self.peer(name), device_id_type=MESH
        )
        out, arrival = make(dst), make(arriving)
        out.start()
        self.finish.append(out)
        rate, delay = (600e3, 1.0) if name == "c" else (46e3, 2.0)
        begin = max(self.now, self.free.get(name[:2], 0.0))
        self.free[name[:2]] = begin + math.prod(arriving.shape) * arriving.dtype.itemsize / rate
        return arrival, self.free[name[:2]] + delay

    def when(self, pending, action=None):
        arrival, time = pending

        def run():
            arrival.wait_recv()
            if action is not None:
                action()

        heapq.heappush(self.queue, (time, self.serial, run))
        self.serial += 1

    def work(self, time, action):
        self.spare.append((time, action))

    def spend(self, time):
        self.now += time

    def run(self):
        while self.queue or self.spare:
            if self.spare and (not self.queue or self.queue[0][0] > self.now + 0.5 * self.spare[0][0]):
                time, action = self.spare.pop(0)
                action()
                self.now += time
                continue
            time, _, action = heapq.heappop(self.queue)
            self.now = max(self.now, time) + 0.02
            action()
        for out in self.finish:
            out.wait_send()


def rows_of(ref, start, size, step=16):
    return ref.at[pl.ds(pl.multiple_of(start, step), size)]


def spread(net, src, out):
    size = src.shape[0]
    a, half_a, half_b = SPLIT, SPLIT // 2, (size - SPLIT) // 2
    b = size - a
    x, low = net.x, net.low

    def part(dx, other, start, rows):
        plane = 1 - low if other else low
        return rows_of(out, net.col_of(x + dx, plane) * size + start, rows)

    def own(start, rows):
        return src.at[pl.ds(start, rows)]

    def from_a(side):
        step = 1 if side == "x-" else -1
        at = -step
        forward = "x+" if step > 0 else "x-"
        start = 0 if step > 0 else half_a
        got = part(at, 0, start, half_a)
        far = net.copy(got, got, part(at - step, 0, start, half_a), forward)
        net.when(far, lambda: to_z(part(2, 0, start, half_a), part(2, 1, start, half_a)))
        to_z(part(at, 0, 0, a), part(at, 1, 0, a))

    def to_z(got, arriving):
        net.when(net.copy(got, got, arriving, "z"))

    def from_b(side, other):
        step = 1 if side == "x-" else -1
        start = a if step > 0 else a + half_b
        got = part(-step, other, start, half_b)
        forward = "x+" if step > 0 else "x-"
        net.when(net.copy(got, got, part(-2 * step, other, start, half_b), forward))

    def from_z():
        got = part(0, 1, a, b)
        for side, forward in (("x-", "x+"), ("x+", "x-")):
            dx = -1 if side == "x-" else 1
            arrival = net.copy(got, got, part(dx, 1, a, b), forward)
            net.when(arrival, lambda side=side: from_b(side, 1))

    arrival = net.copy(own(a, b), part(0, 0, a, b), part(0, 1, a, b), "z")
    net.when(arrival, from_z)
    for side, forward in (("x-", "x+"), ("x+", "x-")):
        dx = -1 if side == "x-" else 1
        arrival = net.copy(own(0, a), part(0, 0, 0, a), part(dx, 0, 0, a), forward)
        net.when(arrival, lambda side=side: from_a(side))
    for side, forward in (("x-", "x+"), ("x+", "x-")):
        dx = -1 if side == "x-" else 1
        arrival = net.copy(own(a, b), part(0, 0, a, b), part(dx, 0, a, b), forward)
        net.when(arrival, lambda side=side: from_b(side, 0))
    to_z_own = net.copy(own(0, a), part(0, 0, 0, a), part(0, 1, 0, a), "z")
    net.when(to_z_own)
    out[pl.ds(pl.multiple_of(net.col * size, size), size), :] = src[...]


def spread_small(net, src, out):
    size = src.shape[0]
    x, low = net.x, net.low

    def part(dx, other):
        plane = 1 - low if other else low
        return rows_of(out, net.col_of(x + dx, plane) * size, size, 8)

    def onward(other):
        got = part(-1, other)
        net.when(net.copy(got, got, part(-2, other), "x+"))

    def around(other, got):
        arrival = net.copy(got, part(0, other), part(-1, other), "x+")
        net.when(arrival, lambda: onward(other))
        net.when(net.copy(got, part(0, other), part(1, other), "x-"))

    around(0, src)
    arrival = net.copy(src, part(0, 0), part(0, 1), "z")
    net.when(arrival, lambda: around(1, part(0, 1)))
    out[pl.ds(pl.multiple_of(net.col * size, size), size), :] = src[...]


def gather(net, src, out, relay, axis):
    depth, width = src.shape
    high, y, core = net.high, net.y, net.core
    middle = depth // 2

    def part(dy, other, core, half=None):
        index = net.row_of(1 - high if other else high, y + dy, core)
        start, size = (0, depth) if half is None else (half * middle, middle)
        if axis == 0:
            return rows_of(out, index * depth + start, size)
        return out.at[pl.ds(start, size), pl.ds(pl.multiple_of(index * width, width), width)]

    def to_core(dy, other, half=None):
        got = part(dy, other, core, half)
        net.when(net.copy(got, got, part(dy, other, 1 - core, half), "c"))

    def from_y(dy, other):
        got = part(dy, other, core, 0 if dy < 0 else 1)
        forward = "y+" if dy < 0 else "y-"
        half = 0 if dy < 0 else 1
        arrival = net.copy(got, got, part(2, other, core, half), forward)
        net.when(arrival, lambda: to_core(2, other, half))
        to_core(dy, other)

    def around(other, got):
        for dy, forward in ((-1, "y+"), (1, "y-")):
            arrival = net.copy(got, part(0, other, core), part(dy, other, core), forward)
            net.when(arrival, lambda dy=dy: from_y(dy, other))

    around(0, src)
    waiting = [2]

    def arrived():
        waiting[0] -= 1
        if waiting[0] == 0:
            around(1, part(0, 1, core))
            to_core(0, 1)

    for half, first, second in ((0, "z", "w"), (1, "w", "z")):
        arrival = net.copy(src.at[pl.ds(half * middle, middle)], relay.at[half], relay.at[half], first)

        def onward(half=half, second=second):
            got = relay.at[half]
            arrival = net.copy(got, part(0, half, core, half), part(0, 1, core, half), second)
            net.when(arrival, arrived)

        net.when(arrival, onward)
    mine = part(0, 0, core)
    net.when(net.copy(src, mine, part(0, 0, 1 - core), "c"))
    index = net.row
    if axis == 0:
        out[pl.ds(pl.multiple_of(index * depth, depth), depth), :] = src[...]
    else:
        out[:, pl.ds(pl.multiple_of(index * width, width), width)] = src[...]


def reduce_scatter(net, src, out, scratch):
    from_z, sums, far_a, near_a, acc_a, far_b, near_b, acc_b, plane, last = scratch
    size = out.shape[0]
    a = SPLIT
    b = size - a
    x, low = net.x, net.low

    def rows(dx, other, start, count):
        index = net.col_of(x + dx, 1 - low if other else low)
        return pl.ds(pl.multiple_of(index * size + start, 16), count)

    def ring(block, count, far, near, acc, done):
        half = count // 2
        halves = {"x+": (0, half), "x-": (half, half)}
        waiting = [4]

        def arrived():
            waiting[0] -= 1
            if waiting[0] == 0:
                done()

        for index, forward in ((0, "x+"), (1, "x-")):
            first = halves[forward][0]
            arrival = net.copy(block(2, first, half), far.at[index], far.at[index], forward)

            def add(index=index, forward=forward, first=first):
                term = block(1 if forward == "x+" else -1, first, half)
                acc[index] = far[index] + term[...]
                net.spend(0.1)
                dst = near.at[index, pl.ds(first, half)]
                net.when(net.copy(acc.at[index], dst, dst, forward), arrived)

            net.when(arrival, add)
        for index, forward in ((0, "x+"), (1, "x-")):
            first = half - halves[forward][0]
            dst = near.at[index, pl.ds(first, half)]
            term = block(1 if forward == "x+" else -1, first, half)
            net.when(net.copy(term, dst, dst, forward), arrived)

    def block_b(other):
        return lambda dx, first, count: src.at[rows(dx, other, a + first, count)]

    def block_a(dx, first, count):
        return sums.at[pl.ds((dx % 4) * a + first, count)]

    left = [4]

    def from_partner(k):
        sums[pl.ds(k * a, a), :] = from_z[pl.ds(k * a, a), :] + src[rows(k, 0, 0, a), :]
        net.spend(0.1)
        left[0] -= 1
        if left[0] == 0:
            ring(block_a, a, far_a, near_a, acc_a, a_done)

    for k in (2, 1, 3, 0):
        landing = from_z.at[pl.ds(k * a, a)]
        net.when(net.copy(src.at[rows(k, 1, 0, a)], landing, landing, "z"), lambda k=k: from_partner(k))

    def plane_done():
        index = rows(0, 1, a, b)
        total = near_b[0, 0].astype(jnp.float32) + near_b[0, 1].astype(jnp.float32)
        plane[...] = (total + src[index, :].astype(jnp.float32)).astype(plane.dtype)
        net.when(net.copy(plane, last, last, "z"), finish_b)

    both = [2]

    def finish_b():
        both[0] -= 1
        if both[0]:
            return
        total = near_b[1, 0].astype(jnp.float32) + near_b[1, 1].astype(jnp.float32)
        out[pl.ds(a, b), :] = total + src[rows(0, 0, a, b), :].astype(jnp.float32) + last[...].astype(jnp.float32)

    def a_done():
        total = near_a[0].astype(jnp.float32) + near_a[1].astype(jnp.float32)
        out[pl.ds(0, a), :] = total + sums[pl.ds(0, a), :].astype(jnp.float32)

    ring(block_b(1), b, far_b.at[0], near_b.at[0], acc_b.at[0], plane_done)
    ring(block_b(0), b, far_b.at[1], near_b.at[1], acc_b.at[1], finish_b)


def scatter_scratch(size, width, dtype):
    a = SPLIT
    b = size - a
    shapes = [(4 * a, width), (4 * a, width), (2, a // 2, width), (2, a, width), (2, a // 2, width)]
    shapes += [(2, 2, b // 2, width), (2, 2, b, width), (2, 2, b // 2, width), (b, width), (b, width)]
    return [pltpu.VMEM(shape, dtype) for shape in shapes]


def comm_body(spreads, smalls, gathers, sums, *refs):
    count = spreads + smalls + len(gathers) + sums
    ins, outs, rest = refs[:count], refs[count : 2 * count], refs[2 * count :]
    scratch, (send, recv) = rest[:-2], rest[-2:]
    net = Net(send, recv)
    names = []
    if spreads or smalls or sums:
        names += ["x+", "x-", "z"]
    if gathers:
        names += ["y+", "y-", "w", "c"] + ([] if names else ["z"])
    net.greet(names)
    relays = list(scratch[10 * sums :])
    k = 0
    for _ in range(sums):
        reduce_scatter(net, ins[k], outs[k], scratch[:10])
        k += 1
    for _ in range(spreads):
        spread(net, ins[k], outs[k])
        k += 1
    for _ in range(smalls):
        spread_small(net, ins[k], outs[k])
        k += 1
    for axis in gathers:
        gather(net, ins[k], outs[k], relays.pop(0), axis)
        k += 1
    net.run()


def exchange(name, collective_id, sums=(), spreads=(), smalls=(), gathers=()):
    row_total = lax.axis_size("row")
    col_total = lax.axis_size("col")
    arrays, shapes, scratch, copies = [], [], [], 0
    for array in sums:
        size = array.shape[0] // col_total
        arrays.append(array)
        shapes.append(jax.ShapeDtypeStruct((size, array.shape[1]), jnp.float32))
        scratch += scatter_scratch(size, array.shape[1], array.dtype)
        copies += 24
    for array in spreads:
        arrays.append(array)
        shapes.append(jax.ShapeDtypeStruct((array.shape[0] * col_total, array.shape[1]), array.dtype))
        copies += 20
    for array in smalls:
        arrays.append(array)
        shapes.append(jax.ShapeDtypeStruct((array.shape[0] * col_total, array.shape[1]), array.dtype))
        copies += 8
    for array, axis in gathers:
        depth, width = array.shape
        arrays.append(array)
        shape = (depth * row_total, width) if axis == 0 else (depth, width * row_total)
        shapes.append(jax.ShapeDtypeStruct(shape, array.dtype))
        scratch.append(pltpu.VMEM((2, depth // 2, width), array.dtype))
        copies += 22
    return pl.pallas_call(
        functools.partial(comm_body, len(spreads), len(smalls), [axis for _, axis in gathers], len(sums)),
        out_shape=shapes,
        in_specs=[pl.BlockSpec(memory_space=pltpu.VMEM)] * len(arrays),
        out_specs=[pl.BlockSpec(memory_space=pltpu.VMEM)] * len(arrays),
        scratch_shapes=scratch + [pltpu.SemaphoreType.DMA((copies,)), pltpu.SemaphoreType.DMA((copies,))],
        compiler_params=pltpu.CompilerParams(
            collective_id=collective_id, has_side_effects=True, vmem_limit_bytes=40 * 2**20
        ),
        name=name,
    )(*arrays)


def y_exchange(net, src, dst, relay, ready=None, arrived=None):
    core = net.core
    half = src.shape[2] // 2
    tell = arrived or (lambda d: None)

    def opposite():
        for index, forward in ((0, "y+"), (1, "y-")):
            rows = pl.ds(index * half, half)
            arrival = net.copy(src.at[2, :, rows], relay.at[index], relay.at[index], forward)

            def onward(index=index, forward=forward, rows=rows):
                for c, name in ((core, forward), (1 - core, forward + "c")):
                    arrival = net.copy(relay.at[index, c], dst.at[2, core, rows], dst.at[2, c, rows], name)
                    net.when(arrival, lambda: tell(2))

            net.when(arrival, onward)

    def beside(d):
        forward = "y+" if d == 1 else "y-"
        for c, name in ((core, forward), (1 - core, forward + "c")):
            arrival = net.copy(src.at[d, c], dst.at[4 - d, core], dst.at[4 - d, c], name)
            net.when(arrival, lambda: tell(4 - d))

    def here():
        net.when(net.copy(src.at[0, 1 - core], dst.at[0, core], dst.at[0, 1 - core], "c"), lambda: tell(0))
        dst[0, core] = src[0, core]

    steps = {2: opposite, 1: lambda: beside(1), 3: lambda: beside(3), 0: here}
    if ready is None:
        for d in (2, 1, 3, 0):
            steps[d]()
    else:
        ready(steps)


def dispatch_body(x_ref, w_ref, table, hidden, out, far, relay, send, recv):
    net = Net(send, recv)
    net.greet(["y+", "y-", "y+c", "y-c", "c", "z", "w"])
    low = net.low
    half = table.shape[3] // 2
    mine, theirs = pl.ds(pl.multiple_of(low * half, half), half), pl.ds(pl.multiple_of((1 - low) * half, half), half)

    def ready(steps):
        for d in (2, 1, 3, 0):
            arrival = net.copy(table.at[1, d, :, mine], far.at[d, :, mine], far.at[d, :, theirs], "w")

            def onward(d=d):
                arrival = net.copy(far.at[d, :, theirs], far.at[d, :, theirs], far.at[d, :, mine], "z")
                net.when(arrival, steps[d])

            net.when(arrival, onward)

    y_exchange(net, table.at[0], out.at[0], relay.at[0])
    y_exchange(net, far, out.at[1], relay.at[1], ready)
    up_tasks(net, x_ref, w_ref, hidden)
    net.run()


def up_tasks(net, x_ref, w_ref, out):
    rows, width = out.shape
    tile = min(256, rows)
    span = min(256, width)

    def piece(j):
        columns = pl.ds(j * span, span)

        @pl.loop(0, rows // tile)
        def _(i):
            at = pl.ds(pl.multiple_of(i * tile, tile), tile)
            inner = jnp.dot(x_ref[at, :], w_ref[:, columns], preferred_element_type=jnp.float32)
            out[at, columns] = (inner * (1.0 + lax.erf(inner * (0.5**0.5))) * 0.5).astype(out.dtype)

    for j in range(width // span):
        net.work(1.2, lambda j=j: piece(j))


def down_tasks(net, x_ref, w_ref, out):
    rows, width = out.shape
    tile = min(256, rows)
    span = min(512, width)

    def piece(j):
        columns = pl.ds(j * span, span)

        @pl.loop(0, rows // tile)
        def _(i):
            at = pl.ds(pl.multiple_of(i * tile, tile), tile)
            product = jnp.dot(x_ref[at, :], w_ref[:, columns], preferred_element_type=jnp.float32)
            out[at, columns] = product.astype(out.dtype)

    for j in range(width // span):
        net.work(1.2, lambda j=j: piece(j))


def collect_body(x_ref, w_ref, parts, dense, near, across, far, other, total, relay, send, recv):
    net = Net(send, recv)
    net.greet(["y+", "y-", "y+c", "y-c", "c", "z", "w"])
    low = net.low
    half = parts.shape[3] // 2
    mine, theirs = pl.ds(pl.multiple_of(low * half, half), half), pl.ds(pl.multiple_of((1 - low) * half, half), half)
    left = {0: 1, 1: 2, 2: 4, 3: 2}

    def arrived(d):
        left[d] -= 1
        if left[d]:
            return

        def add():
            total[d] = far[d, :, theirs] + other[d]
            net.spend(0.2)
            net.when(net.copy(total.at[d], across.at[d], across.at[d], "w"))

        net.when(net.copy(far.at[d, :, mine], other.at[d], other.at[d], "z"), add)

    y_exchange(net, parts.at[1], far, relay.at[1], None, arrived)
    y_exchange(net, parts.at[0], near, relay.at[0])
    down_tasks(net, x_ref, w_ref, dense)
    net.run()


def expert_call(name, body, collective_id, arrays, shapes, scratch):
    copies = 40
    return pl.pallas_call(
        body,
        out_shape=[jax.ShapeDtypeStruct(shape, jnp.bfloat16) for shape in shapes],
        in_specs=[pl.BlockSpec(memory_space=pltpu.VMEM)] * len(arrays),
        out_specs=[pl.BlockSpec(memory_space=pltpu.VMEM)] * len(shapes),
        scratch_shapes=[pltpu.VMEM(shape, jnp.bfloat16) for shape in scratch]
        + [pltpu.SemaphoreType.DMA((copies,)), pltpu.SemaphoreType.DMA((copies,))],
        compiler_params=pltpu.CompilerParams(
            collective_id=collective_id, has_side_effects=True, vmem_limit_bytes=48 * 2**20
        ),
        name=name,
    )(*arrays)


def up_body(x_ref, w_ref, o_ref):
    inner = jnp.dot(x_ref[...], w_ref[...], preferred_element_type=jnp.float32)
    o_ref[...] = (inner * (1.0 + lax.erf(inner * (0.5**0.5))) * 0.5).astype(o_ref.dtype)


def up_gelu(x, w):
    rows, depth = x.shape
    width = w.shape[1]
    tile = min(width, 256)
    return pl.pallas_call(
        up_body,
        grid=(width // tile,),
        out_shape=jax.ShapeDtypeStruct((rows, width), jnp.bfloat16),
        in_specs=[
            pl.BlockSpec((rows, depth), lambda j: (0, 0)),
            pl.BlockSpec((depth, tile), lambda j: (0, j)),
        ],
        out_specs=pl.BlockSpec((rows, tile), lambda j: (0, j)),
        compiler_params=pltpu.CompilerParams(vmem_limit_bytes=32 * 2**20),
        cost_estimate=pl.CostEstimate(
            flops=2 * rows * depth * width,
            bytes_accessed=2 * (rows * depth + depth * width + rows * width),
            transcendentals=0,
        ),
        name="up_gelu",
    )(x, w)


def layer_norm(row_data, gain_vector):
    row_data = row_data.astype(jnp.float32)
    centered = row_data - jnp.mean(row_data, axis=-1, keepdims=True)
    spread = jnp.mean(centered * centered, axis=-1, keepdims=True)
    return centered * lax.rsqrt(spread + 1e-06) * gain_vector


def matmul(a, b):
    return jnp.dot(a, b, preferred_element_type=jnp.float32)


def shards(
    tokens,
    ln1_gain,
    qkv_weight,
    out_weight,
    ln2_gain,
    ffn_in,
    ffn_out,
    expert_ids,
    expert_in,
    expert_out,
):
    tok_count, model_width = tokens.shape
    row_total = lax.axis_size("row")
    col_total = lax.axis_size("col")
    row_index = lax.axis_index("row")
    col_index = lax.axis_index("col")
    expert_count = row_total * col_total // 2
    capacity = max(2, 2 * tok_count // expert_count)
    head_count, head_dim = qkv_weight.shape[1], qkv_weight.shape[3]
    seq_len = tok_count * col_total

    ids_block = jnp.broadcast_to(expert_ids[:, 0][None, :], (8, tok_count))
    image_rows, ids_all, qkv_whole, out_whole = exchange(
        "enter",
        0,
        spreads=(tokens,),
        smalls=(ids_block,),
        gathers=((qkv_weight.reshape(qkv_weight.shape[0], -1), 0), (out_weight, 1)),
    )
    normed = layer_norm(image_rows, ln1_gain).astype(jnp.bfloat16)
    projected = matmul(normed, qkv_whole).astype(jnp.bfloat16)
    projected = projected.reshape(seq_len, head_count, 3, head_dim)
    queries, keys, values = projected[:, :, 0], projected[:, :, 1], projected[:, :, 2]
    scores = jnp.einsum("qhd,khd->hqk", queries, keys, preferred_element_type=jnp.float32)
    scores = scores * (head_dim ** (-0.5))
    weights = jnp.exp(scores - jnp.max(scores, axis=-1, keepdims=True))
    probabilities = (weights / jnp.sum(weights, axis=-1, keepdims=True)).astype(jnp.bfloat16)
    attended = jnp.einsum("hqk,khd->qhd", probabilities, values, preferred_element_type=jnp.float32)
    attended = attended.astype(jnp.bfloat16).reshape(seq_len, head_count * head_dim)
    head_terms = matmul(attended, out_whole).astype(jnp.bfloat16)
    mixed_heads, up_whole = exchange("heads", 1, sums=(head_terms,), gathers=((ffn_in, 0),))
    hidden_mine = (tokens.astype(jnp.float32) + mixed_heads).astype(jnp.bfloat16)
    normed_mine = layer_norm(hidden_mine, ln2_gain).astype(jnp.bfloat16)

    normed_image, down_whole = exchange(
        "norms", 2, spreads=(normed_mine,), gathers=((ffn_out, 1),)
    )

    ids_rows = ids_all.reshape(col_total, 8, tok_count)[:, 0]
    expert_range = jnp.arange(expert_count, dtype=jnp.int32)
    one_hot = (ids_rows[:, :, None] == expert_range).astype(jnp.int32)
    earlier = jnp.cumsum(one_hot, axis=1) - one_hot
    slot_index = jnp.sum(earlier * one_hot, axis=2)
    block_index = jnp.arange(col_total, dtype=jnp.int32)[:, None]
    home_row = 2 * ids_rows // col_total
    mine = (2 * ids_rows % col_total) // 2 == col_index // 2
    other = (home_row // 8 != row_index // 8).astype(jnp.int32)
    step = (home_row // 2 - row_index // 2 + 8) % 4
    chunk = step * 2 + home_row % 2
    place = block_index * capacity + slot_index
    rows = col_total * capacity
    position = jnp.where(mine, (other * 8 + chunk) * rows + place, -1).reshape(seq_len)
    slot_count = row_total * rows
    slots = jnp.arange(slot_count, dtype=jnp.int32)
    placing = (slots[:, None] == position[None, :]).astype(jnp.bfloat16)
    half = rows // 2
    crossed = jnp.where(place // half == col_index % 2, 8 * rows + chunk * half + place % half, -1)
    source = jnp.where(mine, jnp.where(other == 1, crossed, chunk * rows + place), -1).reshape(seq_len)
    returned_slots = jnp.arange(8 * (rows + half), dtype=jnp.int32)
    picking = (source[:, None] == returned_slots[None, :]).astype(jnp.bfloat16)

    table = matmul(placing, normed_image).astype(jnp.bfloat16)
    table = table.reshape(2, 4, 2, rows, model_width)
    full, part = (4, 2, rows, model_width), (4, 2, half, model_width)
    relays = (2, 2, 2, half, model_width)
    hidden_units, expert_rows = expert_call(
        "dispatch",
        dispatch_body,
        3,
        (normed_image, up_whole, table),
        ((seq_len, up_whole.shape[1]), table.shape),
        (full, relays),
    )
    expert_units = up_gelu(expert_rows.reshape(slot_count, model_width), expert_in[0])
    partial_out = matmul(expert_units, expert_out[0]).astype(jnp.bfloat16).reshape(table.shape)
    dense, near, across = expert_call(
        "collect",
        collect_body,
        4,
        (hidden_units, down_whole, partial_out),
        ((seq_len, model_width), full, part),
        (full, part, part, relays),
    )
    rows_two = jnp.concatenate((near.reshape(-1, model_width), across.reshape(-1, model_width)))
    partial = dense.astype(jnp.float32) + matmul(picking, rows_two)
    (total,) = exchange("leave", 5, sums=(partial.astype(jnp.bfloat16),))
    return (hidden_mine.astype(jnp.float32) + total).astype(jnp.bfloat16)


def solution(mesh):
    in_specs = (
        P(("row", "col"), None),
        P(),
        P("row", "col", None, None),
        P("col", "row"),
        P(),
        P("row", "col"),
        P("col", "row"),
        P(("row", "col"), None),
        P(("row", "col"), None, None),
        P(("row", "col"), None, None),
    )
    out_specs = P(("row", "col"), None)
    return jax.shard_map(shards, mesh=mesh, in_specs=in_specs, out_specs=out_specs, check_vma=False)
```

```python
import functools
import heapq
import math
import jax
import jax.numpy as jnp
from jax import lax
from jax.experimental import pallas as pl
from jax.experimental.pallas import tpu as pltpu
from jax.sharding import PartitionSpec as P

MESH = pl.DeviceIdType.MESH
SPLIT = 32


class Net:
    def __init__(self, send, recv):
        row, col = lax.axis_index("row"), lax.axis_index("col")
        self.row, self.col = row, col
        self.high, self.y, self.core = row // 8, lax.rem(row // 2, 4), lax.rem(row, 2)
        self.x, self.low = col // 2, lax.rem(col, 2)
        self.send, self.recv = send, recv
        self.count = 0
        self.finish = []
        self.queue = []
        self.serial = 0
        self.now = 0.0
        self.free = {}
        self.spare = []

    def row_of(self, high, y, core):
        return high * 8 + lax.rem(y + 8, 4) * 2 + core

    def col_of(self, x, low):
        return lax.rem(x + 8, 4) * 2 + low

    def peer(self, name):
        high, y, core, x, low = self.high, self.y, self.core, self.x, self.low
        at = {
            "x+": (high, y, core, x + 1, low),
            "x-": (high, y, core, x - 1, low),
            "z": (high, y, core, x, 1 - low),
            "y+": (high, y + 1, core, x, low),
            "y-": (high, y - 1, core, x, low),
            "w": (1 - high, y, core, x, 1 - low),
            "c": (high, y, 1 - core, x, low),
            "y+c": (high, y + 1, 1 - core, x, low),
            "y-c": (high, y - 1, 1 - core, x, low),
        }[name]
        return self.row_of(*at[:3]), self.col_of(*at[3:])

    def greet(self, names):
        barrier = pltpu.get_barrier_semaphore()
        for name in names:
            pl.semaphore_signal(barrier, inc=1, device_id=self.peer(name), device_id_type=MESH)
        pl.semaphore_wait(barrier, len(names))

    def copy(self, src, dst, arriving, name):
        k = self.count
        self.count += 1
        make = lambda target: pltpu.make_async_remote_copy(
            src, target, self.send.at[k], self.recv.at[k], device_id=self.peer(name), device_id_type=MESH
        )
        out, arrival = make(dst), make(arriving)
        out.start()
        self.finish.append(out)
        rate, delay = (600e3, 1.0) if name == "c" else (46e3, 2.0)
        begin = max(self.now, self.free.get(name[:2], 0.0))
        self.free[name[:2]] = begin + math.prod(arriving.shape) * arriving.dtype.itemsize / rate
        return arrival, self.free[name[:2]] + delay

    def when(self, pending, action=None):
        arrival, time = pending

        def run():
            arrival.wait_recv()
            if action is not None:
                action()

        heapq.heappush(self.queue, (time, self.serial, run))
        self.serial += 1

    def work(self, time, action):
        self.spare.append((time, action))

    def spend(self, time):
        self.now += time

    def run(self):
        while self.queue or self.spare:
            if self.spare and (not self.queue or self.queue[0][0] > self.now + 0.5 * self.spare[0][0]):
                time, action = self.spare.pop(0)
                action()
                self.now += time
                continue
            time, _, action = heapq.heappop(self.queue)
            self.now = max(self.now, time) + 0.02
            action()
        for out in self.finish:
            out.wait_send()


def rows_of(ref, start, size, step=16):
    return ref.at[pl.ds(pl.multiple_of(start, step), size)]


def spread(net, src, out):
    size = src.shape[0]
    a, half_a, half_b = SPLIT, SPLIT // 2, (size - SPLIT) // 2
    b = size - a
    x, low = net.x, net.low

    def part(dx, other, start, rows):
        plane = 1 - low if other else low
        return rows_of(out, net.col_of(x + dx, plane) * size + start, rows)

    def own(start, rows):
        return src.at[pl.ds(start, rows)]

    def from_a(side):
        step = 1 if side == "x-" else -1
        at = -step
        forward = "x+" if step > 0 else "x-"
        start = 0 if step > 0 else half_a
        got = part(at, 0, start, half_a)
        far = net.copy(got, got, part(at - step, 0, start, half_a), forward)
        net.when(far, lambda: to_z(part(2, 0, start, half_a), part(2, 1, start, half_a)))
        to_z(part(at, 0, 0, a), part(at, 1, 0, a))

    def to_z(got, arriving):
        net.when(net.copy(got, got, arriving, "z"))

    def from_b(side, other):
        step = 1 if side == "x-" else -1
        start = a if step > 0 else a + half_b
        got = part(-step, other, start, half_b)
        forward = "x+" if step > 0 else "x-"
        net.when(net.copy(got, got, part(-2 * step, other, start, half_b), forward))

    def from_z():
        got = part(0, 1, a, b)
        for side, forward in (("x-", "x+"), ("x+", "x-")):
            dx = -1 if side == "x-" else 1
            arrival = net.copy(got, got, part(dx, 1, a, b), forward)
            net.when(arrival, lambda side=side: from_b(side, 1))

    arrival = net.copy(own(a, b), part(0, 0, a, b), part(0, 1, a, b), "z")
    net.when(arrival, from_z)
    for side, forward in (("x-", "x+"), ("x+", "x-")):
        dx = -1 if side == "x-" else 1
        arrival = net.copy(own(0, a), part(0, 0, 0, a), part(dx, 0, 0, a), forward)
        net.when(arrival, lambda side=side: from_a(side))
    for side, forward in (("x-", "x+"), ("x+", "x-")):
        dx = -1 if side == "x-" else 1
        arrival = net.copy(own(a, b), part(0, 0, a, b), part(dx, 0, a, b), forward)
        net.when(arrival, lambda side=side: from_b(side, 0))
    to_z_own = net.copy(own(0, a), part(0, 0, 0, a), part(0, 1, 0, a), "z")
    net.when(to_z_own)
    out[pl.ds(pl.multiple_of(net.col * size, size), size), :] = src[...]


def spread_small(net, src, out):
    size = src.shape[0]
    x, low = net.x, net.low

    def part(dx, other):
        plane = 1 - low if other else low
        return rows_of(out, net.col_of(x + dx, plane) * size, size, 8)

    def onward(other):
        got = part(-1, other)
        net.when(net.copy(got, got, part(-2, other), "x+"))

    def around(other, got):
        arrival = net.copy(got, part(0, other), part(-1, other), "x+")
        net.when(arrival, lambda: onward(other))
        net.when(net.copy(got, part(0, other), part(1, other), "x-"))

    around(0, src)
    arrival = net.copy(src, part(0, 0), part(0, 1), "z")
    net.when(arrival, lambda: around(1, part(0, 1)))
    out[pl.ds(pl.multiple_of(net.col * size, size), size), :] = src[...]


def gather(net, src, out, relay, axis):
    depth, width = src.shape
    high, y, core = net.high, net.y, net.core
    middle = depth // 2

    def part(dy, other, core, half=None):
        index = net.row_of(1 - high if other else high, y + dy, core)
        start, size = (0, depth) if half is None else (half * middle, middle)
        if axis == 0:
            return rows_of(out, index * depth + start, size)
        return out.at[pl.ds(start, size), pl.ds(pl.multiple_of(index * width, width), width)]

    def to_core(dy, other, half=None):
        got = part(dy, other, core, half)
        net.when(net.copy(got, got, part(dy, other, 1 - core, half), "c"))

    def from_y(dy, other):
        got = part(dy, other, core, 0 if dy < 0 else 1)
        forward = "y+" if dy < 0 else "y-"
        half = 0 if dy < 0 else 1
        arrival = net.copy(got, got, part(2, other, core, half), forward)
        net.when(arrival, lambda: to_core(2, other, half))
        to_core(dy, other)

    def around(other, got):
        for dy, forward in ((-1, "y+"), (1, "y-")):
            arrival = net.copy(got, part(0, other, core), part(dy, other, core), forward)
            net.when(arrival, lambda dy=dy: from_y(dy, other))

    around(0, src)
    waiting = [2]

    def arrived():
        waiting[0] -= 1
        if waiting[0] == 0:
            around(1, part(0, 1, core))
            to_core(0, 1)

    for half, first, second in ((0, "z", "w"), (1, "w", "z")):
        arrival = net.copy(src.at[pl.ds(half * middle, middle)], relay.at[half], relay.at[half], first)

        def onward(half=half, second=second):
            got = relay.at[half]
            arrival = net.copy(got, part(0, half, core, half), part(0, 1, core, half), second)
            net.when(arrival, arrived)

        net.when(arrival, onward)
    mine = part(0, 0, core)
    net.when(net.copy(src, mine, part(0, 0, 1 - core), "c"))
    index = net.row
    if axis == 0:
        out[pl.ds(pl.multiple_of(index * depth, depth), depth), :] = src[...]
    else:
        out[:, pl.ds(pl.multiple_of(index * width, width), width)] = src[...]


def reduce_scatter(net, fill, src, scratch, finish):
    from_z, sums, far_a, near_a, acc_a, far_b, near_b, acc_b, plane, last = scratch
    size = src.shape[0] // 8
    a = SPLIT
    b = size - a
    x, low = net.x, net.low

    def rows(dx, other, start, count):
        index = net.col_of(x + dx, 1 - low if other else low)
        return pl.ds(pl.multiple_of(index * size + start, 16), count)

    def ring(block, count, far, near, acc, done):
        half = count // 2
        halves = {"x+": (0, half), "x-": (half, half)}
        waiting = [4]

        def arrived():
            waiting[0] -= 1
            if waiting[0] == 0:
                done()

        def start_far():
            for index, forward in ((0, "x+"), (1, "x-")):
                first = halves[forward][0]
                arrival = net.copy(block(2, first, half), far.at[index], far.at[index], forward)

                def add(index=index, forward=forward, first=first):
                    term = block(1 if forward == "x+" else -1, first, half)
                    acc[index] = far[index] + term[...]
                    net.spend(0.1)
                    dst = near.at[index, pl.ds(first, half)]
                    net.when(net.copy(acc.at[index], dst, dst, forward), arrived)

                net.when(arrival, add)

        def start_direct():
            for index, forward in ((0, "x+"), (1, "x-")):
                first = half - halves[forward][0]
                dst = near.at[index, pl.ds(first, half)]
                term = block(1 if forward == "x+" else -1, first, half)
                net.when(net.copy(term, dst, dst, forward), arrived)

        return start_far, start_direct

    def block_b(other):
        return lambda dx, first, count: src.at[rows(dx, other, a + first, count)]

    def block_a(dx, first, count):
        return sums.at[pl.ds((dx % 4) * a + first, count)]

    left = [4]
    both = [3]
    wide = lambda value: value.astype(jnp.float32)

    def from_partner(k):
        sums[pl.ds(k * a, a), :] = from_z[pl.ds(k * a, a), :] + src[rows(k, 0, 0, a), :]
        net.spend(0.1)
        left[0] -= 1
        if left[0] == 0:
            for start in ring(block_a, a, far_a, near_a, acc_a, arrived):
                start()

    def to_partner(k):
        landing = from_z.at[pl.ds(k * a, a)]
        net.when(net.copy(src.at[rows(k, 1, 0, a)], landing, landing, "z"), lambda: from_partner(k))

    def plane_done():
        total = wide(near_b[0, 0]) + wide(near_b[0, 1]) + wide(src[rows(0, 1, a, b), :])
        plane[...] = total.astype(plane.dtype)
        net.spend(0.3)
        net.when(net.copy(plane, last, last, "z"), arrived)

    def arrived():
        both[0] -= 1
        if both[0]:
            return
        first = wide(near_a[0]) + wide(near_a[1]) + wide(sums[pl.ds(0, a), :])
        second = wide(near_b[1, 0]) + wide(near_b[1, 1]) + wide(src[rows(0, 0, a, b), :]) + wide(last[...])
        net.spend(0.5)
        finish(first, second)

    far_other, direct_other = ring(block_b(1), b, far_b.at[0], near_b.at[0], acc_b.at[0], plane_done)
    far_own, direct_own = ring(block_b(0), b, far_b.at[1], near_b.at[1], acc_b.at[1], arrived)
    fill(lambda i: net.col_of(x + 2, lax.rem(low + 1 + i, 2)))
    far_other()
    far_own()
    to_partner(2)
    fill(lambda i: net.col_of(x + 1 - 2 * i, 1 - low))
    direct_other()
    to_partner(1)
    to_partner(3)
    fill(lambda i: net.col_of(x + 1 - 2 * i, low))
    direct_own()
    fill(lambda i: net.col_of(x, lax.rem(low + 1 + i, 2)))
    to_partner(0)


def scatter_scratch(size, width, dtype):
    a = SPLIT
    b = size - a
    shapes = [(4 * a, width), (4 * a, width), (2, a // 2, width), (2, a, width), (2, a // 2, width)]
    shapes += [(2, 2, b // 2, width), (2, 2, b, width), (2, 2, b // 2, width), (b, width), (b, width)]
    return [pltpu.VMEM(shape, dtype) for shape in shapes]


def comm_body(spreads, smalls, gathers, *refs):
    count = spreads + smalls + len(gathers)
    ins, outs, relays = refs[:count], refs[count : 2 * count], refs[2 * count : -2]
    net = Net(*refs[-2:])
    net.greet(["x+", "x-", "z", "y+", "y-", "w", "c"])
    for k in range(spreads):
        spread(net, ins[k], outs[k])
    for k in range(spreads, spreads + smalls):
        spread_small(net, ins[k], outs[k])
    for i, axis in enumerate(gathers):
        k = spreads + smalls + i
        gather(net, ins[k], outs[k], relays[i], axis)
    net.run()


def communicate(name, body, collective_id, arrays, shapes, scratch, copies):
    return pl.pallas_call(
        body,
        out_shape=shapes,
        in_specs=[pl.BlockSpec(memory_space=pltpu.VMEM)] * len(arrays),
        out_specs=[pl.BlockSpec(memory_space=pltpu.VMEM)] * len(shapes),
        scratch_shapes=scratch + [pltpu.SemaphoreType.DMA((copies,)), pltpu.SemaphoreType.DMA((copies,))],
        compiler_params=pltpu.CompilerParams(
            collective_id=collective_id, has_side_effects=True, vmem_limit_bytes=56 * 2**20
        ),
        name=name,
    )(*arrays)


def gathered(array, axis):
    depth, width = array.shape
    total = lax.axis_size("row")
    shape = (depth * total, width) if axis == 0 else (depth, width * total)
    return jax.ShapeDtypeStruct(shape, array.dtype)


def relay_of(array):
    return pltpu.VMEM((2, array.shape[0] // 2, array.shape[1]), array.dtype)


def exchange(name, collective_id, spreads=(), smalls=(), gathers=()):
    whole = [jax.ShapeDtypeStruct((8 * a.shape[0], a.shape[1]), a.dtype) for a in (*spreads, *smalls)]
    return communicate(
        name,
        functools.partial(comm_body, len(spreads), len(smalls), [axis for _, axis in gathers]),
        collective_id,
        [*spreads, *smalls, *(array for array, _ in gathers)],
        whole + [gathered(*pair) for pair in gathers],
        [relay_of(array) for array, _ in gathers],
        20 * len(spreads) + 8 * len(smalls) + 22 * len(gathers),
    )


def middle_body(heads, qkv, weight, tokens, gain, up, down, hidden, normed_image, up_whole, down_whole, terms, mixed, normed, up_relay, down_relay, *rest):
    net = Net(*rest[-2:])
    net.greet(["x+", "x-", "z", "y+", "y-", "w", "c"])
    size = tokens.shape[0]
    dim = qkv.shape[1] // (3 * heads)

    def fill(column):
        @pl.loop(0, 2)
        def _(i):
            at = pl.ds(pl.multiple_of(column(i) * size, size), size)

            @pl.loop(0, heads)
            def _(h):
                part = lambda k: pl.ds(pl.multiple_of((3 * h + k) * dim, dim), dim)
                scores = lax.dot_general(
                    qkv[at, part(0)], qkv[:, part(1)], (((1,), (1,)), ((), ())), preferred_element_type=jnp.float32
                )
                scores = scores * (dim ** (-0.5))
                weights = jnp.exp(scores - jnp.max(scores, axis=-1, keepdims=True))
                chances = (weights / jnp.sum(weights, axis=-1, keepdims=True)).astype(jnp.bfloat16)
                mixed[:, pl.ds(pl.multiple_of(h * dim, dim), dim)] = matmul(chances, qkv[:, part(2)]).astype(jnp.bfloat16)

            @pl.loop(0, weight.shape[1] // 512)
            def _(j):
                columns = pl.ds(pl.multiple_of(j * 512, 512), 512)
                terms[at, columns] = matmul(mixed[...], weight[:, columns]).astype(jnp.bfloat16)

        net.spend(2.6)

    def finish(first, second):
        for start, total in ((0, first), (SPLIT, second)):
            at = pl.ds(start, total.shape[0])
            state = (tokens[at, :].astype(jnp.float32) + total).astype(jnp.bfloat16)
            hidden[at, :] = state
            normed[at, :] = layer_norm(state, gain[...]).astype(jnp.bfloat16)
        net.spend(0.5)
        spread(net, normed, normed_image)

    gather(net, up, up_whole, up_relay, 0)
    gather(net, down, down_whole, down_relay, 1)
    reduce_scatter(net, fill, terms, rest[:-2], finish)
    net.run()


def middle(collective_id, heads, qkv, weight, tokens, gain, up, down):
    size, width = tokens.shape
    image = jax.ShapeDtypeStruct((8 * size, width), tokens.dtype)
    scratch = [
        pltpu.VMEM(image.shape, image.dtype),
        pltpu.VMEM((size, weight.shape[0]), image.dtype),
        pltpu.VMEM(tokens.shape, image.dtype),
        relay_of(up),
        relay_of(down),
    ]
    return communicate(
        "middle",
        functools.partial(middle_body, heads),
        collective_id,
        (qkv, weight, tokens, gain, up, down),
        [jax.ShapeDtypeStruct(tokens.shape, tokens.dtype), image, gathered(up, 0), gathered(down, 1)],
        scratch + scatter_scratch(size, width, tokens.dtype),
        24 + 20 + 2 * 22,
    )


def leave_body(dense, picking, returned, hidden, out, terms, *rest):
    net = Net(*rest[-2:])
    net.greet(["x+", "x-", "z"])
    size = hidden.shape[0]

    def fill(column):
        @pl.loop(0, 2)
        def _(i):
            at = pl.ds(pl.multiple_of(column(i) * size, size), size)

            @pl.loop(0, dense.shape[1] // 512)
            def _(j):
                columns = pl.ds(pl.multiple_of(j * 512, 512), 512)
                total = dense[at, columns].astype(jnp.float32) + matmul(picking[at, :], returned[:, columns])
                terms[at, columns] = total.astype(jnp.bfloat16)

        net.spend(0.8)

    def finish(first, second):
        for start, total in ((0, first), (SPLIT, second)):
            at = pl.ds(start, total.shape[0])
            out[at, :] = (hidden[at, :].astype(jnp.float32) + total).astype(jnp.bfloat16)

    reduce_scatter(net, fill, terms, rest[:-2], finish)
    net.run()


def leave(collective_id, dense, picking, returned, hidden):
    return communicate(
        "leave",
        leave_body,
        collective_id,
        (dense, picking, returned, hidden),
        [jax.ShapeDtypeStruct(hidden.shape, hidden.dtype)],
        [pltpu.VMEM(dense.shape, dense.dtype)] + scatter_scratch(*hidden.shape, hidden.dtype),
        24,
    )


def y_exchange(net, src, dst, relay, ready=None, arrived=None, then=None):
    core = net.core
    half = src.shape[2] // 2
    tell = arrived or (lambda d: None)
    forwarded = [2]

    def opposite():
        for index, forward in ((0, "y+"), (1, "y-")):
            rows = pl.ds(index * half, half)
            arrival = net.copy(src.at[2, :, rows], relay.at[index], relay.at[index], forward)

            def onward(index=index, forward=forward, rows=rows):
                for c, name in ((core, forward), (1 - core, forward + "c")):
                    arrival = net.copy(relay.at[index, c], dst.at[2, core, rows], dst.at[2, c, rows], name)
                    net.when(arrival, lambda: tell(2))
                forwarded[0] -= 1
                if then is not None and forwarded[0] == 0:
                    then()

            net.when(arrival, onward)

    def beside(d):
        forward = "y+" if d == 1 else "y-"
        for c, name in ((core, forward), (1 - core, forward + "c")):
            arrival = net.copy(src.at[d, c], dst.at[4 - d, core], dst.at[4 - d, c], name)
            net.when(arrival, lambda: tell(4 - d))

    def here():
        net.when(net.copy(src.at[0, 1 - core], dst.at[0, core], dst.at[0, 1 - core], "c"), lambda: tell(0))
        dst[0, core] = src[0, core]

    steps = {2: opposite, 1: lambda: beside(1), 3: lambda: beside(3), 0: here}
    if ready is None:
        for d in (2, 1, 3, 0):
            steps[d]()
    else:
        ready(steps)


def dispatch_body(x_ref, w_ref, table, hidden, out, far, relay, send, recv):
    net = Net(send, recv)
    net.greet(["y+", "y-", "y+c", "y-c", "c", "z", "w"])
    low = net.low
    half = table.shape[3] // 2
    mine, theirs = pl.ds(pl.multiple_of(low * half, half), half), pl.ds(pl.multiple_of((1 - low) * half, half), half)

    def ready(steps):
        for d in (2, 1, 3, 0):
            arrival = net.copy(table.at[1, d, :, mine], far.at[d, :, mine], far.at[d, :, theirs], "w")

            def onward(d=d):
                arrival = net.copy(far.at[d, :, theirs], far.at[d, :, theirs], far.at[d, :, mine], "z")
                net.when(arrival, steps[d])

            net.when(arrival, onward)

    y_exchange(net, table.at[0], out.at[0], relay.at[0])
    y_exchange(net, far, out.at[1], relay.at[1], ready)
    up_tasks(net, x_ref, w_ref, hidden)
    net.run()


def up_tasks(net, x_ref, w_ref, out):
    rows, width = out.shape
    tile = min(256, rows)
    span = min(256, width)

    def piece(j):
        columns = pl.ds(j * span, span)

        @pl.loop(0, rows // tile)
        def _(i):
            at = pl.ds(pl.multiple_of(i * tile, tile), tile)
            inner = jnp.dot(x_ref[at, :], w_ref[:, columns], preferred_element_type=jnp.float32)
            out[at, columns] = (inner * (1.0 + lax.erf(inner * (0.5**0.5))) * 0.5).astype(out.dtype)

    for j in range(width // span):
        net.work(1.2, lambda j=j: piece(j))


def down_tasks(net, x_ref, w_ref, out):
    rows, width = out.shape
    tile = min(256, rows)
    span = min(512, width)

    def piece(j):
        columns = pl.ds(j * span, span)

        @pl.loop(0, rows // tile)
        def _(i):
            at = pl.ds(pl.multiple_of(i * tile, tile), tile)
            product = jnp.dot(x_ref[at, :], w_ref[:, columns], preferred_element_type=jnp.float32)
            out[at, columns] = product.astype(out.dtype)

    for j in range(width // span):
        net.work(1.2, lambda j=j: piece(j))


def collect_body(x_ref, w_ref, parts, dense, near, across, far, other, total, relay, send, recv):
    net = Net(send, recv)
    net.greet(["y+", "y-", "y+c", "y-c", "c", "z", "w"])
    low = net.low
    half = parts.shape[3] // 2
    mine, theirs = pl.ds(pl.multiple_of(low * half, half), half), pl.ds(pl.multiple_of((1 - low) * half, half), half)
    left = {0: 1, 1: 2, 2: 4, 3: 2}

    def arrived(d):
        left[d] -= 1
        if left[d]:
            return

        def add():
            total[d] = far[d, :, theirs] + other[d]
            net.spend(0.2)
            net.when(net.copy(total.at[d], across.at[d], across.at[d], "w"))

        net.when(net.copy(far.at[d, :, mine], other.at[d], other.at[d], "z"), add)

    second = lambda: y_exchange(net, parts.at[0], near, relay.at[0])
    y_exchange(net, parts.at[1], far, relay.at[1], None, arrived, second)
    down_tasks(net, x_ref, w_ref, dense)
    net.run()


def expert_call(name, body, collective_id, arrays, shapes, scratch):
    shapes = [jax.ShapeDtypeStruct(shape, jnp.bfloat16) for shape in shapes]
    return communicate(name, body, collective_id, arrays, shapes, [pltpu.VMEM(shape, jnp.bfloat16) for shape in scratch], 40)


def up_body(x_ref, w_ref, o_ref):
    inner = jnp.dot(x_ref[...], w_ref[...], preferred_element_type=jnp.float32)
    o_ref[...] = (inner * (1.0 + lax.erf(inner * (0.5**0.5))) * 0.5).astype(o_ref.dtype)


def up_gelu(x, w):
    rows, depth = x.shape
    width = w.shape[1]
    tile = min(width, 256)
    return pl.pallas_call(
        up_body,
        grid=(width // tile,),
        out_shape=jax.ShapeDtypeStruct((rows, width), jnp.bfloat16),
        in_specs=[
            pl.BlockSpec((rows, depth), lambda j: (0, 0)),
            pl.BlockSpec((depth, tile), lambda j: (0, j)),
        ],
        out_specs=pl.BlockSpec((rows, tile), lambda j: (0, j)),
        compiler_params=pltpu.CompilerParams(vmem_limit_bytes=32 * 2**20),
        cost_estimate=pl.CostEstimate(
            flops=2 * rows * depth * width,
            bytes_accessed=2 * (rows * depth + depth * width + rows * width),
            transcendentals=0,
        ),
        name="up_gelu",
    )(x, w)


def layer_norm(row_data, gain_vector):
    row_data = row_data.astype(jnp.float32)
    centered = row_data - jnp.mean(row_data, axis=-1, keepdims=True)
    spread = jnp.mean(centered * centered, axis=-1, keepdims=True)
    return centered * lax.rsqrt(spread + 1e-06) * gain_vector


def matmul(a, b):
    return jnp.dot(a, b, preferred_element_type=jnp.float32)


def shards(
    tokens,
    ln1_gain,
    qkv_weight,
    out_weight,
    ln2_gain,
    ffn_in,
    ffn_out,
    expert_ids,
    expert_in,
    expert_out,
):
    tok_count, model_width = tokens.shape
    row_total = lax.axis_size("row")
    col_total = lax.axis_size("col")
    row_index = lax.axis_index("row")
    col_index = lax.axis_index("col")
    expert_count = row_total * col_total // 2
    capacity = max(2, 2 * tok_count // expert_count)
    head_count, head_dim = qkv_weight.shape[1], qkv_weight.shape[3]
    seq_len = tok_count * col_total

    ids_block = jnp.broadcast_to(expert_ids[:, 0][None, :], (8, tok_count))
    image_rows, ids_all, qkv_whole, out_whole = exchange(
        "enter",
        0,
        spreads=(tokens,),
        smalls=(ids_block,),
        gathers=((qkv_weight.reshape(qkv_weight.shape[0], -1), 0), (out_weight, 1)),
    )
    normed = layer_norm(image_rows, ln1_gain).astype(jnp.bfloat16)
    projected = matmul(normed, qkv_whole).astype(jnp.bfloat16)
    hidden_mine, normed_image, up_whole, down_whole = middle(
        1, head_count, projected, out_whole, tokens, ln2_gain[None, :], ffn_in, ffn_out
    )

    ids_rows = ids_all.reshape(col_total, 8, tok_count)[:, 0]
    expert_range = jnp.arange(expert_count, dtype=jnp.int32)
    one_hot = (ids_rows[:, :, None] == expert_range).astype(jnp.int32)
    earlier = jnp.cumsum(one_hot, axis=1) - one_hot
    slot_index = jnp.sum(earlier * one_hot, axis=2)
    block_index = jnp.arange(col_total, dtype=jnp.int32)[:, None]
    home_row = 2 * ids_rows // col_total
    mine = (2 * ids_rows % col_total) // 2 == col_index // 2
    other = (home_row // 8 != row_index // 8).astype(jnp.int32)
    step = (home_row // 2 - row_index // 2 + 8) % 4
    chunk = step * 2 + home_row % 2
    place = block_index * capacity + slot_index
    rows = col_total * capacity
    position = jnp.where(mine, (other * 8 + chunk) * rows + place, -1).reshape(seq_len)
    slot_count = row_total * rows
    slots = jnp.arange(slot_count, dtype=jnp.int32)
    placing = (slots[:, None] == position[None, :]).astype(jnp.bfloat16)
    half = rows // 2
    crossed = jnp.where(place // half == col_index % 2, 8 * rows + chunk * half + place % half, -1)
    source = jnp.where(mine, jnp.where(other == 1, crossed, chunk * rows + place), -1).reshape(seq_len)
    returned_slots = jnp.arange(8 * (rows + half), dtype=jnp.int32)
    picking = (source[:, None] == returned_slots[None, :]).astype(jnp.bfloat16)

    table = matmul(placing, normed_image).astype(jnp.bfloat16)
    table = table.reshape(2, 4, 2, rows, model_width)
    full, part = (4, 2, rows, model_width), (4, 2, half, model_width)
    relays = (2, 2, 2, half, model_width)
    hidden_units, expert_rows = expert_call(
        "dispatch",
        dispatch_body,
        3,
        (normed_image, up_whole, table),
        ((seq_len, up_whole.shape[1]), table.shape),
        (full, relays),
    )
    expert_units = up_gelu(expert_rows.reshape(slot_count, model_width), expert_in[0])
    partial_out = matmul(expert_units, expert_out[0]).astype(jnp.bfloat16).reshape(table.shape)
    dense, near, across = expert_call(
        "collect",
        collect_body,
        4,
        (hidden_units, down_whole, partial_out),
        ((seq_len, model_width), full, part),
        (full, part, part, relays),
    )
    rows_two = jnp.concatenate((near.reshape(-1, model_width), across.reshape(-1, model_width)))
    (out,) = leave(5, dense, picking, rows_two, hidden_mine)
    return out


def solution(mesh):
    in_specs = (
        P(("row", "col"), None),
        P(),
        P("row", "col", None, None),
        P("col", "row"),
        P(),
        P("row", "col"),
        P("col", "row"),
        P(("row", "col"), None),
        P(("row", "col"), None, None),
        P(("row", "col"), None, None),
    )
    out_specs = P(("row", "col"), None)
    return jax.shard_map(shards, mesh=mesh, in_specs=in_specs, out_specs=out_specs, check_vma=False)
```

```python
import functools
import heapq
import math
import jax
import jax.numpy as jnp
from jax import lax
from jax.experimental import pallas as pl
from jax.experimental.pallas import tpu as pltpu
from jax.sharding import PartitionSpec as P

MESH = pl.DeviceIdType.MESH
SPLIT = 32


class Net:
    def __init__(self, send, recv):
        row, col = lax.axis_index("row"), lax.axis_index("col")
        self.row, self.col = row, col
        self.high, self.y, self.core = row // 8, lax.rem(row // 2, 4), lax.rem(row, 2)
        self.x, self.low = col // 2, lax.rem(col, 2)
        self.send, self.recv = send, recv
        self.count = 0
        self.finish = []
        self.queue = []
        self.serial = 0
        self.now = 0.0
        self.free = {}
        self.spare = []

    def row_of(self, high, y, core):
        return high * 8 + lax.rem(y + 8, 4) * 2 + core

    def col_of(self, x, low):
        return lax.rem(x + 8, 4) * 2 + low

    def block_of(self, x, low):
        return low * 4 + lax.rem(x + 8, 4)

    def peer(self, name):
        high, y, core, x, low = self.high, self.y, self.core, self.x, self.low
        at = {
            "x+": (high, y, core, x + 1, low),
            "x-": (high, y, core, x - 1, low),
            "z": (high, y, core, x, 1 - low),
            "y+": (high, y + 1, core, x, low),
            "y-": (high, y - 1, core, x, low),
            "w": (1 - high, y, core, x, 1 - low),
            "c": (high, y, 1 - core, x, low),
            "y+c": (high, y + 1, 1 - core, x, low),
            "y-c": (high, y - 1, 1 - core, x, low),
        }[name]
        return self.row_of(*at[:3]), self.col_of(*at[3:])

    def greet(self, names):
        barrier = pltpu.get_barrier_semaphore()
        for name in names:
            pl.semaphore_signal(barrier, inc=1, device_id=self.peer(name), device_id_type=MESH)
        pl.semaphore_wait(barrier, len(names))

    def copy(self, src, dst, arriving, name):
        k = self.count
        self.count += 1
        make = lambda target: pltpu.make_async_remote_copy(
            src, target, self.send.at[k], self.recv.at[k], device_id=self.peer(name), device_id_type=MESH
        )
        out, arrival = make(dst), make(arriving)
        out.start()
        self.finish.append(out)
        rate, delay = (600e3, 1.0) if name == "c" else (46e3, 2.0)
        begin = max(self.now, self.free.get(name[:2], 0.0))
        self.free[name[:2]] = begin + math.prod(arriving.shape) * arriving.dtype.itemsize / rate
        return arrival, self.free[name[:2]] + delay

    def when(self, pending, action=None):
        arrival, time = pending

        def run():
            arrival.wait_recv()
            if action is not None:
                action()

        heapq.heappush(self.queue, (time, self.serial, run))
        self.serial += 1

    def work(self, time, action):
        self.spare.append((time, action))

    def spend(self, time):
        self.now += time

    def run(self):
        while self.queue or self.spare:
            if self.spare and (not self.queue or self.queue[0][0] > self.now + 0.5 * self.spare[0][0]):
                time, action = self.spare.pop(0)
                action()
                self.now += time
                continue
            time, _, action = heapq.heappop(self.queue)
            self.now = max(self.now, time) + 0.02
            action()
        for out in self.finish:
            out.wait_send()


def rows_of(ref, start, size, step=16):
    return ref.at[pl.ds(pl.multiple_of(start, step), size)]


def counted(count, action):
    left = [count]

    def step():
        left[0] -= 1
        if left[0] == 0:
            action()

    return step


def spread(net, src, out, plane_done=lambda: None, done=lambda: None):
    size = src.shape[0]
    a, half_a, half_b = SPLIT, SPLIT // 2, (size - SPLIT) // 2
    b = size - a
    x, low = net.x, net.low
    mine = counted(8, plane_done)
    theirs = counted(12, done)
    sides = ((-1, "x+", 0), (1, "x-", 1))

    def part(dx, other, start, rows):
        plane = 1 - low if other else low
        return rows_of(out, net.block_of(x + dx, plane) * size + start, rows)

    def own(start, rows):
        return src.at[pl.ds(start, rows)]

    def to_z(dx, start, rows):
        got = part(dx, 0, start, rows)
        net.when(net.copy(got, got, part(dx, 1, start, rows), "z"), theirs)

    def onward(dx, forward, other, start, rows, then):
        got = part(dx, other, start, rows)
        net.when(net.copy(got, got, part(2, other, start, rows), forward), then)

    def from_a(dx, forward, index):
        mine()

        def far():
            mine()
            to_z(2, index * half_a, half_a)

        onward(dx, forward, 0, index * half_a, half_a, far)
        to_z(dx, 0, a)

    def from_b(dx, forward, index):
        mine()
        onward(dx, forward, 0, a + index * half_b, half_b, mine)
        later()

    def partner(index, half, then):
        dx, forward, _ = sides[index]
        got = part(0, 1, a + half * half_b, half_b)
        net.when(net.copy(got, got, part(dx, 1, a + half * half_b, half_b), forward), then)

    def from_z():
        theirs()
        for dx, forward, index in sides:

            def first(dx=dx, forward=forward, index=index):
                theirs()
                onward(dx, forward, 1, a + index * half_b, half_b, theirs)

            partner(index, index, first)
        later()

    def second():
        for _, _, index in sides:
            partner(index, 1 - index, theirs)

    later = counted(3, second)
    net.when(net.copy(own(a, b), part(0, 0, a, b), part(0, 1, a, b), "z"), from_z)
    for start, rows, action in ((0, a, from_a), (a, b, from_b)):
        for dx, forward, index in sides:
            arrival = net.copy(own(start, rows), part(0, 0, start, rows), part(dx, 0, start, rows), forward)
            net.when(arrival, functools.partial(action, dx, forward, index))
    net.when(net.copy(own(0, a), part(0, 0, 0, a), part(0, 1, 0, a), "z"), theirs)
    out[pl.ds(pl.multiple_of(net.block_of(x, low) * size, size), size), :] = src[...]


def spread_small(net, src, out):
    size = src.shape[0]
    x, low = net.x, net.low

    def part(dx, other):
        plane = 1 - low if other else low
        return rows_of(out, net.block_of(x + dx, plane) * size, size, 8)

    def onward(other):
        got = part(-1, other)
        net.when(net.copy(got, got, part(-2, other), "x+"))

    def around(other, got):
        arrival = net.copy(got, part(0, other), part(-1, other), "x+")
        net.when(arrival, lambda: onward(other))
        net.when(net.copy(got, part(0, other), part(1, other), "x-"))

    around(0, src)
    arrival = net.copy(src, part(0, 0), part(0, 1), "z")
    net.when(arrival, lambda: around(1, part(0, 1)))
    out[pl.ds(pl.multiple_of(net.block_of(x, net.low) * size, size), size), :] = src[...]


def gather(net, src, out, relay, axis, done=lambda: None):
    depth, width = src.shape
    high, y, core = net.high, net.y, net.core
    middle = depth // 2
    landed = counted(10, done)

    def part(dy, other, core, half=None):
        index = net.row_of(1 - high if other else high, y + dy, core)
        start, size = (0, depth) if half is None else (half * middle, middle)
        if axis == 0:
            return rows_of(out, index * depth + start, size)
        return out.at[pl.ds(start, size), pl.ds(pl.multiple_of(index * width, width), width)]

    def to_core(dy, other, half=None):
        got = part(dy, other, core, half)
        net.when(net.copy(got, got, part(dy, other, 1 - core, half), "c"), landed)

    def from_y(dy, other):
        got = part(dy, other, core, 0 if dy < 0 else 1)
        forward = "y+" if dy < 0 else "y-"
        half = 0 if dy < 0 else 1
        arrival = net.copy(got, got, part(2, other, core, half), forward)
        net.when(arrival, lambda: to_core(2, other, half))
        to_core(dy, other)

    def around(other, got):
        for dy, forward in ((-1, "y+"), (1, "y-")):
            arrival = net.copy(got, part(0, other, core), part(dy, other, core), forward)
            net.when(arrival, lambda dy=dy: from_y(dy, other))

    around(0, src)
    waiting = [2]

    def arrived():
        waiting[0] -= 1
        if waiting[0] == 0:
            around(1, part(0, 1, core))
            to_core(0, 1)

    for half, first, second in ((0, "z", "w"), (1, "w", "z")):
        arrival = net.copy(src.at[pl.ds(half * middle, middle)], relay.at[half], relay.at[half], first)

        def onward(half=half, second=second):
            got = relay.at[half]
            arrival = net.copy(got, part(0, half, core, half), part(0, 1, core, half), second)
            net.when(arrival, arrived)

        net.when(arrival, onward)
    mine = part(0, 0, core)
    net.when(net.copy(src, mine, part(0, 0, 1 - core), "c"), landed)
    index = net.row
    if axis == 0:
        out[pl.ds(pl.multiple_of(index * depth, depth), depth), :] = src[...]
    else:
        out[:, pl.ds(pl.multiple_of(index * width, width), width)] = src[...]


def reduce_scatter(net, fill, src, scratch, finish):
    from_z, sums, far_a, near_a, acc_a, far_b, near_b, acc_b, plane, last = scratch
    size = src.shape[0] // 8
    a = SPLIT
    b = size - a
    x, low = net.x, net.low

    def rows(dx, other, start, count):
        index = net.block_of(x + dx, 1 - low if other else low)
        return pl.ds(pl.multiple_of(index * size + start, 16), count)

    def ring(block, count, far, near, acc, done):
        half = count // 2
        halves = {"x+": (0, half), "x-": (half, half)}
        waiting = [4]

        def arrived():
            waiting[0] -= 1
            if waiting[0] == 0:
                done()

        def start_far():
            for index, forward in ((0, "x+"), (1, "x-")):
                first = halves[forward][0]
                arrival = net.copy(block(2, first, half), far.at[index], far.at[index], forward)

                def add(index=index, forward=forward, first=first):
                    term = block(1 if forward == "x+" else -1, first, half)
                    acc[index] = far[index] + term[...]
                    net.spend(0.1)
                    dst = near.at[index, pl.ds(first, half)]
                    net.when(net.copy(acc.at[index], dst, dst, forward), arrived)

                net.when(arrival, add)

        def start_direct():
            for index, forward in ((0, "x+"), (1, "x-")):
                first = half - halves[forward][0]
                dst = near.at[index, pl.ds(first, half)]
                term = block(1 if forward == "x+" else -1, first, half)
                net.when(net.copy(term, dst, dst, forward), arrived)

        return start_far, start_direct

    def block_b(other):
        return lambda dx, first, count: src.at[rows(dx, other, a + first, count)]

    def block_a(dx, first, count):
        return sums.at[pl.ds((dx % 4) * a + first, count)]

    left = [4]
    both = [3]
    wide = lambda value: value.astype(jnp.float32)

    def from_partner(k):
        sums[pl.ds(k * a, a), :] = from_z[pl.ds(k * a, a), :] + src[rows(k, 0, 0, a), :]
        net.spend(0.1)
        left[0] -= 1
        if left[0] == 0:
            for start in ring(block_a, a, far_a, near_a, acc_a, arrived):
                start()

    def to_partner(k):
        landing = from_z.at[pl.ds(k * a, a)]
        net.when(net.copy(src.at[rows(k, 1, 0, a)], landing, landing, "z"), lambda: from_partner(k))

    def plane_done():
        total = wide(near_b[0, 0]) + wide(near_b[0, 1]) + wide(src[rows(0, 1, a, b), :])
        plane[...] = total.astype(plane.dtype)
        net.spend(0.3)
        net.when(net.copy(plane, last, last, "z"), arrived)

    def arrived():
        both[0] -= 1
        if both[0]:
            return
        first = wide(near_a[0]) + wide(near_a[1]) + wide(sums[pl.ds(0, a), :])
        second = wide(near_b[1, 0]) + wide(near_b[1, 1]) + wide(src[rows(0, 0, a, b), :]) + wide(last[...])
        net.spend(0.5)
        finish(first, second)

    far_other, direct_other = ring(block_b(1), b, far_b.at[0], near_b.at[0], acc_b.at[0], plane_done)
    far_own, direct_own = ring(block_b(0), b, far_b.at[1], near_b.at[1], acc_b.at[1], arrived)
    fill(lambda i: net.block_of(x + 2, lax.rem(low + 1 + i, 2)))
    far_other()
    far_own()
    to_partner(2)
    fill(lambda i: net.block_of(x + 1 - 2 * i, 1 - low))
    direct_other()
    to_partner(1)
    to_partner(3)
    fill(lambda i: net.block_of(x + 1 - 2 * i, low))
    direct_own()
    fill(lambda i: net.block_of(x, lax.rem(low + 1 + i, 2)))
    to_partner(0)


def scatter_scratch(size, width, dtype):
    a = SPLIT
    b = size - a
    shapes = [(4 * a, width), (4 * a, width), (2, a // 2, width), (2, a, width), (2, a // 2, width)]
    shapes += [(2, 2, b // 2, width), (2, 2, b, width), (2, 2, b // 2, width), (b, width), (b, width)]
    return [pltpu.VMEM(shape, dtype) for shape in shapes]


def comm_body(spreads, smalls, gathers, *refs):
    count = spreads + smalls + len(gathers)
    ins, outs, relays = refs[:count], refs[count : 2 * count], refs[2 * count : -2]
    net = Net(*refs[-2:])
    net.greet(["x+", "x-", "z", "y+", "y-", "w", "c"])
    for k in range(spreads):
        spread(net, ins[k], outs[k])
    for k in range(spreads, spreads + smalls):
        spread_small(net, ins[k], outs[k])
    for i, axis in enumerate(gathers):
        k = spreads + smalls + i
        gather(net, ins[k], outs[k], relays[i], axis)
    net.run()


def communicate(name, body, collective_id, arrays, shapes, scratch, copies):
    used = sum(math.prod(ref.shape) * jnp.dtype(ref.dtype).itemsize for ref in scratch)
    return pl.pallas_call(
        body,
        out_shape=shapes,
        in_specs=[pl.BlockSpec(memory_space=pltpu.VMEM)] * len(arrays),
        out_specs=[pl.BlockSpec(memory_space=pltpu.VMEM)] * len(shapes),
        scratch_shapes=scratch + [pltpu.SemaphoreType.DMA((copies,)), pltpu.SemaphoreType.DMA((copies,))],
        compiler_params=pltpu.CompilerParams(
            collective_id=collective_id, has_side_effects=True, vmem_limit_bytes=used + 6 * 2**20
        ),
        name=name,
    )(*arrays)


def gathered(array, axis):
    depth, width = array.shape
    total = lax.axis_size("row")
    shape = (depth * total, width) if axis == 0 else (depth, width * total)
    return jax.ShapeDtypeStruct(shape, array.dtype)


def relay_of(array):
    return pltpu.VMEM((2, array.shape[0] // 2, array.shape[1]), array.dtype)


def exchange(name, collective_id, spreads=(), smalls=(), gathers=()):
    whole = [jax.ShapeDtypeStruct((8 * a.shape[0], a.shape[1]), a.dtype) for a in (*spreads, *smalls)]
    return communicate(
        name,
        functools.partial(comm_body, len(spreads), len(smalls), [axis for _, axis in gathers]),
        collective_id,
        [*spreads, *smalls, *(array for array, _ in gathers)],
        whole + [gathered(*pair) for pair in gathers],
        [relay_of(array) for array, _ in gathers],
        22 * len(spreads) + 8 * len(smalls) + 22 * len(gathers),
    )


def middle_body(heads, qkv, weight, tokens, gain, up, down, position, hidden, down_whole, units, out, *rest):
    terms, mixed, normed, image, up_whole, table, far, y_relay, up_relay, down_relay = rest[:10]
    net = Net(*rest[-2:])
    net.greet(["x+", "x-", "z", "y+", "y-", "w", "c", "y+c", "y-c"])
    size = tokens.shape[0]
    dim = qkv.shape[1] // (3 * heads)
    low = net.low
    slots = out.shape[3] // 2
    mine = pl.ds(pl.multiple_of(low * slots, slots), slots)
    theirs = pl.ds(pl.multiple_of((1 - low) * slots, slots), slots)

    def fill(column):
        @pl.loop(0, 2)
        def _(i):
            at = pl.ds(pl.multiple_of(column(i) * size, size), size)

            @pl.loop(0, heads)
            def _(h):
                part = lambda k: pl.ds(pl.multiple_of((3 * h + k) * dim, dim), dim)
                scores = lax.dot_general(
                    qkv[at, part(0)], qkv[:, part(1)], (((1,), (1,)), ((), ())), preferred_element_type=jnp.float32
                )
                scores = scores * (dim ** (-0.5))
                weights = jnp.exp(scores - jnp.max(scores, axis=-1, keepdims=True))
                chances = (weights / jnp.sum(weights, axis=-1, keepdims=True)).astype(jnp.bfloat16)
                mixed[:, pl.ds(pl.multiple_of(h * dim, dim), dim)] = matmul(chances, qkv[:, part(2)]).astype(jnp.bfloat16)

            @pl.loop(0, weight.shape[1] // 512)
            def _(j):
                columns = pl.ds(pl.multiple_of(j * 512, 512), 512)
                terms[at, columns] = matmul(mixed[...], weight[:, columns]).astype(jnp.bfloat16)

        net.spend(2.6)

    def place(index, plane):
        rows = pl.ds(pl.multiple_of(plane * 4 * size, 4 * size), 4 * size)
        flat = math.prod(table.shape[1:5])
        here = lax.broadcasted_iota(jnp.int32, (flat, 4 * size), 0) == position[pl.ds(0, 1), rows]
        placing = jnp.where(here, 1.0, 0.0).astype(jnp.bfloat16)
        span = 512

        @pl.loop(0, image.shape[1] // span)
        def _(j):
            columns = pl.ds(pl.multiple_of(j * span, span), span)
            put = matmul(placing, image[rows, columns]).astype(jnp.bfloat16)
            table[index, :, :, :, :, columns] = put.reshape(table.shape[1:5] + (span,))

        net.spend(1.2)

    def plane_done():
        place(0, low)

        def from_w(d):
            got = far.at[d, :, theirs]
            arrival = net.copy(got, got, far.at[d, :, mine], "z")
            net.when(arrival, last[d])
            first[d]()

        for d in (2, 1, 3, 0):
            arrival = net.copy(table.at[0, 1, d], far.at[d, :, mine], far.at[d, :, theirs], "w")
            net.when(arrival, functools.partial(from_w, d))
        start_all(own)
        ready()

    def image_done():
        place(1, 1 - low)
        start_all(other)
        ready()

    own = y_exchange(net, chunks(table.at[0, 0]), chunks(out.at[0], mine), y_relay.at[0])
    first = y_exchange(net, chunks(far, theirs), chunks(out.at[1], theirs), y_relay.at[1])
    last = y_exchange(net, chunks(far, mine), chunks(out.at[1], mine), y_relay.at[2])
    other = y_exchange(net, chunks(table.at[1, 0]), chunks(out.at[0], theirs), y_relay.at[3])
    ready = counted(3, lambda: up_tasks(net, image, up_whole, units))

    def finish(first_rows, second_rows):
        for start, total in ((0, first_rows), (SPLIT, second_rows)):
            at = pl.ds(start, total.shape[0])
            state = (tokens[at, :].astype(jnp.float32) + total).astype(jnp.bfloat16)
            hidden[at, :] = state
            normed[at, :] = layer_norm(state, gain[...]).astype(jnp.bfloat16)
        net.spend(0.5)
        spread(net, normed, image, plane_done, image_done)

    gather(net, up, up_whole, up_relay, 0, ready)
    gather(net, down, down_whole, down_relay, 1)
    reduce_scatter(net, fill, terms, rest[10:-2], finish)
    net.run()


def middle(collective_id, heads, qkv, weight, tokens, gain, up, down, position, slots):
    size, width = tokens.shape
    image = (8 * size, width)
    sixteen = lambda *shape: pltpu.VMEM(shape, tokens.dtype)
    scratch = [
        sixteen(*image),
        sixteen(size, weight.shape[0]),
        sixteen(size, width),
        sixteen(*image),
        sixteen(*gathered(up, 0).shape),
        sixteen(2, 2, 4, 2, slots // 2, width),
        sixteen(4, 2, slots, width),
        sixteen(4, 2, slots // 2, width),
        relay_of(up),
        relay_of(down),
    ]
    made = lambda *shape: jax.ShapeDtypeStruct(shape, tokens.dtype)
    return communicate(
        "middle",
        functools.partial(middle_body, heads),
        collective_id,
        (qkv, weight, tokens, gain, up, down, position),
        [made(size, width), gathered(down, 1), made(8 * size, up.shape[1]), made(2, 4, 2, slots, width)],
        scratch + scatter_scratch(size, width, tokens.dtype),
        24 + 22 + 2 * 22 + 8 + 4 * 10,
    )


def leave_body(dense, picking, near, across, hidden, out, terms, *rest):
    net = Net(*rest[-2:])
    net.greet(["x+", "x-", "z"])
    size = hidden.shape[0]
    count = near.shape[0]

    def fill(column):
        @pl.loop(0, 2)
        def _(i):
            at = pl.ds(pl.multiple_of(column(i) * size, size), size)

            @pl.loop(0, dense.shape[1] // 512)
            def _(j):
                columns = pl.ds(pl.multiple_of(j * 512, 512), 512)
                total = dense[at, columns].astype(jnp.float32)
                total += matmul(picking[at, pl.ds(0, count)], near[:, columns])
                total += matmul(picking[at, pl.ds(count, across.shape[0])], across[:, columns])
                terms[at, columns] = total.astype(jnp.bfloat16)

        net.spend(0.8)

    def finish(first, second):
        for start, total in ((0, first), (SPLIT, second)):
            at = pl.ds(start, total.shape[0])
            out[at, :] = (hidden[at, :].astype(jnp.float32) + total).astype(jnp.bfloat16)

    reduce_scatter(net, fill, terms, rest[:-2], finish)
    net.run()


def leave(collective_id, dense, picking, near, across, hidden):
    return communicate(
        "leave",
        leave_body,
        collective_id,
        (dense, picking, near, across, hidden),
        [jax.ShapeDtypeStruct(hidden.shape, hidden.dtype)],
        [pltpu.VMEM(dense.shape, dense.dtype)] + scatter_scratch(*hidden.shape, hidden.dtype),
        24,
    )


def y_exchange(net, src, dst, relay, arrived=lambda d: None, then=lambda: None):
    core = net.core
    forwarded = counted(2, then)

    def opposite():
        for index, c, forward, last in ((0, core, "y+", "y+"), (1, 1 - core, "y-", "y-c")):

            def onward(index=index, c=c, last=last):
                arrival = net.copy(relay.at[index], dst(2, core), dst(2, c), last)
                net.when(arrival, lambda: arrived(2))
                forwarded()

            net.when(net.copy(src(2, c), relay.at[index], relay.at[index], forward), onward)

    def beside(d):
        forward = "y+" if d == 1 else "y-"
        for c, name in ((core, forward), (1 - core, forward + "c")):
            net.when(net.copy(src(d, c), dst(4 - d, core), dst(4 - d, c), name), lambda: arrived(4 - d))

    def here():
        net.when(net.copy(src(0, 1 - core), dst(0, core), dst(0, 1 - core), "c"), lambda: arrived(0))
        dst(0, core)[...] = src(0, core)[...]

    return {2: opposite, 1: lambda: beside(1), 3: lambda: beside(3), 0: here}


def chunks(ref, *rest):
    return lambda d, c: ref.at[(d, c, *rest)]


def start_all(steps):
    for d in (2, 1, 3, 0):
        steps[d]()


def up_tasks(net, x_ref, w_ref, out):
    rows, width = out.shape
    tile = min(256, rows)
    span = min(256, width)

    def piece(j):
        columns = pl.ds(j * span, span)

        @pl.loop(0, rows // tile)
        def _(i):
            at = pl.ds(pl.multiple_of(i * tile, tile), tile)
            inner = jnp.dot(x_ref[at, :], w_ref[:, columns], preferred_element_type=jnp.float32)
            out[at, columns] = (inner * (1.0 + lax.erf(inner * (0.5**0.5))) * 0.5).astype(out.dtype)

    for j in range(width // span):
        net.work(1.6, lambda j=j: piece(j))


def down_tasks(net, x_ref, w_ref, out):
    rows, width = out.shape
    tile = min(256, rows)
    span = min(512, width)

    def piece(j):
        columns = pl.ds(j * span, span)

        @pl.loop(0, rows // tile)
        def _(i):
            at = pl.ds(pl.multiple_of(i * tile, tile), tile)
            product = jnp.dot(x_ref[at, :], w_ref[:, columns], preferred_element_type=jnp.float32)
            out[at, columns] = product.astype(out.dtype)

    for j in range(width // span):
        net.work(1.2, lambda j=j: piece(j))


def collect_body(x_ref, w_ref, parts, dense, near, across, far, other, total, relay, send, recv):
    net = Net(send, recv)
    net.greet(["y+", "y-", "y+c", "y-c", "c", "z", "w"])
    low = net.low
    half = parts.shape[3] // 2
    mine, theirs = pl.ds(pl.multiple_of(low * half, half), half), pl.ds(pl.multiple_of((1 - low) * half, half), half)

    def landed(d):
        def add():
            total[d] = far[d, :, theirs] + other[d]
            net.spend(0.2)
            net.when(net.copy(total.at[d], across.at[d], across.at[d], "w"))

        net.when(net.copy(far.at[d, :, mine], other.at[d], other.at[d], "z"), add)

    counts = {d: counted(1 if d == 0 else 2, functools.partial(landed, d)) for d in range(4)}
    second = y_exchange(net, chunks(parts.at[0]), chunks(near), relay.at[0])
    first = y_exchange(net, chunks(parts.at[1]), chunks(far), relay.at[1], lambda d: counts[d](), lambda: start_all(second))
    start_all(first)
    down_tasks(net, x_ref, w_ref, dense)
    net.run()


def expert_call(name, body, collective_id, arrays, shapes, scratch):
    shapes = [jax.ShapeDtypeStruct(shape, jnp.bfloat16) for shape in shapes]
    return communicate(name, body, collective_id, arrays, shapes, [pltpu.VMEM(shape, jnp.bfloat16) for shape in scratch], 40)


def up_body(x_ref, w_ref, o_ref):
    inner = jnp.dot(x_ref[...], w_ref[...], preferred_element_type=jnp.float32)
    o_ref[...] = (inner * (1.0 + lax.erf(inner * (0.5**0.5))) * 0.5).astype(o_ref.dtype)


def up_gelu(x, w):
    rows, depth = x.shape
    width = w.shape[1]
    tile = min(width, 256)
    return pl.pallas_call(
        up_body,
        grid=(width // tile,),
        out_shape=jax.ShapeDtypeStruct((rows, width), jnp.bfloat16),
        in_specs=[
            pl.BlockSpec((rows, depth), lambda j: (0, 0)),
            pl.BlockSpec((depth, tile), lambda j: (0, j)),
        ],
        out_specs=pl.BlockSpec((rows, tile), lambda j: (0, j)),
        compiler_params=pltpu.CompilerParams(vmem_limit_bytes=32 * 2**20),
        cost_estimate=pl.CostEstimate(
            flops=2 * rows * depth * width,
            bytes_accessed=2 * (rows * depth + depth * width + rows * width),
            transcendentals=0,
        ),
        name="up_gelu",
    )(x, w)


def layer_norm(row_data, gain_vector):
    row_data = row_data.astype(jnp.float32)
    centered = row_data - jnp.mean(row_data, axis=-1, keepdims=True)
    spread = jnp.mean(centered * centered, axis=-1, keepdims=True)
    return centered * lax.rsqrt(spread + 1e-06) * gain_vector


def matmul(a, b):
    return jnp.dot(a, b, preferred_element_type=jnp.float32)


def shards(
    tokens,
    ln1_gain,
    qkv_weight,
    out_weight,
    ln2_gain,
    ffn_in,
    ffn_out,
    expert_ids,
    expert_in,
    expert_out,
):
    tok_count, model_width = tokens.shape
    row_total = lax.axis_size("row")
    col_total = lax.axis_size("col")
    row_index = lax.axis_index("row")
    col_index = lax.axis_index("col")
    expert_count = row_total * col_total // 2
    capacity = max(2, 2 * tok_count // expert_count)
    head_count, head_dim = qkv_weight.shape[1], qkv_weight.shape[3]
    seq_len = tok_count * col_total

    ids = expert_ids[:, 0]
    token = jnp.arange(tok_count, dtype=jnp.int32)
    same = (expert_ids == ids[None, :]) & (token[:, None] < token[None, :])
    codes = ids * capacity + jnp.sum(same.astype(jnp.int32), axis=0)
    image_rows, codes_all, qkv_whole, out_whole = exchange(
        "enter",
        0,
        spreads=(tokens,),
        smalls=(jnp.broadcast_to(codes[None, :], (8, tok_count)),),
        gathers=((qkv_weight.reshape(qkv_weight.shape[0], -1), 0), (out_weight, 1)),
    )
    normed = layer_norm(image_rows, ln1_gain).astype(jnp.bfloat16)
    projected = matmul(normed, qkv_whole).astype(jnp.bfloat16)
    codes_all = codes_all.reshape(col_total, 8, tok_count)[:, 0]
    ids_rows, slot_index = codes_all // capacity, codes_all % capacity
    block = jnp.arange(col_total, dtype=jnp.int32)[:, None]
    plane, place = block // 4, block % 4 * capacity + slot_index
    home_row = 2 * ids_rows // col_total
    mine = (2 * ids_rows % col_total) // 2 == col_index // 2
    other = (home_row // 8 != row_index // 8).astype(jnp.int32)
    chunk = (home_row // 2 - row_index // 2 + 8) % 4 * 2 + home_row % 2
    half = 4 * capacity
    rows = 2 * half
    slot_count = row_total * rows
    position = jnp.where(mine, (other * 8 + chunk) * half + place, -1).reshape(1, seq_len)
    position = jnp.broadcast_to(position, (8, seq_len))
    crossed = jnp.where(plane == col_index % 2, (8 * rows) + chunk * half + place, -1)
    source = jnp.where(mine, jnp.where(other == 1, crossed, chunk * rows + plane * half + place), -1).reshape(seq_len)
    returned_slots = jnp.arange(8 * (rows + half), dtype=jnp.int32)
    picking = (source[:, None] == returned_slots[None, :]).astype(jnp.bfloat16)

    hidden_mine, down_whole, hidden_units, expert_rows = middle(
        1, head_count, projected, out_whole, tokens, ln2_gain[None, :], ffn_in, ffn_out, position, rows
    )
    full, part = (4, 2, rows, model_width), (4, 2, half, model_width)
    expert_units = up_gelu(expert_rows.reshape(slot_count, model_width), expert_in[0])
    partial_out = matmul(expert_units, expert_out[0]).astype(jnp.bfloat16).reshape(expert_rows.shape)
    dense, near, across = expert_call(
        "collect",
        collect_body,
        4,
        (hidden_units, down_whole, partial_out),
        ((seq_len, model_width), full, part),
        (full, part, part, (2, 2, rows, model_width)),
    )
    flat = lambda array: array.reshape(-1, model_width)
    (out,) = leave(5, dense, picking, flat(near), flat(across), hidden_mine)
    return out


def solution(mesh):
    in_specs = (
        P(("row", "col"), None),
        P(),
        P("row", "col", None, None),
        P("col", "row"),
        P(),
        P("row", "col"),
        P("col", "row"),
        P(("row", "col"), None),
        P(("row", "col"), None, None),
        P(("row", "col"), None, None),
    )
    out_specs = P(("row", "col"), None)
    return jax.shard_map(shards, mesh=mesh, in_specs=in_specs, out_specs=out_specs, check_vma=False)
```

```python
import functools
import heapq
import math
import jax
import jax.numpy as jnp
from jax import lax
from jax.experimental import pallas as pl
from jax.experimental.pallas import tpu as pltpu
from jax.sharding import PartitionSpec as P

MESH = pl.DeviceIdType.MESH
SPLIT = 32


class Net:
    def __init__(self, send, recv):
        row, col = lax.axis_index("row"), lax.axis_index("col")
        self.row, self.col = row, col
        self.high, self.y, self.core = row // 8, lax.rem(row // 2, 4), lax.rem(row, 2)
        self.x, self.low = col // 2, lax.rem(col, 2)
        self.send, self.recv = send, recv
        self.count = 0
        self.finish = []
        self.queue = []
        self.serial = 0
        self.now = 0.0
        self.free = {}
        self.spare = []

    def row_of(self, high, y, core):
        return high * 8 + lax.rem(y + 8, 4) * 2 + core

    def col_of(self, x, low):
        return lax.rem(x + 8, 4) * 2 + low

    def block_of(self, x, low):
        return low * 4 + lax.rem(x + 8, 4)

    def peer(self, name):
        high, y, core, x, low = self.high, self.y, self.core, self.x, self.low
        at = {
            "x+": (high, y, core, x + 1, low),
            "x-": (high, y, core, x - 1, low),
            "z": (high, y, core, x, 1 - low),
            "y+": (high, y + 1, core, x, low),
            "y-": (high, y - 1, core, x, low),
            "w": (1 - high, y, core, x, 1 - low),
            "c": (high, y, 1 - core, x, low),
            "y+c": (high, y + 1, 1 - core, x, low),
            "y-c": (high, y - 1, 1 - core, x, low),
        }[name]
        return self.row_of(*at[:3]), self.col_of(*at[3:])

    def greet(self, names):
        barrier = pltpu.get_barrier_semaphore()
        for name in names:
            pl.semaphore_signal(barrier, inc=1, device_id=self.peer(name), device_id_type=MESH)
        pl.semaphore_wait(barrier, len(names))

    def copy(self, src, dst, arriving, name):
        k = self.count
        self.count += 1
        make = lambda target: pltpu.make_async_remote_copy(
            src, target, self.send.at[k], self.recv.at[k], device_id=self.peer(name), device_id_type=MESH
        )
        out, arrival = make(dst), make(arriving)
        out.start()
        self.finish.append(out)
        rate, delay = (600e3, 1.0) if name == "c" else (46e3, 2.0)
        begin = max(self.now, self.free.get(name[:2], 0.0))
        self.free[name[:2]] = begin + math.prod(arriving.shape) * arriving.dtype.itemsize / rate
        return arrival, self.free[name[:2]] + delay

    def when(self, pending, action=None):
        arrival, time = pending

        def run():
            arrival.wait_recv()
            if action is not None:
                action()

        heapq.heappush(self.queue, (time, self.serial, run))
        self.serial += 1

    def work(self, time, action):
        self.spare.append((time, action))

    def spend(self, time):
        self.now += time

    def run(self):
        while self.queue or self.spare:
            if self.spare and (not self.queue or self.queue[0][0] > self.now + 0.5 * self.spare[0][0]):
                time, action = self.spare.pop(0)
                action()
                self.now += time
                continue
            time, _, action = heapq.heappop(self.queue)
            self.now = max(self.now, time) + 0.02
            action()
        for out in self.finish:
            out.wait_send()


def rows_of(ref, start, size, step=16):
    return ref.at[pl.ds(pl.multiple_of(start, step), size)]


def counted(count, action):
    left = [count]

    def step():
        left[0] -= 1
        if left[0] == 0:
            action()

    return step


def spread(net, src, out, plane_done=lambda: None, done=lambda: None):
    size = src.shape[0]
    a, half_a, half_b = SPLIT, SPLIT // 2, (size - SPLIT) // 2
    b = size - a
    x, low = net.x, net.low
    mine = counted(8, plane_done)
    theirs = counted(12, done)
    sides = ((-1, "x+", 0), (1, "x-", 1))

    def part(dx, other, start, rows):
        plane = 1 - low if other else low
        return rows_of(out, net.block_of(x + dx, plane) * size + start, rows)

    def own(start, rows):
        return src.at[pl.ds(start, rows)]

    def to_z(dx, start, rows):
        got = part(dx, 0, start, rows)
        net.when(net.copy(got, got, part(dx, 1, start, rows), "z"), theirs)

    def onward(dx, forward, other, start, rows, then):
        got = part(dx, other, start, rows)
        net.when(net.copy(got, got, part(2, other, start, rows), forward), then)

    def from_a(dx, forward, index):
        mine()

        def far():
            mine()
            to_z(2, index * half_a, half_a)

        onward(dx, forward, 0, index * half_a, half_a, far)
        to_z(dx, 0, a)

    def from_b(dx, forward, index):
        mine()
        onward(dx, forward, 0, a + index * half_b, half_b, mine)
        later()

    def partner(index, half, then):
        dx, forward, _ = sides[index]
        got = part(0, 1, a + half * half_b, half_b)
        net.when(net.copy(got, got, part(dx, 1, a + half * half_b, half_b), forward), then)

    def from_z():
        theirs()
        for dx, forward, index in sides:

            def first(dx=dx, forward=forward, index=index):
                theirs()
                onward(dx, forward, 1, a + index * half_b, half_b, theirs)

            partner(index, index, first)
        later()

    def second():
        for _, _, index in sides:
            partner(index, 1 - index, theirs)

    later = counted(3, second)
    net.when(net.copy(own(a, b), part(0, 0, a, b), part(0, 1, a, b), "z"), from_z)
    for start, rows, action in ((0, a, from_a), (a, b, from_b)):
        for dx, forward, index in sides:
            arrival = net.copy(own(start, rows), part(0, 0, start, rows), part(dx, 0, start, rows), forward)
            net.when(arrival, functools.partial(action, dx, forward, index))
    net.when(net.copy(own(0, a), part(0, 0, 0, a), part(0, 1, 0, a), "z"), theirs)
    out[pl.ds(pl.multiple_of(net.block_of(x, low) * size, size), size), :] = src[...]


def spread_small(net, src, out):
    size = src.shape[0]
    x, low = net.x, net.low

    def part(dx, other):
        plane = 1 - low if other else low
        return rows_of(out, net.block_of(x + dx, plane) * size, size, 8)

    def onward(other):
        got = part(-1, other)
        net.when(net.copy(got, got, part(-2, other), "x+"))

    def around(other, got):
        arrival = net.copy(got, part(0, other), part(-1, other), "x+")
        net.when(arrival, lambda: onward(other))
        net.when(net.copy(got, part(0, other), part(1, other), "x-"))

    around(0, src)
    arrival = net.copy(src, part(0, 0), part(0, 1), "z")
    net.when(arrival, lambda: around(1, part(0, 1)))
    out[pl.ds(pl.multiple_of(net.block_of(x, net.low) * size, size), size), :] = src[...]


def gather(net, src, out, relay, axis, done=lambda: None):
    depth, width = src.shape
    high, y, core = net.high, net.y, net.core
    middle = depth // 2
    landed = counted(10, done)

    def part(dy, other, core, half=None):
        index = net.row_of(1 - high if other else high, y + dy, core)
        start, size = (0, depth) if half is None else (half * middle, middle)
        if axis == 0:
            return rows_of(out, index * depth + start, size)
        return out.at[pl.ds(start, size), pl.ds(pl.multiple_of(index * width, width), width)]

    def to_core(dy, other, half=None):
        got = part(dy, other, core, half)
        net.when(net.copy(got, got, part(dy, other, 1 - core, half), "c"), landed)

    def from_y(dy, other):
        got = part(dy, other, core, 0 if dy < 0 else 1)
        forward = "y+" if dy < 0 else "y-"
        half = 0 if dy < 0 else 1
        arrival = net.copy(got, got, part(2, other, core, half), forward)
        net.when(arrival, lambda: to_core(2, other, half))
        to_core(dy, other)

    def around(other, got):
        for dy, forward in ((-1, "y+"), (1, "y-")):
            arrival = net.copy(got, part(0, other, core), part(dy, other, core), forward)
            net.when(arrival, lambda dy=dy: from_y(dy, other))

    around(0, src)
    waiting = [2]

    def arrived():
        waiting[0] -= 1
        if waiting[0] == 0:
            around(1, part(0, 1, core))
            to_core(0, 1)

    for half, first, second in ((0, "z", "w"), (1, "w", "z")):
        arrival = net.copy(src.at[pl.ds(half * middle, middle)], relay.at[half], relay.at[half], first)

        def onward(half=half, second=second):
            got = relay.at[half]
            arrival = net.copy(got, part(0, half, core, half), part(0, 1, core, half), second)
            net.when(arrival, arrived)

        net.when(arrival, onward)
    mine = part(0, 0, core)
    net.when(net.copy(src, mine, part(0, 0, 1 - core), "c"), landed)
    index = net.row
    if axis == 0:
        out[pl.ds(pl.multiple_of(index * depth, depth), depth), :] = src[...]
    else:
        out[:, pl.ds(pl.multiple_of(index * width, width), width)] = src[...]


def reduce_scatter(net, fill, src, scratch, finish, split, step=lambda action: action()):
    far_b, near_b, acc_b, plane, last = scratch[:5]
    if split:
        from_z, sums, far_a, near_a, acc_a = scratch[5:]
    size = src.shape[0] // 8
    a = split
    b = size - a
    x, low = net.x, net.low

    def rows(dx, other, start, count):
        index = net.block_of(x + dx, 1 - low if other else low)
        return pl.ds(pl.multiple_of(index * size + start, 16), count)

    def ring(block, count, far, near, acc, done):
        half = count // 2
        halves = {"x+": (0, half), "x-": (half, half)}
        waiting = [4]

        def arrived():
            waiting[0] -= 1
            if waiting[0] == 0:
                done()

        def start_far():
            for index, forward in ((0, "x+"), (1, "x-")):
                first = halves[forward][0]
                arrival = net.copy(block(2, first, half), far.at[index], far.at[index], forward)

                def add(index=index, forward=forward, first=first):
                    need(3)
                    term = block(1 if forward == "x+" else -1, first, half)
                    acc[index] = far[index] + term[...]
                    net.spend(0.1)
                    dst = near.at[index, pl.ds(first, half)]
                    net.when(net.copy(acc.at[index], dst, dst, forward), arrived)

                net.when(arrival, add)

        def start_direct():
            for index, forward in ((0, "x+"), (1, "x-")):
                first = half - halves[forward][0]
                dst = near.at[index, pl.ds(first, half)]
                term = block(1 if forward == "x+" else -1, first, half)
                net.when(net.copy(term, dst, dst, forward), arrived)

        return start_far, start_direct

    def block_b(other):
        return lambda dx, first, count: src.at[rows(dx, other, a + first, count)]

    def block_a(dx, first, count):
        return sums.at[pl.ds((dx % 4) * a + first, count)]

    left = [4]
    both = [3 if a else 2]
    wide = lambda value: value.astype(jnp.float32)

    def from_partner(k):
        need(4)
        sums[pl.ds(k * a, a), :] = from_z[pl.ds(k * a, a), :] + src[rows(k, 0, 0, a), :]
        net.spend(0.1)
        left[0] -= 1
        if left[0] == 0:
            for start in ring(block_a, a, far_a, near_a, acc_a, arrived):
                start()

    def to_partner(k):
        if a == 0:
            return
        landing = from_z.at[pl.ds(k * a, a)]
        net.when(net.copy(src.at[rows(k, 1, 0, a)], landing, landing, "z"), lambda: from_partner(k))

    def plane_done():
        need(4)
        total = wide(near_b[0, 0]) + wide(near_b[0, 1]) + wide(src[rows(0, 1, a, b), :])
        plane[...] = total.astype(plane.dtype)
        net.spend(0.3)
        net.when(net.copy(plane, last, last, "z"), arrived)

    def arrived():
        both[0] -= 1
        if both[0]:
            return
        if a:
            finish(0, wide(near_a[0]) + wide(near_a[1]) + wide(sums[pl.ds(0, a), :]))
        total = wide(near_b[1, 0]) + wide(near_b[1, 1]) + wide(src[rows(0, 0, a, b), :]) + wide(last[...])
        net.spend(0.5)
        finish(a, total)

    far_other, direct_other = ring(block_b(1), b, far_b.at[0], near_b.at[0], acc_b.at[0], plane_done)
    far_own, direct_own = ring(block_b(0), b, far_b.at[1], near_b.at[1], acc_b.at[1], arrived)
    def first():
        fill(lambda i: net.block_of(x + 2, lax.rem(low + 1 + i, 2)))
        far_other()
        far_own()
        to_partner(2)

    def second():
        fill(lambda i: net.block_of(x + 1 - 2 * i, 1 - low))
        direct_other()
        to_partner(1)
        to_partner(3)

    def third():
        fill(lambda i: net.block_of(x + 1 - 2 * i, low))
        direct_own()

    def fourth():
        fill(lambda i: net.block_of(x, lax.rem(low + 1 + i, 2)))
        to_partner(0)

    actions = [first, second, third, fourth]

    def need(number):
        while len(actions) > 4 - number:
            actions.pop(0)()

    for number in range(1, 5):
        step(lambda number=number: need(number))


def scatter_scratch(size, width, dtype, split):
    a, b = split, size - split
    shapes = [(2, 2, b // 2, width), (2, 2, b, width), (2, 2, b // 2, width), (b, width), (b, width)]
    if a:
        shapes += [(4 * a, width), (4 * a, width), (2, a // 2, width), (2, a, width), (2, a // 2, width)]
    return [pltpu.VMEM(shape, dtype) for shape in shapes]


def comm_body(spreads, smalls, gathers, *refs):
    count = spreads + smalls + len(gathers)
    ins, outs, relays = refs[:count], refs[count : 2 * count], refs[2 * count : -2]
    net = Net(*refs[-2:])
    net.greet(["x+", "x-", "z", "y+", "y-", "w", "c"])
    for k in range(spreads):
        spread(net, ins[k], outs[k])
    for k in range(spreads, spreads + smalls):
        spread_small(net, ins[k], outs[k])
    for i, axis in enumerate(gathers):
        k = spreads + smalls + i
        gather(net, ins[k], outs[k], relays[i], axis)
    net.run()


def communicate(name, body, collective_id, arrays, shapes, scratch, copies):
    used = sum(math.prod(ref.shape) * jnp.dtype(ref.dtype).itemsize for ref in scratch)
    return pl.pallas_call(
        body,
        out_shape=shapes,
        in_specs=[pl.BlockSpec(memory_space=pltpu.VMEM)] * len(arrays),
        out_specs=[pl.BlockSpec(memory_space=pltpu.VMEM)] * len(shapes),
        scratch_shapes=scratch + [pltpu.SemaphoreType.DMA((copies,)), pltpu.SemaphoreType.DMA((copies,))],
        compiler_params=pltpu.CompilerParams(
            collective_id=collective_id, has_side_effects=True, vmem_limit_bytes=used + 6 * 2**20
        ),
        name=name,
    )(*arrays)


def gathered(array, axis):
    depth, width = array.shape
    total = lax.axis_size("row")
    shape = (depth * total, width) if axis == 0 else (depth, width * total)
    return jax.ShapeDtypeStruct(shape, array.dtype)


def relay_of(array):
    return pltpu.VMEM((2, array.shape[0] // 2, array.shape[1]), array.dtype)


def exchange(name, collective_id, spreads=(), smalls=(), gathers=()):
    whole = [jax.ShapeDtypeStruct((8 * a.shape[0], a.shape[1]), a.dtype) for a in (*spreads, *smalls)]
    return communicate(
        name,
        functools.partial(comm_body, len(spreads), len(smalls), [axis for _, axis in gathers]),
        collective_id,
        [*spreads, *smalls, *(array for array, _ in gathers)],
        whole + [gathered(*pair) for pair in gathers],
        [relay_of(array) for array, _ in gathers],
        22 * len(spreads) + 8 * len(smalls) + 22 * len(gathers),
    )


def middle_body(heads, qkv, weight, tokens, gain, up, down, position, hidden, down_whole, units, out, *rest):
    terms, mixed, normed, image, up_whole, table, far, y_relay, up_relay, down_relay = rest[:10]
    net = Net(*rest[-2:])
    net.greet(["x+", "x-", "z", "y+", "y-", "w", "c", "y+c", "y-c"])
    size = tokens.shape[0]
    dim = qkv.shape[1] // (3 * heads)
    low = net.low
    slots = out.shape[3] // 2
    mine = pl.ds(pl.multiple_of(low * slots, slots), slots)
    theirs = pl.ds(pl.multiple_of((1 - low) * slots, slots), slots)

    def fill(column):
        @pl.loop(0, 2)
        def _(i):
            at = pl.ds(pl.multiple_of(column(i) * size, size), size)

            @pl.loop(0, heads)
            def _(h):
                part = lambda k: pl.ds(pl.multiple_of((3 * h + k) * dim, dim), dim)
                scores = lax.dot_general(
                    qkv[at, part(0)], qkv[:, part(1)], (((1,), (1,)), ((), ())), preferred_element_type=jnp.float32
                )
                scores = scores * (dim ** (-0.5))
                weights = jnp.exp(scores - jnp.max(scores, axis=-1, keepdims=True))
                chances = (weights / jnp.sum(weights, axis=-1, keepdims=True)).astype(jnp.bfloat16)
                mixed[:, pl.ds(pl.multiple_of(h * dim, dim), dim)] = matmul(chances, qkv[:, part(2)]).astype(jnp.bfloat16)

            @pl.loop(0, weight.shape[1] // 512)
            def _(j):
                columns = pl.ds(pl.multiple_of(j * 512, 512), 512)
                terms[at, columns] = matmul(mixed[...], weight[:, columns]).astype(jnp.bfloat16)

        net.spend(2.6)

    def place(index, plane):
        rows = pl.ds(pl.multiple_of(plane * 4 * size, 4 * size), 4 * size)
        flat = math.prod(table.shape[1:5])
        here = lax.broadcasted_iota(jnp.int32, (flat, 4 * size), 0) == position[pl.ds(0, 1), rows]
        placing = jnp.where(here, 1.0, 0.0).astype(jnp.bfloat16)
        span = 512

        @pl.loop(0, image.shape[1] // span)
        def _(j):
            columns = pl.ds(pl.multiple_of(j * span, span), span)
            put = matmul(placing, image[rows, columns]).astype(jnp.bfloat16)
            table[index, :, :, :, :, columns] = put.reshape(table.shape[1:5] + (span,))

        net.spend(1.2)

    def plane_done():
        place(0, low)

        def from_w(d):
            got = far.at[d, :, theirs]
            arrival = net.copy(got, got, far.at[d, :, mine], "z")
            net.when(arrival, last[d])
            first[d]()

        for d in (2, 1, 3, 0):
            arrival = net.copy(table.at[0, 1, d], far.at[d, :, mine], far.at[d, :, theirs], "w")
            net.when(arrival, functools.partial(from_w, d))
        start_all(own)
        ready()

    def image_done():
        place(1, 1 - low)
        start_all(other)
        ready()

    own = y_exchange(net, chunks(table.at[0, 0]), chunks(out.at[0], mine), y_relay.at[0])
    first = y_exchange(net, chunks(far, theirs), chunks(out.at[1], theirs), y_relay.at[1])
    last = y_exchange(net, chunks(far, mine), chunks(out.at[1], mine), y_relay.at[2])
    other = y_exchange(net, chunks(table.at[1, 0]), chunks(out.at[0], theirs), y_relay.at[3])
    ready = counted(3, lambda: up_tasks(net, image, up_whole, units))

    def finish(start, total):
        at = pl.ds(start, total.shape[0])
        state = (tokens[at, :].astype(jnp.float32) + total).astype(jnp.bfloat16)
        hidden[at, :] = state
        normed[at, :] = layer_norm(state, gain[...]).astype(jnp.bfloat16)
        if start == 0:
            return
        net.spend(0.5)
        spread(net, normed, image, plane_done, image_done)

    gather(net, up, up_whole, up_relay, 0, ready)
    gather(net, down, down_whole, down_relay, 1)
    reduce_scatter(net, fill, terms, rest[10:-2], finish, SPLIT)
    net.run()


def middle(collective_id, heads, qkv, weight, tokens, gain, up, down, position, slots):
    size, width = tokens.shape
    image = (8 * size, width)
    sixteen = lambda *shape: pltpu.VMEM(shape, tokens.dtype)
    scratch = [
        sixteen(*image),
        sixteen(size, weight.shape[0]),
        sixteen(size, width),
        sixteen(*image),
        sixteen(*gathered(up, 0).shape),
        sixteen(2, 2, 4, 2, slots // 2, width),
        sixteen(4, 2, slots, width),
        sixteen(4, 2, slots // 2, width),
        relay_of(up),
        relay_of(down),
    ]
    made = lambda *shape: jax.ShapeDtypeStruct(shape, tokens.dtype)
    return communicate(
        "middle",
        functools.partial(middle_body, heads),
        collective_id,
        (qkv, weight, tokens, gain, up, down, position),
        [made(size, width), gathered(down, 1), made(8 * size, up.shape[1]), made(2, 4, 2, slots, width)],
        scratch + scatter_scratch(size, width, tokens.dtype, SPLIT),
        24 + 22 + 2 * 22 + 8 + 4 * 10,
    )


def y_exchange(net, src, dst, relay, arrived=lambda d: None, then=lambda: None):
    core = net.core
    forwarded = counted(2, then)

    def opposite():
        for index, c, forward, last in ((0, core, "y+", "y+"), (1, 1 - core, "y-", "y-c")):

            def onward(index=index, c=c, last=last):
                arrival = net.copy(relay.at[index], dst(2, core), dst(2, c), last)
                net.when(arrival, lambda: arrived(2))
                forwarded()

            net.when(net.copy(src(2, c), relay.at[index], relay.at[index], forward), onward)

    def beside(d):
        forward = "y+" if d == 1 else "y-"
        for c, name in ((core, forward), (1 - core, forward + "c")):
            net.when(net.copy(src(d, c), dst(4 - d, core), dst(4 - d, c), name), lambda: arrived(4 - d))

    def here():
        net.when(net.copy(src(0, 1 - core), dst(0, core), dst(0, 1 - core), "c"), lambda: arrived(0))
        dst(0, core)[...] = src(0, core)[...]

    return {2: opposite, 1: lambda: beside(1), 3: lambda: beside(3), 0: here}


def chunks(ref, *rest):
    return lambda d, c: ref.at[(d, c, *rest)]


def start_all(steps):
    for d in (2, 1, 3, 0):
        steps[d]()


def up_tasks(net, x_ref, w_ref, out):
    rows, width = out.shape
    tile = min(256, rows)
    span = min(256, width)

    def piece(j):
        columns = pl.ds(j * span, span)

        @pl.loop(0, rows // tile)
        def _(i):
            at = pl.ds(pl.multiple_of(i * tile, tile), tile)
            inner = jnp.dot(x_ref[at, :], w_ref[:, columns], preferred_element_type=jnp.float32)
            out[at, columns] = (inner * (1.0 + lax.erf(inner * (0.5**0.5))) * 0.5).astype(out.dtype)

    for j in range(width // span):
        net.work(1.6, lambda j=j: piece(j))


def tail_body(units, down, parts, pick, hidden, out, *rest):
    terms, pair, far, other, total, near, partial, found, packed, relay, y_relay = rest[:11]
    net = Net(*rest[-2:])
    net.greet(["x+", "x-", "y+", "y-", "y+c", "y-c", "c", "z", "w"])
    low = net.low
    half = parts.shape[3] // 2
    size = hidden.shape[0]
    mine, theirs = pl.ds(pl.multiple_of(low * half, half), half), pl.ds(pl.multiple_of((1 - low) * half, half), half)
    count = packed.shape[1] // 4

    def fill(column):
        at = [pl.ds(pl.multiple_of(column(i) * size, size), size) for i in range(2)]
        for i in range(2):
            pair[pl.ds(i * size, size), :] = units[at[i], :]

        @pl.loop(0, down.shape[1] // 256)
        def _(j):
            columns = pl.ds(pl.multiple_of(j * 256, 256), 256)
            product = matmul(pair[...], down[:, columns]).astype(jnp.bfloat16)
            for i in range(2):
                terms[at[i], columns] = product[i * size : (i + 1) * size]

    def pack(index):
        flat = math.prod(found.shape[1:4])
        row = lax.broadcasted_iota(jnp.int32, (count, flat), 0)
        slot = lax.broadcasted_iota(jnp.int32, (count, flat), 1)
        each = half // 4
        same = (row // each == slot // half) & (row % each == slot % each)
        for k in range(4):
            chosen = same & (slot % half // each == lax.rem(net.x + k, 4))
            chosen = jnp.where(chosen, 1.0, 0.0).astype(jnp.bfloat16)

            @pl.loop(0, found.shape[4] // 512)
            def _(j):
                columns = pl.ds(pl.multiple_of(j * 512, 512), 512)
                rows = found[index, :, :, :, columns].reshape(flat, 512)
                value = matmul(chosen, rows).astype(jnp.bfloat16)
                packed[index, k * count : (k + 1) * count, columns] = value

        net.spend(0.6)

    def send(index):
        pack(index)
        at = lambda k, first=0, rows=count: packed.at[index, pl.ds(k * count + first, rows)]
        place = lambda k, first=0, rows=count: arrived_rows.at[index, pl.ds(k * count + first, rows)]
        middle = count // 2
        for i, forward in ((0, "x+"), (1, "x-")):

            def onward(i=i, forward=forward):
                dst = place(2, i * middle, middle)
                net.when(net.copy(relay.at[index, i], dst, dst, forward), landed)

            net.when(net.copy(at(2, i * middle, middle), relay.at[index, i], relay.at[index, i], forward), onward)
        for k, forward in ((1, "x+"), (3, "x-")):
            net.when(net.copy(at(k), place(k), place(k), forward), landed)

    arrived_rows, dense = rest[11:13]

    def finish_dense(start, total):
        dense[pl.ds(start, total.shape[0]), :] = total
        ready()

    def combine():
        flat = 4 * count
        for index in range(2):
            arrived_rows[index, pl.ds(0, count), :] = packed[index, pl.ds(0, count), :]

        @pl.loop(0, out.shape[1] // 512)
        def _(j):
            columns = pl.ds(pl.multiple_of(j * 512, 512), 512)
            value = hidden[:, columns].astype(jnp.float32) + dense[:, columns]
            for index in range(2):
                value += matmul(pick[:, pl.ds(index * flat, flat)], arrived_rows[index, :, columns])
            out[:, columns] = value.astype(jnp.bfloat16)

    ready = counted(9, combine)
    landed = ready

    def far_landed(d):
        def add():
            total[d] = far[d, :, theirs] + other[d]
            net.spend(0.2)
            arrival = net.copy(total.at[d], found.at[1, d], found.at[1, d], "w")
            net.when(arrival, complete[1])

        net.when(net.copy(far.at[d, :, mine], other.at[d], other.at[d], "z"), add)

    def near_landed(d):
        def add():
            found[0, d] = near[d, :, mine] + partial[d]
            net.spend(0.2)
            complete[0]()

        net.when(net.copy(near.at[d, :, theirs], partial.at[d], partial.at[d], "z"), add)

    complete = [counted(4, functools.partial(send, index)) for index in range(2)]
    far_counts = {d: counted(1 if d == 0 else 2, functools.partial(far_landed, d)) for d in range(4)}
    near_counts = {d: counted(1 if d == 0 else 2, functools.partial(near_landed, d)) for d in range(4)}
    second = y_exchange(net, chunks(parts.at[0]), chunks(near), y_relay.at[0], lambda d: near_counts[d]())
    first = y_exchange(net, chunks(parts.at[1]), chunks(far), y_relay.at[1], lambda d: far_counts[d](), lambda: start_all(second))
    start_all(first)
    reduce_scatter(net, fill, terms, rest[13:-2], finish_dense, 0, lambda action: net.work(1.6, action))
    net.run()


def tail(collective_id, units, down, parts, pick, hidden):
    size, width = hidden.shape
    rows = parts.shape[3]
    full, part = (4, 2, rows, width), (4, 2, rows // 2, width)
    sixteen = lambda *shape: pltpu.VMEM(shape, hidden.dtype)
    count = rows
    scratch = [
        sixteen(8 * size, width),
        sixteen(2 * size, units.shape[1]),
        sixteen(*full),
        sixteen(*part),
        sixteen(*part),
        sixteen(*full),
        sixteen(*part),
        sixteen(2, *part),
        sixteen(2, 4 * count, width),
        sixteen(2, 2, count // 2, width),
        sixteen(2, 2, rows, width),
        sixteen(2, 4 * count, width),
        pltpu.VMEM((size, width), jnp.float32),
    ]
    return communicate(
        "tail",
        tail_body,
        collective_id,
        (units, down, parts, pick, hidden),
        [jax.ShapeDtypeStruct(hidden.shape, hidden.dtype)],
        scratch + scatter_scratch(size, width, hidden.dtype, 0),
        24 + 2 * 10 + 12 + 12,
    )


def up_body(x_ref, w_ref, o_ref):
    inner = jnp.dot(x_ref[...], w_ref[...], preferred_element_type=jnp.float32)
    o_ref[...] = (inner * (1.0 + lax.erf(inner * (0.5**0.5))) * 0.5).astype(o_ref.dtype)


def up_gelu(x, w):
    rows, depth = x.shape
    width = w.shape[1]
    tile = min(width, 256)
    return pl.pallas_call(
        up_body,
        grid=(width // tile,),
        out_shape=jax.ShapeDtypeStruct((rows, width), jnp.bfloat16),
        in_specs=[
            pl.BlockSpec((rows, depth), lambda j: (0, 0)),
            pl.BlockSpec((depth, tile), lambda j: (0, j)),
        ],
        out_specs=pl.BlockSpec((rows, tile), lambda j: (0, j)),
        compiler_params=pltpu.CompilerParams(vmem_limit_bytes=32 * 2**20),
        cost_estimate=pl.CostEstimate(
            flops=2 * rows * depth * width,
            bytes_accessed=2 * (rows * depth + depth * width + rows * width),
            transcendentals=0,
        ),
        name="up_gelu",
    )(x, w)


def layer_norm(row_data, gain_vector):
    row_data = row_data.astype(jnp.float32)
    centered = row_data - jnp.mean(row_data, axis=-1, keepdims=True)
    spread = jnp.mean(centered * centered, axis=-1, keepdims=True)
    return centered * lax.rsqrt(spread + 1e-06) * gain_vector


def matmul(a, b):
    return jnp.dot(a, b, preferred_element_type=jnp.float32)


def shards(
    tokens,
    ln1_gain,
    qkv_weight,
    out_weight,
    ln2_gain,
    ffn_in,
    ffn_out,
    expert_ids,
    expert_in,
    expert_out,
):
    tok_count, model_width = tokens.shape
    row_total = lax.axis_size("row")
    col_total = lax.axis_size("col")
    row_index = lax.axis_index("row")
    col_index = lax.axis_index("col")
    expert_count = row_total * col_total // 2
    capacity = max(2, 2 * tok_count // expert_count)
    head_count, head_dim = qkv_weight.shape[1], qkv_weight.shape[3]
    seq_len = tok_count * col_total

    ids = expert_ids[:, 0]
    token = jnp.arange(tok_count, dtype=jnp.int32)
    same = (expert_ids == ids[None, :]) & (token[:, None] < token[None, :])
    codes = ids * capacity + jnp.sum(same.astype(jnp.int32), axis=0)
    image_rows, codes_all, qkv_whole, out_whole = exchange(
        "enter",
        0,
        spreads=(tokens,),
        smalls=(jnp.broadcast_to(codes[None, :], (8, tok_count)),),
        gathers=((qkv_weight.reshape(qkv_weight.shape[0], -1), 0), (out_weight, 1)),
    )
    normed = layer_norm(image_rows, ln1_gain).astype(jnp.bfloat16)
    projected = matmul(normed, qkv_whole).astype(jnp.bfloat16)
    codes_all = codes_all.reshape(col_total, 8, tok_count)[:, 0]
    ids_rows, slot_index = codes_all // capacity, codes_all % capacity
    block = jnp.arange(col_total, dtype=jnp.int32)[:, None]
    plane, place = block // 4, block % 4 * capacity + slot_index
    home_row = 2 * ids_rows // col_total
    mine = (2 * ids_rows % col_total) // 2 == col_index // 2
    other = (home_row // 8 != row_index // 8).astype(jnp.int32)
    chunk = (home_row // 2 - row_index // 2 + 8) % 4 * 2 + home_row % 2
    half = 4 * capacity
    rows = 2 * half
    slot_count = row_total * rows
    position = jnp.where(mine, (other * 8 + chunk) * half + place, -1).reshape(1, seq_len)
    position = jnp.broadcast_to(position, (8, seq_len))
    home = ids // 4
    turn = (home // 2 - row_index // 2 + 8) % 4 * 2 + home % 2
    found = (col_index // 2 - ids % 4 + 4) % 4 * rows + turn * capacity + codes % capacity
    found = jnp.where(home // 8 != row_index // 8, found + 4 * rows, found)
    pick = (found[:, None] == jnp.arange(8 * rows, dtype=jnp.int32)[None, :]).astype(jnp.bfloat16)

    hidden_mine, down_whole, hidden_units, expert_rows = middle(
        1, head_count, projected, out_whole, tokens, ln2_gain[None, :], ffn_in, ffn_out, position, rows
    )
    expert_units = up_gelu(expert_rows.reshape(slot_count, model_width), expert_in[0])
    partial_out = matmul(expert_units, expert_out[0]).astype(jnp.bfloat16).reshape(expert_rows.shape)
    (out,) = tail(2, hidden_units, down_whole, partial_out, pick, hidden_mine)
    return out


def solution(mesh):
    in_specs = (
        P(("row", "col"), None),
        P(),
        P("row", "col", None, None),
        P("col", "row"),
        P(),
        P("row", "col"),
        P("col", "row"),
        P(("row", "col"), None),
        P(("row", "col"), None, None),
        P(("row", "col"), None, None),
    )
    out_specs = P(("row", "col"), None)
    return jax.shard_map(shards, mesh=mesh, in_specs=in_specs, out_specs=out_specs, check_vma=False)
```

```python
import functools
import heapq
import math
import jax
import jax.numpy as jnp
from jax import lax
from jax.experimental import pallas as pl
from jax.experimental.pallas import tpu as pltpu
from jax.sharding import PartitionSpec as P

MESH = pl.DeviceIdType.MESH
SPLIT = 32


class Net:
    def __init__(self, send, recv):
        row, col = lax.axis_index("row"), lax.axis_index("col")
        self.row, self.col = row, col
        self.high, self.y, self.core = row // 8, lax.rem(row // 2, 4), lax.rem(row, 2)
        self.x, self.low = col // 2, lax.rem(col, 2)
        self.send, self.recv = send, recv
        self.count = 0
        self.finish = []
        self.queue = []
        self.serial = 0
        self.now = 0.0
        self.free = {}
        self.spare = []

    def row_of(self, high, y, core):
        return high * 8 + lax.rem(y + 8, 4) * 2 + core

    def col_of(self, x, low):
        return lax.rem(x + 8, 4) * 2 + low

    def block_of(self, x, low):
        return low * 4 + lax.rem(x + 8, 4)

    def peer(self, name):
        high, y, core, x, low = self.high, self.y, self.core, self.x, self.low
        at = {
            "x+": (high, y, core, x + 1, low),
            "x-": (high, y, core, x - 1, low),
            "z": (high, y, core, x, 1 - low),
            "y+": (high, y + 1, core, x, low),
            "y-": (high, y - 1, core, x, low),
            "w": (1 - high, y, core, x, 1 - low),
            "c": (high, y, 1 - core, x, low),
            "y+c": (high, y + 1, 1 - core, x, low),
            "y-c": (high, y - 1, 1 - core, x, low),
        }[name]
        return self.row_of(*at[:3]), self.col_of(*at[3:])

    def greet(self, names):
        barrier = pltpu.get_barrier_semaphore()
        for name in names:
            pl.semaphore_signal(barrier, inc=1, device_id=self.peer(name), device_id_type=MESH)
        pl.semaphore_wait(barrier, len(names))

    def copy(self, src, dst, arriving, name):
        k = self.count
        self.count += 1
        make = lambda target: pltpu.make_async_remote_copy(
            src, target, self.send.at[k], self.recv.at[k], device_id=self.peer(name), device_id_type=MESH
        )
        out, arrival = make(dst), make(arriving)
        out.start()
        self.finish.append(out)
        rate, delay = (600e3, 1.0) if name == "c" else (46e3, 2.0)
        begin = max(self.now, self.free.get(name[:2], 0.0))
        self.free[name[:2]] = begin + math.prod(arriving.shape) * arriving.dtype.itemsize / rate
        return arrival, self.free[name[:2]] + delay

    def when(self, pending, action=None):
        arrival, time = pending

        def run():
            arrival.wait_recv()
            if action is not None:
                action()

        heapq.heappush(self.queue, (time, self.serial, run))
        self.serial += 1

    def work(self, time, action):
        self.spare.append((time, action))

    def spend(self, time):
        self.now += time

    def run(self):
        while self.queue or self.spare:
            if self.spare and (not self.queue or self.queue[0][0] > self.now + 0.5 * self.spare[0][0]):
                time, action = self.spare.pop(0)
                action()
                self.now += time
                continue
            time, _, action = heapq.heappop(self.queue)
            self.now = max(self.now, time) + 0.02
            action()
        for out in self.finish:
            out.wait_send()


def rows_of(ref, start, size, step=16):
    return ref.at[pl.ds(pl.multiple_of(start, step), size)]


def counted(count, action):
    left = [count]

    def step():
        left[0] -= 1
        if left[0] == 0:
            action()

    return step


def spread(net, src, out, plane_done=lambda: None, done=lambda: None):
    size = src.shape[0]
    a, half_a, half_b = SPLIT, SPLIT // 2, (size - SPLIT) // 2
    b = size - a
    x, low = net.x, net.low
    mine = counted(8, plane_done)
    theirs = counted(12, done)
    sides = ((-1, "x+", 0), (1, "x-", 1))

    def part(dx, other, start, rows):
        plane = 1 - low if other else low
        return rows_of(out, net.block_of(x + dx, plane) * size + start, rows)

    def own(start, rows):
        return src.at[pl.ds(start, rows)]

    def to_z(dx, start, rows):
        got = part(dx, 0, start, rows)
        net.when(net.copy(got, got, part(dx, 1, start, rows), "z"), theirs)

    def onward(dx, forward, other, start, rows, then):
        got = part(dx, other, start, rows)
        net.when(net.copy(got, got, part(2, other, start, rows), forward), then)

    def from_a(dx, forward, index):
        mine()

        def far():
            mine()
            to_z(2, index * half_a, half_a)

        onward(dx, forward, 0, index * half_a, half_a, far)
        to_z(dx, 0, a)

    def from_b(dx, forward, index):
        mine()
        onward(dx, forward, 0, a + index * half_b, half_b, mine)
        later()

    def partner(index, half, then):
        dx, forward, _ = sides[index]
        got = part(0, 1, a + half * half_b, half_b)
        net.when(net.copy(got, got, part(dx, 1, a + half * half_b, half_b), forward), then)

    def from_z():
        theirs()
        for dx, forward, index in sides:

            def first(dx=dx, forward=forward, index=index):
                theirs()
                onward(dx, forward, 1, a + index * half_b, half_b, theirs)

            partner(index, index, first)
        later()

    def second():
        for _, _, index in sides:
            partner(index, 1 - index, theirs)

    later = counted(3, second)
    net.when(net.copy(own(a, b), part(0, 0, a, b), part(0, 1, a, b), "z"), from_z)
    for start, rows, action in ((0, a, from_a), (a, b, from_b)):
        for dx, forward, index in sides:
            arrival = net.copy(own(start, rows), part(0, 0, start, rows), part(dx, 0, start, rows), forward)
            net.when(arrival, functools.partial(action, dx, forward, index))
    net.when(net.copy(own(0, a), part(0, 0, 0, a), part(0, 1, 0, a), "z"), theirs)
    out[pl.ds(pl.multiple_of(net.block_of(x, low) * size, size), size), :] = src[...]


def spread_small(net, src, out):
    size = src.shape[0]
    x, low = net.x, net.low

    def part(dx, other):
        plane = 1 - low if other else low
        return rows_of(out, net.block_of(x + dx, plane) * size, size, 8)

    def onward(other):
        got = part(-1, other)
        net.when(net.copy(got, got, part(-2, other), "x+"))

    def around(other, got):
        arrival = net.copy(got, part(0, other), part(-1, other), "x+")
        net.when(arrival, lambda: onward(other))
        net.when(net.copy(got, part(0, other), part(1, other), "x-"))

    around(0, src)
    arrival = net.copy(src, part(0, 0), part(0, 1), "z")
    net.when(arrival, lambda: around(1, part(0, 1)))
    out[pl.ds(pl.multiple_of(net.block_of(x, net.low) * size, size), size), :] = src[...]


def gather(net, src, out, relay, axis, done=lambda: None):
    depth, width = src.shape
    high, y, core = net.high, net.y, net.core
    middle = depth // 2
    landed = counted(10, done)

    def part(dy, other, core, half=None):
        index = net.row_of(1 - high if other else high, y + dy, core)
        start, size = (0, depth) if half is None else (half * middle, middle)
        if axis == 0:
            return rows_of(out, index * depth + start, size)
        return out.at[pl.ds(start, size), pl.ds(pl.multiple_of(index * width, width), width)]

    def to_core(dy, other, half=None):
        got = part(dy, other, core, half)
        net.when(net.copy(got, got, part(dy, other, 1 - core, half), "c"), landed)

    def from_y(dy, other):
        got = part(dy, other, core, 0 if dy < 0 else 1)
        forward = "y+" if dy < 0 else "y-"
        half = 0 if dy < 0 else 1
        arrival = net.copy(got, got, part(2, other, core, half), forward)
        net.when(arrival, lambda: to_core(2, other, half))
        to_core(dy, other)

    def around(other, got):
        for dy, forward in ((-1, "y+"), (1, "y-")):
            arrival = net.copy(got, part(0, other, core), part(dy, other, core), forward)
            net.when(arrival, lambda dy=dy: from_y(dy, other))

    around(0, src)
    waiting = [2]

    def arrived():
        waiting[0] -= 1
        if waiting[0] == 0:
            around(1, part(0, 1, core))
            to_core(0, 1)

    for half, first, second in ((0, "z", "w"), (1, "w", "z")):
        arrival = net.copy(src.at[pl.ds(half * middle, middle)], relay.at[half], relay.at[half], first)

        def onward(half=half, second=second):
            got = relay.at[half]
            arrival = net.copy(got, part(0, half, core, half), part(0, 1, core, half), second)
            net.when(arrival, arrived)

        net.when(arrival, onward)
    mine = part(0, 0, core)
    net.when(net.copy(src, mine, part(0, 0, 1 - core), "c"), landed)
    index = net.row
    if axis == 0:
        out[pl.ds(pl.multiple_of(index * depth, depth), depth), :] = src[...]
    else:
        out[:, pl.ds(pl.multiple_of(index * width, width), width)] = src[...]


def reduce_scatter(net, fill, src, scratch, finish, split, step=lambda action: action()):
    far_b, near_b, acc_b, plane, last = scratch[:5]
    if split:
        from_z, sums, far_a, near_a, acc_a = scratch[5:]
    size = src.shape[0] // 8
    a = split
    b = size - a
    x, low = net.x, net.low

    def rows(dx, other, start, count):
        index = net.block_of(x + dx, 1 - low if other else low)
        return pl.ds(pl.multiple_of(index * size + start, 16), count)

    def ring(block, count, far, near, acc, done):
        half = count // 2
        halves = {"x+": (0, half), "x-": (half, half)}
        waiting = [4]

        def arrived():
            waiting[0] -= 1
            if waiting[0] == 0:
                done()

        def start_far():
            for index, forward in ((0, "x+"), (1, "x-")):
                first = halves[forward][0]
                arrival = net.copy(block(2, first, half), far.at[index], far.at[index], forward)

                def add(index=index, forward=forward, first=first):
                    need(3)
                    term = block(1 if forward == "x+" else -1, first, half)
                    acc[index] = far[index] + term[...]
                    net.spend(0.1)
                    dst = near.at[index, pl.ds(first, half)]
                    net.when(net.copy(acc.at[index], dst, dst, forward), arrived)

                net.when(arrival, add)

        def start_direct():
            for index, forward in ((0, "x+"), (1, "x-")):
                first = half - halves[forward][0]
                dst = near.at[index, pl.ds(first, half)]
                term = block(1 if forward == "x+" else -1, first, half)
                net.when(net.copy(term, dst, dst, forward), arrived)

        return start_far, start_direct

    def block_b(other):
        return lambda dx, first, count: src.at[rows(dx, other, a + first, count)]

    def block_a(dx, first, count):
        return sums.at[pl.ds((dx % 4) * a + first, count)]

    left = [4]
    both = [3 if a else 2]
    wide = lambda value: value.astype(jnp.float32)

    def from_partner(k):
        need(4)
        sums[pl.ds(k * a, a), :] = from_z[pl.ds(k * a, a), :] + src[rows(k, 0, 0, a), :]
        net.spend(0.1)
        left[0] -= 1
        if left[0] == 0:
            for start in ring(block_a, a, far_a, near_a, acc_a, arrived):
                start()

    def to_partner(k):
        if a == 0:
            return
        landing = from_z.at[pl.ds(k * a, a)]
        net.when(net.copy(src.at[rows(k, 1, 0, a)], landing, landing, "z"), lambda: from_partner(k))

    def plane_done():
        need(4)
        total = wide(near_b[0, 0]) + wide(near_b[0, 1]) + wide(src[rows(0, 1, a, b), :])
        plane[...] = total.astype(plane.dtype)
        net.spend(0.3)
        net.when(net.copy(plane, last, last, "z"), arrived)

    def arrived():
        both[0] -= 1
        if both[0]:
            return
        if a:
            finish(0, wide(near_a[0]) + wide(near_a[1]) + wide(sums[pl.ds(0, a), :]))
        total = wide(near_b[1, 0]) + wide(near_b[1, 1]) + wide(src[rows(0, 0, a, b), :]) + wide(last[...])
        net.spend(0.5)
        finish(a, total)

    far_other, direct_other = ring(block_b(1), b, far_b.at[0], near_b.at[0], acc_b.at[0], plane_done)
    far_own, direct_own = ring(block_b(0), b, far_b.at[1], near_b.at[1], acc_b.at[1], arrived)
    def first():
        fill(lambda i: net.block_of(x + 2, lax.rem(low + 1 + i, 2)))
        far_other()
        far_own()
        to_partner(2)

    def second():
        fill(lambda i: net.block_of(x + 1 - 2 * i, 1 - low))
        direct_other()
        to_partner(1)
        to_partner(3)

    def third():
        fill(lambda i: net.block_of(x + 1 - 2 * i, low))
        direct_own()

    def fourth():
        fill(lambda i: net.block_of(x, lax.rem(low + 1 + i, 2)))
        to_partner(0)

    actions = [first, second, third, fourth]

    def need(number):
        while len(actions) > 4 - number:
            actions.pop(0)()

    for number in range(1, 5):
        step(lambda number=number: need(number))


def scatter_scratch(size, width, dtype, split):
    a, b = split, size - split
    shapes = [(2, 2, b // 2, width), (2, 2, b, width), (2, 2, b // 2, width), (b, width), (b, width)]
    if a:
        shapes += [(4 * a, width), (4 * a, width), (2, a // 2, width), (2, a, width), (2, a // 2, width)]
    return [pltpu.VMEM(shape, dtype) for shape in shapes]


def comm_body(spreads, smalls, gathers, *refs):
    count = spreads + smalls + len(gathers)
    ins, outs, relays = refs[:count], refs[count : 2 * count], refs[2 * count : -2]
    net = Net(*refs[-2:])
    net.greet(["x+", "x-", "z", "y+", "y-", "w", "c"])
    for k in range(spreads):
        spread(net, ins[k], outs[k])
    for k in range(spreads, spreads + smalls):
        spread_small(net, ins[k], outs[k])
    for i, axis in enumerate(gathers):
        k = spreads + smalls + i
        gather(net, ins[k], outs[k], relays[i], axis)
    net.run()


def communicate(name, body, collective_id, arrays, shapes, scratch, copies, outside=()):
    used = sum(math.prod(r.shape) * jnp.dtype(r.dtype).itemsize for r in scratch if r.memory_space == pltpu.VMEM)
    spaces = [pl.ANY if i in outside else pltpu.VMEM for i in range(len(arrays))]
    return pl.pallas_call(
        body,
        out_shape=shapes,
        in_specs=[pl.BlockSpec(memory_space=space) for space in spaces],
        out_specs=[pl.BlockSpec(memory_space=pltpu.VMEM)] * len(shapes),
        scratch_shapes=scratch + [pltpu.SemaphoreType.DMA((copies,)), pltpu.SemaphoreType.DMA((copies,))],
        compiler_params=pltpu.CompilerParams(
            collective_id=collective_id, has_side_effects=True, vmem_limit_bytes=used + 6 * 2**20
        ),
        name=name,
    )(*arrays)


def gathered(array, axis):
    depth, width = array.shape
    total = lax.axis_size("row")
    shape = (depth * total, width) if axis == 0 else (depth, width * total)
    return jax.ShapeDtypeStruct(shape, array.dtype)


def relay_of(array):
    return pltpu.VMEM((2, array.shape[0] // 2, array.shape[1]), array.dtype)


def exchange(name, collective_id, spreads=(), smalls=(), gathers=()):
    whole = [jax.ShapeDtypeStruct((8 * a.shape[0], a.shape[1]), a.dtype) for a in (*spreads, *smalls)]
    return communicate(
        name,
        functools.partial(comm_body, len(spreads), len(smalls), [axis for _, axis in gathers]),
        collective_id,
        [*spreads, *smalls, *(array for array, _ in gathers)],
        whole + [gathered(*pair) for pair in gathers],
        [relay_of(array) for array, _ in gathers],
        22 * len(spreads) + 8 * len(smalls) + 22 * len(gathers),
    )


def middle_body(heads, qkv, weight, tokens, gain, up, down, position, hidden, down_whole, units, out, *rest):
    terms, mixed, normed, image, up_whole, table, far, y_relay, up_relay, down_relay = rest[:10]
    net = Net(*rest[-2:])
    net.greet(["x+", "x-", "z", "y+", "y-", "w", "c", "y+c", "y-c"])
    size = tokens.shape[0]
    dim = qkv.shape[1] // (3 * heads)
    low = net.low
    slots = out.shape[3] // 2
    mine = pl.ds(pl.multiple_of(low * slots, slots), slots)
    theirs = pl.ds(pl.multiple_of((1 - low) * slots, slots), slots)

    def fill(column):
        @pl.loop(0, 2)
        def _(i):
            at = pl.ds(pl.multiple_of(column(i) * size, size), size)

            @pl.loop(0, heads)
            def _(h):
                part = lambda k: pl.ds(pl.multiple_of((3 * h + k) * dim, dim), dim)
                scores = lax.dot_general(
                    qkv[at, part(0)], qkv[:, part(1)], (((1,), (1,)), ((), ())), preferred_element_type=jnp.float32
                )
                scores = scores * (dim ** (-0.5))
                weights = jnp.exp(scores - jnp.max(scores, axis=-1, keepdims=True))
                chances = (weights / jnp.sum(weights, axis=-1, keepdims=True)).astype(jnp.bfloat16)
                mixed[:, pl.ds(pl.multiple_of(h * dim, dim), dim)] = matmul(chances, qkv[:, part(2)]).astype(jnp.bfloat16)

            @pl.loop(0, weight.shape[1] // 512)
            def _(j):
                columns = pl.ds(pl.multiple_of(j * 512, 512), 512)
                terms[at, columns] = matmul(mixed[...], weight[:, columns]).astype(jnp.bfloat16)

        net.spend(2.6)

    def place(index, plane):
        rows = pl.ds(pl.multiple_of(plane * 4 * size, 4 * size), 4 * size)
        flat = math.prod(table.shape[1:5])
        here = lax.broadcasted_iota(jnp.int32, (flat, 4 * size), 0) == position[pl.ds(0, 1), rows]
        placing = jnp.where(here, 1.0, 0.0).astype(jnp.bfloat16)
        span = 512

        @pl.loop(0, image.shape[1] // span)
        def _(j):
            columns = pl.ds(pl.multiple_of(j * span, span), span)
            put = matmul(placing, image[rows, columns]).astype(jnp.bfloat16)
            table[index, :, :, :, :, columns] = put.reshape(table.shape[1:5] + (span,))

        net.spend(1.2)

    def plane_done():
        place(0, low)

        def from_w(d):
            got = far.at[d, :, theirs]
            arrival = net.copy(got, got, far.at[d, :, mine], "z")
            net.when(arrival, last[d])
            first[d]()

        for d in (2, 1, 3, 0):
            arrival = net.copy(table.at[0, 1, d], far.at[d, :, mine], far.at[d, :, theirs], "w")
            net.when(arrival, functools.partial(from_w, d))
        start_all(own)
        ready()

    def image_done():
        place(1, 1 - low)
        start_all(other)
        ready()

    own = y_exchange(net, chunks(table.at[0, 0]), chunks(out.at[0], mine), y_relay.at[0])
    first = y_exchange(net, chunks(far, theirs), chunks(out.at[1], theirs), y_relay.at[1])
    last = y_exchange(net, chunks(far, mine), chunks(out.at[1], mine), y_relay.at[2])
    other = y_exchange(net, chunks(table.at[1, 0]), chunks(out.at[0], theirs), y_relay.at[3])
    ready = counted(3, lambda: up_tasks(net, image, up_whole, units))

    def finish(start, total):
        at = pl.ds(start, total.shape[0])
        state = (tokens[at, :].astype(jnp.float32) + total).astype(jnp.bfloat16)
        hidden[at, :] = state
        normed[at, :] = layer_norm(state, gain[...]).astype(jnp.bfloat16)
        if start == 0:
            return
        net.spend(0.5)
        spread(net, normed, image, plane_done, image_done)

    gather(net, up, up_whole, up_relay, 0, ready)
    gather(net, down, down_whole, down_relay, 1)
    reduce_scatter(net, fill, terms, rest[10:-2], finish, SPLIT)
    net.run()


def middle(collective_id, heads, qkv, weight, tokens, gain, up, down, position, slots):
    size, width = tokens.shape
    image = (8 * size, width)
    sixteen = lambda *shape: pltpu.VMEM(shape, tokens.dtype)
    scratch = [
        sixteen(*image),
        sixteen(size, weight.shape[0]),
        sixteen(size, width),
        sixteen(*image),
        sixteen(*gathered(up, 0).shape),
        sixteen(2, 2, 4, 2, slots // 2, width),
        sixteen(4, 2, slots, width),
        sixteen(4, 2, slots // 2, width),
        relay_of(up),
        relay_of(down),
    ]
    made = lambda *shape: jax.ShapeDtypeStruct(shape, tokens.dtype)
    return communicate(
        "middle",
        functools.partial(middle_body, heads),
        collective_id,
        (qkv, weight, tokens, gain, up, down, position),
        [made(size, width), gathered(down, 1), made(8 * size, up.shape[1]), made(2, 4, 2, slots, width)],
        scratch + scatter_scratch(size, width, tokens.dtype, SPLIT),
        24 + 22 + 2 * 22 + 8 + 4 * 10,
    )


def y_exchange(net, src, dst, relay, arrived=lambda d: None, then=lambda: None):
    core = net.core
    forwarded = counted(2, then)

    def opposite():
        for index, c, forward, last in ((0, core, "y+", "y+"), (1, 1 - core, "y-", "y-c")):

            def onward(index=index, c=c, last=last):
                arrival = net.copy(relay.at[index], dst(2, core), dst(2, c), last)
                net.when(arrival, lambda: arrived(2))
                forwarded()

            net.when(net.copy(src(2, c), relay.at[index], relay.at[index], forward), onward)

    def beside(d):
        forward = "y+" if d == 1 else "y-"
        for c, name in ((core, forward), (1 - core, forward + "c")):
            net.when(net.copy(src(d, c), dst(4 - d, core), dst(4 - d, c), name), lambda: arrived(4 - d))

    def here():
        net.when(net.copy(src(0, 1 - core), dst(0, core), dst(0, 1 - core), "c"), lambda: arrived(0))
        dst(0, core)[...] = src(0, core)[...]

    return {2: opposite, 1: lambda: beside(1), 3: lambda: beside(3), 0: here}


def chunks(ref, *rest):
    return lambda d, c: ref.at[(d, c, *rest)]


def start_all(steps):
    for d in (2, 1, 3, 0):
        steps[d]()


def up_tasks(net, x_ref, w_ref, out):
    rows, width = out.shape
    tile = min(256, rows)
    span = min(256, width)

    def piece(j):
        columns = pl.ds(j * span, span)

        @pl.loop(0, rows // tile)
        def _(i):
            at = pl.ds(pl.multiple_of(i * tile, tile), tile)
            inner = jnp.dot(x_ref[at, :], w_ref[:, columns], preferred_element_type=jnp.float32)
            out[at, columns] = (inner * (1.0 + lax.erf(inner * (0.5**0.5))) * 0.5).astype(out.dtype)

    for j in range(width // span):
        net.work(1.6, lambda j=j: piece(j))


def tail_body(units, down, rows, expert_in, expert_out, pick, hidden, out, *rest):
    terms, pair, far, other, total, near, partial, found, packed, relay, y_relay = rest[:11]
    arrived_rows, dense, parts, inner, weights, fetched = rest[11:17]
    tiles, span = weights.shape[1], weights.shape[3]
    fetches = []
    for i, source in enumerate((expert_in, expert_out)):
        for j in range(tiles):
            fetch = pltpu.make_async_copy(source.at[:, pl.ds(j * span, span)], weights.at[i, j], fetched.at[i, j])
            fetch.start()
            fetches.append(fetch)
    net = Net(*rest[-2:])
    net.greet(["x+", "x-", "y+", "y-", "y+c", "y-c", "c", "z", "w"])
    low = net.low
    half = parts.shape[3] // 2
    size = hidden.shape[0]
    mine, theirs = pl.ds(pl.multiple_of(low * half, half), half), pl.ds(pl.multiple_of((1 - low) * half, half), half)
    count = packed.shape[1] // 4

    def fill(column):
        at = [pl.ds(pl.multiple_of(column(i) * size, size), size) for i in range(2)]
        for i in range(2):
            pair[pl.ds(i * size, size), :] = units[at[i], :]

        @pl.loop(0, down.shape[1] // 256)
        def _(j):
            columns = pl.ds(pl.multiple_of(j * 256, 256), 256)
            product = matmul(pair[...], down[:, columns]).astype(jnp.bfloat16)
            for i in range(2):
                terms[at[i], columns] = product[i * size : (i + 1) * size]

    def pack(index):
        flat = math.prod(found.shape[1:4])
        row = lax.broadcasted_iota(jnp.int32, (count, flat), 0)
        slot = lax.broadcasted_iota(jnp.int32, (count, flat), 1)
        each = half // 4
        same = (row // each == slot // half) & (row % each == slot % each)
        for k in range(4):
            chosen = same & (slot % half // each == lax.rem(net.x + k, 4))
            chosen = jnp.where(chosen, 1.0, 0.0).astype(jnp.bfloat16)

            @pl.loop(0, found.shape[4] // 512)
            def _(j):
                columns = pl.ds(pl.multiple_of(j * 512, 512), 512)
                rows = found[index, :, :, :, columns].reshape(flat, 512)
                value = matmul(chosen, rows).astype(jnp.bfloat16)
                packed[index, k * count : (k + 1) * count, columns] = value

        net.spend(0.6)

    def send(index):
        pack(index)
        at = lambda k, first=0, rows=count: packed.at[index, pl.ds(k * count + first, rows)]
        place = lambda k, first=0, rows=count: arrived_rows.at[index, pl.ds(k * count + first, rows)]
        middle = count // 2
        for i, forward in ((0, "x+"), (1, "x-")):

            def onward(i=i, forward=forward):
                dst = place(2, i * middle, middle)
                net.when(net.copy(relay.at[index, i], dst, dst, forward), landed)

            net.when(net.copy(at(2, i * middle, middle), relay.at[index, i], relay.at[index, i], forward), onward)
        for k, forward in ((1, "x+"), (3, "x-")):
            net.when(net.copy(at(k), place(k), place(k), forward), landed)

    flat_rows = math.prod(parts.shape[1:4])

    def expert_up(j):
        fetches[j].wait()

        @pl.loop(0, 2)
        def _(i):
            value = matmul(rows[i].reshape(flat_rows, rows.shape[4]), weights[0, j])
            value = value * (1.0 + lax.erf(value * (0.5**0.5))) * 0.5
            inner[i, :, pl.ds(j * span, span)] = value.astype(inner.dtype)

        net.spend(1.5)

    def expert_down(i, j):
        if i == 1:
            fetches[tiles + j].wait()
        value = matmul(inner[i], weights[1, j]).astype(parts.dtype)
        parts[i, :, :, :, pl.ds(j * span, span)] = value.reshape(parts.shape[1:4] + (span,))
        net.spend(0.7)

    def finish_dense(start, total):
        dense[pl.ds(start, total.shape[0]), :] = total
        ready()

    def combine():
        flat = 4 * count
        for index in range(2):
            arrived_rows[index, pl.ds(0, count), :] = packed[index, pl.ds(0, count), :]

        @pl.loop(0, out.shape[1] // 512)
        def _(j):
            columns = pl.ds(pl.multiple_of(j * 512, 512), 512)
            value = hidden[:, columns].astype(jnp.float32) + dense[:, columns]
            for index in range(2):
                value += matmul(pick[:, pl.ds(index * flat, flat)], arrived_rows[index, :, columns])
            out[:, columns] = value.astype(jnp.bfloat16)

    ready = counted(9, combine)
    landed = ready

    def far_landed(d):
        def add():
            total[d] = far[d, :, theirs] + other[d]
            net.spend(0.2)
            arrival = net.copy(total.at[d], found.at[1, d], found.at[1, d], "w")
            net.when(arrival, complete[1])

        net.when(net.copy(far.at[d, :, mine], other.at[d], other.at[d], "z"), add)

    def near_landed(d):
        def add():
            found[0, d] = near[d, :, mine] + partial[d]
            net.spend(0.2)
            complete[0]()

        net.when(net.copy(near.at[d, :, theirs], partial.at[d], partial.at[d], "z"), add)

    complete = [counted(4, functools.partial(send, index)) for index in range(2)]
    far_counts = {d: counted(1 if d == 0 else 2, functools.partial(far_landed, d)) for d in range(4)}
    near_counts = {d: counted(1 if d == 0 else 2, functools.partial(near_landed, d)) for d in range(4)}
    second = y_exchange(net, chunks(parts.at[0]), chunks(near), y_relay.at[0], lambda d: near_counts[d]())
    go = counted(2, lambda: start_all(second))
    first = y_exchange(net, chunks(parts.at[1]), chunks(far), y_relay.at[1], lambda d: far_counts[d](), go)
    steps = []
    reduce_scatter(net, fill, terms, rest[17:-2], finish_dense, 0, steps.append)
    steps[0]()
    net.spend(1.6)
    for j in range(tiles):
        expert_up(j)
    for j in range(tiles):
        expert_down(1, j)
    start_all(first)
    for j in range(tiles):
        expert_down(0, j)
    go()
    for step in steps[1:]:
        step()
        net.spend(1.6)
    net.run()


def tail(collective_id, units, down, rows, expert_in, expert_out, pick, hidden):
    size, width = hidden.shape
    count = rows.shape[3]
    full, part = (4, 2, count, width), (4, 2, count // 2, width)
    depth, inside = expert_in.shape
    span = min(512, width)
    sixteen = lambda *shape: pltpu.VMEM(shape, hidden.dtype)
    scratch = [
        sixteen(8 * size, width),
        sixteen(2 * size, units.shape[1]),
        sixteen(*full),
        sixteen(*part),
        sixteen(*part),
        sixteen(*full),
        sixteen(*part),
        sixteen(2, *part),
        sixteen(2, 4 * count, width),
        sixteen(2, 2, count // 2, width),
        sixteen(2, 2, count, width),
        sixteen(2, 4 * count, width),
        pltpu.VMEM((size, width), jnp.float32),
        sixteen(2, *full),
        sixteen(2, 8 * count, inside),
        sixteen(2, width // span, depth, span),
        pltpu.SemaphoreType.DMA((2, width // span)),
    ]
    return communicate(
        "tail",
        tail_body,
        collective_id,
        (units, down, rows, expert_in, expert_out, pick, hidden),
        [jax.ShapeDtypeStruct(hidden.shape, hidden.dtype)],
        scratch + scatter_scratch(size, width, hidden.dtype, 0),
        24 + 2 * 10 + 12 + 12,
        outside=(3, 4),
    )


def layer_norm(row_data, gain_vector):
    row_data = row_data.astype(jnp.float32)
    centered = row_data - jnp.mean(row_data, axis=-1, keepdims=True)
    spread = jnp.mean(centered * centered, axis=-1, keepdims=True)
    return centered * lax.rsqrt(spread + 1e-06) * gain_vector


def matmul(a, b):
    return jnp.dot(a, b, preferred_element_type=jnp.float32)


def shards(
    tokens,
    ln1_gain,
    qkv_weight,
    out_weight,
    ln2_gain,
    ffn_in,
    ffn_out,
    expert_ids,
    expert_in,
    expert_out,
):
    tok_count, model_width = tokens.shape
    row_total = lax.axis_size("row")
    col_total = lax.axis_size("col")
    row_index = lax.axis_index("row")
    col_index = lax.axis_index("col")
    expert_count = row_total * col_total // 2
    capacity = max(2, 2 * tok_count // expert_count)
    head_count, head_dim = qkv_weight.shape[1], qkv_weight.shape[3]
    seq_len = tok_count * col_total

    ids = expert_ids[:, 0]
    token = jnp.arange(tok_count, dtype=jnp.int32)
    same = (expert_ids == ids[None, :]) & (token[:, None] < token[None, :])
    codes = ids * capacity + jnp.sum(same.astype(jnp.int32), axis=0)
    image_rows, codes_all, qkv_whole, out_whole = exchange(
        "enter",
        0,
        spreads=(tokens,),
        smalls=(jnp.broadcast_to(codes[None, :], (8, tok_count)),),
        gathers=((qkv_weight.reshape(qkv_weight.shape[0], -1), 0), (out_weight, 1)),
    )
    normed = layer_norm(image_rows, ln1_gain).astype(jnp.bfloat16)
    projected = matmul(normed, qkv_whole).astype(jnp.bfloat16)
    codes_all = codes_all.reshape(col_total, 8, tok_count)[:, 0]
    ids_rows, slot_index = codes_all // capacity, codes_all % capacity
    block = jnp.arange(col_total, dtype=jnp.int32)[:, None]
    plane, place = block // 4, block % 4 * capacity + slot_index
    home_row = 2 * ids_rows // col_total
    mine = (2 * ids_rows % col_total) // 2 == col_index // 2
    other = (home_row // 8 != row_index // 8).astype(jnp.int32)
    chunk = (home_row // 2 - row_index // 2 + 8) % 4 * 2 + home_row % 2
    half = 4 * capacity
    rows = 2 * half
    slot_count = row_total * rows
    position = jnp.where(mine, (other * 8 + chunk) * half + place, -1).reshape(1, seq_len)
    position = jnp.broadcast_to(position, (8, seq_len))
    home = ids // 4
    turn = (home // 2 - row_index // 2 + 8) % 4 * 2 + home % 2
    found = (col_index // 2 - ids % 4 + 4) % 4 * rows + turn * capacity + codes % capacity
    found = jnp.where(home // 8 != row_index // 8, found + 4 * rows, found)
    pick = (found[:, None] == jnp.arange(8 * rows, dtype=jnp.int32)[None, :]).astype(jnp.bfloat16)

    hidden_mine, down_whole, hidden_units, expert_rows = middle(
        1, head_count, projected, out_whole, tokens, ln2_gain[None, :], ffn_in, ffn_out, position, rows
    )
    (out,) = tail(2, hidden_units, down_whole, expert_rows, expert_in[0], expert_out[0], pick, hidden_mine)
    return out


def solution(mesh):
    in_specs = (
        P(("row", "col"), None),
        P(),
        P("row", "col", None, None),
        P("col", "row"),
        P(),
        P("row", "col"),
        P("col", "row"),
        P(("row", "col"), None),
        P(("row", "col"), None, None),
        P(("row", "col"), None, None),
    )
    out_specs = P(("row", "col"), None)
    return jax.shard_map(shards, mesh=mesh, in_specs=in_specs, out_specs=out_specs, check_vma=False)
```

```python
import functools
import heapq
import math
import jax
import jax.numpy as jnp
from jax import lax
from jax.experimental import pallas as pl
from jax.experimental.pallas import tpu as pltpu
from jax.sharding import PartitionSpec as P

MESH = pl.DeviceIdType.MESH
SPLIT = 32


class Net:
    def __init__(self, send, recv):
        row, col = lax.axis_index("row"), lax.axis_index("col")
        self.row, self.col = row, col
        self.high, self.y, self.core = row // 8, lax.rem(row // 2, 4), lax.rem(row, 2)
        self.x, self.low = col // 2, lax.rem(col, 2)
        self.send, self.recv = send, recv
        self.count = 0
        self.finish = []
        self.queue = []
        self.serial = 0
        self.now = 0.0
        self.free = {}
        self.spare = []

    def row_of(self, high, y, core):
        return high * 8 + lax.rem(y + 8, 4) * 2 + core

    def col_of(self, x, low):
        return lax.rem(x + 8, 4) * 2 + low

    def block_of(self, x, low):
        return low * 4 + lax.rem(x + 8, 4)

    def peer(self, name):
        high, y, core, x, low = self.high, self.y, self.core, self.x, self.low
        at = {
            "x+": (high, y, core, x + 1, low),
            "x-": (high, y, core, x - 1, low),
            "z": (high, y, core, x, 1 - low),
            "y+": (high, y + 1, core, x, low),
            "y-": (high, y - 1, core, x, low),
            "w": (1 - high, y, core, x, 1 - low),
            "c": (high, y, 1 - core, x, low),
            "y+c": (high, y + 1, 1 - core, x, low),
            "y-c": (high, y - 1, 1 - core, x, low),
        }[name]
        return self.row_of(*at[:3]), self.col_of(*at[3:])

    def greet(self, names):
        barrier = pltpu.get_barrier_semaphore()
        for name in names:
            pl.semaphore_signal(barrier, inc=1, device_id=self.peer(name), device_id_type=MESH)
        pl.semaphore_wait(barrier, len(names))

    def copy(self, src, dst, arriving, name):
        k = self.count
        self.count += 1
        make = lambda target: pltpu.make_async_remote_copy(
            src, target, self.send.at[k], self.recv.at[k], device_id=self.peer(name), device_id_type=MESH
        )
        out, arrival = make(dst), make(arriving)
        out.start()
        self.finish.append(out)
        rate, delay = (600e3, 1.0) if name == "c" else (46e3, 2.0)
        begin = max(self.now, self.free.get(name[:2], 0.0))
        self.free[name[:2]] = begin + math.prod(arriving.shape) * arriving.dtype.itemsize / rate
        return arrival, self.free[name[:2]] + delay

    def when(self, pending, action=None):
        arrival, time = pending

        def run():
            arrival.wait_recv()
            if action is not None:
                action()

        heapq.heappush(self.queue, (time, self.serial, run))
        self.serial += 1

    def work(self, time, action):
        self.spare.append((time, action))

    def spend(self, time):
        self.now += time

    def run(self):
        while self.queue or self.spare:
            if self.spare and (not self.queue or self.queue[0][0] > self.now + 0.5 * self.spare[0][0]):
                time, action = self.spare.pop(0)
                action()
                self.now += time
                continue
            time, _, action = heapq.heappop(self.queue)
            self.now = max(self.now, time) + 0.02
            action()
        for out in self.finish:
            out.wait_send()


def rows_of(ref, start, size, step=16):
    return ref.at[pl.ds(pl.multiple_of(start, step), size)]


def counted(count, action):
    left = [count]

    def step():
        left[0] -= 1
        if left[0] == 0:
            action()

    return step


def spread(net, src, out, plane_done=lambda: None, done=lambda: None):
    size = src.shape[0]
    a, half_a, half_b = SPLIT, SPLIT // 2, (size - SPLIT) // 2
    b = size - a
    x, low = net.x, net.low
    mine = counted(8, plane_done)
    theirs = counted(12, done)
    sides = ((-1, "x+", 0), (1, "x-", 1))

    def part(dx, other, start, rows):
        plane = 1 - low if other else low
        return rows_of(out, net.block_of(x + dx, plane) * size + start, rows)

    def own(start, rows):
        return src.at[pl.ds(start, rows)]

    def to_z(dx, start, rows):
        got = part(dx, 0, start, rows)
        net.when(net.copy(got, got, part(dx, 1, start, rows), "z"), theirs)

    def onward(dx, forward, other, start, rows, then):
        got = part(dx, other, start, rows)
        net.when(net.copy(got, got, part(2, other, start, rows), forward), then)

    def from_a(dx, forward, index):
        mine()

        def far():
            mine()
            to_z(2, index * half_a, half_a)

        onward(dx, forward, 0, index * half_a, half_a, far)
        to_z(dx, 0, a)

    def from_b(dx, forward, index):
        mine()
        onward(dx, forward, 0, a + index * half_b, half_b, mine)
        later()

    def partner(index, half, then):
        dx, forward, _ = sides[index]
        got = part(0, 1, a + half * half_b, half_b)
        net.when(net.copy(got, got, part(dx, 1, a + half * half_b, half_b), forward), then)

    def from_z():
        theirs()
        for dx, forward, index in sides:

            def first(dx=dx, forward=forward, index=index):
                theirs()
                onward(dx, forward, 1, a + index * half_b, half_b, theirs)

            partner(index, index, first)
        later()

    def second():
        for _, _, index in sides:
            partner(index, 1 - index, theirs)

    later = counted(3, second)
    net.when(net.copy(own(a, b), part(0, 0, a, b), part(0, 1, a, b), "z"), from_z)
    for start, rows, action in ((0, a, from_a), (a, b, from_b)):
        for dx, forward, index in sides:
            arrival = net.copy(own(start, rows), part(0, 0, start, rows), part(dx, 0, start, rows), forward)
            net.when(arrival, functools.partial(action, dx, forward, index))
    net.when(net.copy(own(0, a), part(0, 0, 0, a), part(0, 1, 0, a), "z"), theirs)
    out[pl.ds(pl.multiple_of(net.block_of(x, low) * size, size), size), :] = src[...]


def spread_small(net, src, out):
    size = src.shape[0]
    x, low = net.x, net.low

    def part(dx, other):
        plane = 1 - low if other else low
        return rows_of(out, net.block_of(x + dx, plane) * size, size, 8)

    def onward(other):
        got = part(-1, other)
        net.when(net.copy(got, got, part(-2, other), "x+"))

    def around(other, got):
        arrival = net.copy(got, part(0, other), part(-1, other), "x+")
        net.when(arrival, lambda: onward(other))
        net.when(net.copy(got, part(0, other), part(1, other), "x-"))

    around(0, src)
    arrival = net.copy(src, part(0, 0), part(0, 1), "z")
    net.when(arrival, lambda: around(1, part(0, 1)))
    out[pl.ds(pl.multiple_of(net.block_of(x, net.low) * size, size), size), :] = src[...]


def gather(net, src, out, relay, axis, done=lambda: None):
    depth, width = src.shape
    high, y, core = net.high, net.y, net.core
    middle = depth // 2
    landed = counted(10, done)

    def part(dy, other, core, half=None):
        index = net.row_of(1 - high if other else high, y + dy, core)
        start, size = (0, depth) if half is None else (half * middle, middle)
        if axis == 0:
            return rows_of(out, index * depth + start, size)
        return out.at[pl.ds(start, size), pl.ds(pl.multiple_of(index * width, width), width)]

    def to_core(dy, other, half=None):
        got = part(dy, other, core, half)
        net.when(net.copy(got, got, part(dy, other, 1 - core, half), "c"), landed)

    def from_y(dy, other):
        got = part(dy, other, core, 0 if dy < 0 else 1)
        forward = "y+" if dy < 0 else "y-"
        half = 0 if dy < 0 else 1
        arrival = net.copy(got, got, part(2, other, core, half), forward)
        net.when(arrival, lambda: to_core(2, other, half))
        to_core(dy, other)

    def around(other, got):
        for dy, forward in ((-1, "y+"), (1, "y-")):
            arrival = net.copy(got, part(0, other, core), part(dy, other, core), forward)
            net.when(arrival, lambda dy=dy: from_y(dy, other))

    around(0, src)
    waiting = [2]

    def arrived():
        waiting[0] -= 1
        if waiting[0] == 0:
            around(1, part(0, 1, core))
            to_core(0, 1)

    for half, first, second in ((0, "z", "w"), (1, "w", "z")):
        arrival = net.copy(src.at[pl.ds(half * middle, middle)], relay.at[half], relay.at[half], first)

        def onward(half=half, second=second):
            got = relay.at[half]
            arrival = net.copy(got, part(0, half, core, half), part(0, 1, core, half), second)
            net.when(arrival, arrived)

        net.when(arrival, onward)
    mine = part(0, 0, core)
    net.when(net.copy(src, mine, part(0, 0, 1 - core), "c"), landed)
    index = net.row
    if axis == 0:
        out[pl.ds(pl.multiple_of(index * depth, depth), depth), :] = src[...]
    else:
        out[:, pl.ds(pl.multiple_of(index * width, width), width)] = src[...]


def reduce_scatter(net, fill, src, scratch, finish, split, step=lambda action: action(), gate=lambda action: action()):
    far_b, near_b, acc_b, plane, last = scratch[:5]
    if split:
        from_z, sums, far_a, near_a, acc_a = scratch[5:]
    size = src.shape[0] // 8
    a = split
    b = size - a
    x, low = net.x, net.low

    def rows(dx, other, start, count):
        index = net.block_of(x + dx, 1 - low if other else low)
        return pl.ds(pl.multiple_of(index * size + start, 16), count)

    def ring(block, count, far, near, acc, done):
        half = count // 2
        halves = {"x+": (0, half), "x-": (half, half)}
        waiting = [4]

        def arrived():
            waiting[0] -= 1
            if waiting[0] == 0:
                done()

        def start_far():
            for index, forward in ((0, "x+"), (1, "x-")):
                first = halves[forward][0]
                arrival = net.copy(block(2, first, half), far.at[index], far.at[index], forward)

                def add(index=index, forward=forward, first=first):
                    need(3)
                    term = block(1 if forward == "x+" else -1, first, half)
                    acc[index] = far[index] + term[...]
                    net.spend(0.1)
                    dst = near.at[index, pl.ds(first, half)]
                    net.when(net.copy(acc.at[index], dst, dst, forward), arrived)

                net.when(arrival, add)

        def start_direct():
            for index, forward in ((0, "x+"), (1, "x-")):
                first = half - halves[forward][0]
                dst = near.at[index, pl.ds(first, half)]
                term = block(1 if forward == "x+" else -1, first, half)
                net.when(net.copy(term, dst, dst, forward), arrived)

        return start_far, start_direct

    def block_b(other):
        return lambda dx, first, count: src.at[rows(dx, other, a + first, count)]

    def block_a(dx, first, count):
        return sums.at[pl.ds((dx % 4) * a + first, count)]

    left = [4]
    both = [3 if a else 2]
    wide = lambda value: value.astype(jnp.float32)

    def from_partner(k):
        need(4)
        sums[pl.ds(k * a, a), :] = from_z[pl.ds(k * a, a), :] + src[rows(k, 0, 0, a), :]
        net.spend(0.1)
        left[0] -= 1
        if left[0] == 0:
            for start in ring(block_a, a, far_a, near_a, acc_a, arrived):
                start()

    def to_partner(k):
        if a == 0:
            return
        landing = from_z.at[pl.ds(k * a, a)]
        net.when(net.copy(src.at[rows(k, 1, 0, a)], landing, landing, "z"), lambda: from_partner(k))

    def plane_done():
        need(4)
        total = wide(near_b[0, 0]) + wide(near_b[0, 1]) + wide(src[rows(0, 1, a, b), :])
        plane[...] = total.astype(plane.dtype)
        net.spend(0.3)
        gate(lambda: net.when(net.copy(plane, last, last, "z"), arrived))

    def arrived():
        both[0] -= 1
        if both[0]:
            return
        if a:
            finish(0, wide(near_a[0]) + wide(near_a[1]) + wide(sums[pl.ds(0, a), :]))
        total = wide(near_b[1, 0]) + wide(near_b[1, 1]) + wide(src[rows(0, 0, a, b), :]) + wide(last[...])
        net.spend(0.5)
        finish(a, total)

    far_other, direct_other = ring(block_b(1), b, far_b.at[0], near_b.at[0], acc_b.at[0], plane_done)
    far_own, direct_own = ring(block_b(0), b, far_b.at[1], near_b.at[1], acc_b.at[1], arrived)
    def first():
        fill(lambda i: net.block_of(x + 2, lax.rem(low + 1 + i, 2)))
        far_other()
        far_own()
        to_partner(2)

    def second():
        fill(lambda i: net.block_of(x + 1 - 2 * i, 1 - low))
        direct_other()
        to_partner(1)
        to_partner(3)

    def third():
        fill(lambda i: net.block_of(x + 1 - 2 * i, low))
        direct_own()

    def fourth():
        fill(lambda i: net.block_of(x, lax.rem(low + 1 + i, 2)))
        to_partner(0)

    actions = [first, second, third, fourth]

    def need(number):
        while len(actions) > 4 - number:
            actions.pop(0)()

    for number in range(1, 5):
        step(lambda number=number: need(number))


def scatter_scratch(size, width, dtype, split):
    a, b = split, size - split
    shapes = [(2, 2, b // 2, width), (2, 2, b, width), (2, 2, b // 2, width), (b, width), (b, width)]
    if a:
        shapes += [(4 * a, width), (4 * a, width), (2, a // 2, width), (2, a, width), (2, a // 2, width)]
    return [pltpu.VMEM(shape, dtype) for shape in shapes]


def comm_body(spreads, smalls, gathers, *refs):
    count = spreads + smalls + len(gathers)
    ins, outs, relays = refs[:count], refs[count : 2 * count], refs[2 * count : -2]
    net = Net(*refs[-2:])
    net.greet(["x+", "x-", "z", "y+", "y-", "w", "c"])
    for k in range(spreads):
        spread(net, ins[k], outs[k])
    for k in range(spreads, spreads + smalls):
        spread_small(net, ins[k], outs[k])
    for i, axis in enumerate(gathers):
        k = spreads + smalls + i
        gather(net, ins[k], outs[k], relays[i], axis)
    net.run()


def communicate(name, body, collective_id, arrays, shapes, scratch, copies, outside=(), spare=6 * 2**20):
    used = sum(math.prod(r.shape) * jnp.dtype(r.dtype).itemsize for r in scratch if r.memory_space == pltpu.VMEM)
    spaces = [pl.ANY if i in outside else pltpu.VMEM for i in range(len(arrays))]
    return pl.pallas_call(
        body,
        out_shape=shapes,
        in_specs=[pl.BlockSpec(memory_space=space) for space in spaces],
        out_specs=[pl.BlockSpec(memory_space=pltpu.VMEM)] * len(shapes),
        scratch_shapes=scratch + [pltpu.SemaphoreType.DMA((copies,)), pltpu.SemaphoreType.DMA((copies,))],
        compiler_params=pltpu.CompilerParams(
            collective_id=collective_id, has_side_effects=True, vmem_limit_bytes=min(used + spare, 62 * 2**20)
        ),
        name=name,
    )(*arrays)


def gathered(array, axis):
    depth, width = array.shape
    total = lax.axis_size("row")
    shape = (depth * total, width) if axis == 0 else (depth, width * total)
    return jax.ShapeDtypeStruct(shape, array.dtype)


def relay_of(array):
    return pltpu.VMEM((2, array.shape[0] // 2, array.shape[1]), array.dtype)


def exchange(name, collective_id, spreads=(), smalls=(), gathers=()):
    whole = [jax.ShapeDtypeStruct((8 * a.shape[0], a.shape[1]), a.dtype) for a in (*spreads, *smalls)]
    return communicate(
        name,
        functools.partial(comm_body, len(spreads), len(smalls), [axis for _, axis in gathers]),
        collective_id,
        [*spreads, *smalls, *(array for array, _ in gathers)],
        whole + [gathered(*pair) for pair in gathers],
        [relay_of(array) for array, _ in gathers],
        22 * len(spreads) + 8 * len(smalls) + 22 * len(gathers),
    )


def block_body(heads, qkv, weight, tokens, gain, up, down, position, expert_in, expert_out, pick, result, *rest):
    terms, mixed, normed, image, up_whole, table, far, y_relay, up_relay, down_relay = rest[:10]
    hidden, down_whole, units, out, pair, weights, fetched = rest[10:17]
    held, _, span = weights.shape
    tiles = expert_in.shape[1] // span
    fetches = []

    def fetch():
        t = len(fetches)
        if t == 3 * tiles:
            return
        source = expert_in if t < tiles else expert_out
        tile = source.at[:, pl.ds(t % tiles * span, span)]
        copy = pltpu.make_async_copy(tile, weights.at[t % held], fetched.at[t])
        copy.start()
        fetches.append(copy)

    for _ in range(held):
        fetch()
    net = Net(*rest[-2:])
    net.greet(["x+", "x-", "z", "y+", "y-", "w", "c", "y+c", "y-c"])
    size = tokens.shape[0]
    dim = qkv.shape[1] // (3 * heads)
    low = net.low
    slots = out.shape[3] // 2
    mine = pl.ds(pl.multiple_of(low * slots, slots), slots)
    theirs = pl.ds(pl.multiple_of((1 - low) * slots, slots), slots)

    def fill(column):
        @pl.loop(0, 2)
        def _(i):
            at = pl.ds(pl.multiple_of(column(i) * size, size), size)

            @pl.loop(0, heads)
            def _(h):
                part = lambda k: pl.ds(pl.multiple_of((3 * h + k) * dim, dim), dim)
                scores = lax.dot_general(
                    qkv[at, part(0)], qkv[:, part(1)], (((1,), (1,)), ((), ())), preferred_element_type=jnp.float32
                )
                scale = dim ** (-0.5) * math.log2(math.e)
                chances = jnp.exp2((scores - jnp.max(scores, axis=-1, keepdims=True)) * scale)
                total = jnp.sum(chances, axis=-1, keepdims=True)
                value = matmul(chances.astype(jnp.bfloat16), qkv[:, part(2)]) / total
                mixed[:, pl.ds(pl.multiple_of(h * dim, dim), dim)] = value.astype(jnp.bfloat16)

            @pl.loop(0, weight.shape[1] // 512)
            def _(j):
                columns = pl.ds(pl.multiple_of(j * 512, 512), 512)
                terms[at, columns] = matmul(mixed[...], weight[:, columns]).astype(jnp.bfloat16)

        net.spend(2.6)

    def fill_dense(column):
        while early:
            early.pop().wait_send()
        at = [pl.ds(pl.multiple_of(column(i) * size, size), size) for i in range(2)]
        for i in range(2):
            pair[pl.ds(i * size, size), :] = units[at[i], :]

        @pl.loop(0, down_whole.shape[1] // 512)
        def _(j):
            columns = pl.ds(pl.multiple_of(j * 512, 512), 512)
            product = matmul(pair[...], down_whole[:, columns]).astype(jnp.bfloat16)
            for i in range(2):
                terms[at[i], columns] = product[i * size : (i + 1) * size]

    def place(index, plane):
        rows = pl.ds(pl.multiple_of(plane * 4 * size, 4 * size), 4 * size)
        flat = math.prod(table.shape[1:5])
        here = lax.broadcasted_iota(jnp.int32, (flat, 4 * size), 0) == position[pl.ds(0, 1), rows]
        placing = jnp.where(here, 1.0, 0.0).astype(jnp.bfloat16)
        span = 512

        @pl.loop(0, image.shape[1] // span)
        def _(j):
            columns = pl.ds(pl.multiple_of(j * span, span), span)
            put = matmul(placing, image[rows, columns]).astype(jnp.bfloat16)
            table[index, :, :, :, :, columns] = put.reshape(table.shape[1:5] + (span,))

        net.spend(1.2)

    def plane_done():
        place(0, low)

        def from_w(d):
            got = far.at[d, :, theirs]
            arrival = net.copy(got, got, far.at[d, :, mine], "z")
            net.when(arrival, last[d])
            first[d]()

        for d in (2, 1, 3, 0):
            arrival = net.copy(table.at[0, 1, d], far.at[d, :, mine], far.at[d, :, theirs], "w")
            net.when(arrival, functools.partial(from_w, d))
        start_all(own)
        ready()

    def image_done():
        place(1, 1 - low)
        start_all(other)
        ready()

    finish_dense, start_expert, gate = returning(
        net, out, pick, hidden, result, weights, fetches, fetch, *rest[17:30]
    )
    dispatched = counted(28, start_expert)
    came = lambda d: dispatched()
    own = y_exchange(net, chunks(table.at[0, 0]), chunks(out.at[0], mine), y_relay.at[0], came)
    first = y_exchange(net, chunks(far, theirs), chunks(out.at[1], theirs), y_relay.at[1], came)
    last = y_exchange(net, chunks(far, mine), chunks(out.at[1], mine), y_relay.at[2], came)
    other = y_exchange(net, chunks(table.at[1, 0]), chunks(out.at[0], theirs), y_relay.at[3], came)
    early = []

    def dense():
        up_tasks(net, image, up_whole, units)
        reduce_scatter(net, fill_dense, terms, rest[30:40], finish_dense, 32, lambda action: net.work(1.4, action), gate)

    ready = counted(4, dense)

    def finish(start, total):
        at = pl.ds(start, total.shape[0])
        state = (tokens[at, :].astype(jnp.float32) + total).astype(jnp.bfloat16)
        hidden[at, :] = state
        normed[at, :] = layer_norm(state, gain[...]).astype(jnp.bfloat16)
        if start == 0:
            return
        early.extend(net.finish)
        net.finish.clear()
        net.spend(0.5)
        spread(net, normed, image, plane_done, image_done)

    gather(net, up, up_whole, up_relay, 0, ready)
    gather(net, down, down_whole, down_relay, 1, ready)
    reduce_scatter(net, fill, terms, rest[40:-2], finish, SPLIT)
    net.run()


def whole_block(collective_id, heads, qkv, weight, tokens, gain, up, down, position, expert_in, expert_out, pick, slots):
    size, width = tokens.shape
    depth, inside = expert_in.shape
    span = min(512, width)
    full, part = (4, 2, slots, width), (4, 2, slots // 2, width)
    sixteen = lambda *shape: pltpu.VMEM(shape, tokens.dtype)
    scratch = [
        sixteen(8 * size, width),
        sixteen(size, weight.shape[0]),
        sixteen(size, width),
        sixteen(8 * size, width),
        sixteen(*gathered(up, 0).shape),
        sixteen(2, 2, *part),
        sixteen(*full),
        sixteen(4, 2, slots // 2, width),
        relay_of(up),
        relay_of(down),
        sixteen(size, width),
        sixteen(*gathered(down, 1).shape),
        sixteen(8 * size, up.shape[1]),
        sixteen(2, *full),
        sixteen(2 * size, up.shape[1]),
        sixteen(3, depth, span),
        pltpu.SemaphoreType.DMA((3 * (width // span),)),
        sixteen(*full),
        sixteen(*part),
        sixteen(*part),
        sixteen(*full),
        sixteen(*part),
        sixteen(2, *part),
        sixteen(2, 4 * slots, width),
        sixteen(2, 2, slots // 2, width),
        sixteen(2, 2, slots, width),
        sixteen(2, 4 * slots, width),
        pltpu.VMEM((size, width), jnp.float32),
        sixteen(2, *full),
        sixteen(2, 8 * slots, inside),
    ]
    scratch += scatter_scratch(size, width, tokens.dtype, 32) + scatter_scratch(size, width, tokens.dtype, SPLIT)
    return communicate(
        "block",
        functools.partial(block_body, heads),
        collective_id,
        (qkv, weight, tokens, gain, up, down, position, expert_in, expert_out, pick),
        [jax.ShapeDtypeStruct(tokens.shape, tokens.dtype)],
        scratch,
        24 + 22 + 2 * 22 + 8 + 4 * 10 + 24 + 2 * 10 + 12 + 12,
        outside=(7, 8),
        spare=7 * 2**20,
    )


def y_exchange(net, src, dst, relay, arrived=lambda d: None, then=lambda: None):
    core = net.core
    forwarded = counted(2, then)

    def opposite():
        for index, c, forward, last in ((0, core, "y+", "y+"), (1, 1 - core, "y-", "y-c")):

            def onward(index=index, c=c, last=last):
                arrival = net.copy(relay.at[index], dst(2, core), dst(2, c), last)
                net.when(arrival, lambda: arrived(2))
                forwarded()

            net.when(net.copy(src(2, c), relay.at[index], relay.at[index], forward), onward)

    def beside(d):
        forward = "y+" if d == 1 else "y-"
        for c, name in ((core, forward), (1 - core, forward + "c")):
            net.when(net.copy(src(d, c), dst(4 - d, core), dst(4 - d, c), name), lambda: arrived(4 - d))

    def here():
        net.when(net.copy(src(0, 1 - core), dst(0, core), dst(0, 1 - core), "c"), lambda: arrived(0))
        dst(0, core)[...] = src(0, core)[...]

    return {2: opposite, 1: lambda: beside(1), 3: lambda: beside(3), 0: here}


def chunks(ref, *rest):
    return lambda d, c: ref.at[(d, c, *rest)]


def start_all(steps):
    for d in (2, 1, 3, 0):
        steps[d]()


def up_tasks(net, x_ref, w_ref, out):
    rows, width = out.shape
    tile = min(256, rows)
    span = min(256, width)

    def piece(j):
        columns = pl.ds(j * span, span)

        @pl.loop(0, rows // tile)
        def _(i):
            at = pl.ds(pl.multiple_of(i * tile, tile), tile)
            inner = jnp.dot(x_ref[at, :], w_ref[:, columns], preferred_element_type=jnp.float32)
            out[at, columns] = (inner * (1.0 + lax.erf(inner * (0.5**0.5))) * 0.5).astype(out.dtype)

    for j in range(width // span):
        net.work(1.6, lambda j=j: piece(j))


def returning(net, rows, pick, hidden, out, weights, fetches, fetch, *rest):
    far, other, total, near, partial, found, packed, relay, y_relay = rest[:9]
    arrived_rows, dense, parts, inner = rest[9:13]
    held, _, span = weights.shape
    tiles = inner.shape[2] // span
    low = net.low
    half = parts.shape[3] // 2
    mine, theirs = pl.ds(pl.multiple_of(low * half, half), half), pl.ds(pl.multiple_of((1 - low) * half, half), half)
    count = packed.shape[1] // 4

    def pack(index):
        flat = math.prod(found.shape[1:4])
        row = lax.broadcasted_iota(jnp.int32, (count, flat), 0)
        slot = lax.broadcasted_iota(jnp.int32, (count, flat), 1)
        each = half // 4
        same = (row // each == slot // half) & (row % each == slot % each)
        for k in range(4):
            chosen = same & (slot % half // each == lax.rem(net.x + k, 4))
            chosen = jnp.where(chosen, 1.0, 0.0).astype(jnp.bfloat16)

            @pl.loop(0, found.shape[4] // 512)
            def _(j):
                columns = pl.ds(pl.multiple_of(j * 512, 512), 512)
                rows = found[index, :, :, :, columns].reshape(flat, 512)
                value = matmul(chosen, rows).astype(jnp.bfloat16)
                packed[index, k * count : (k + 1) * count, columns] = value

        net.spend(0.6)

    def send(index):
        pack(index)
        at = lambda k, first=0, rows=count: packed.at[index, pl.ds(k * count + first, rows)]
        place = lambda k, first=0, rows=count: arrived_rows.at[index, pl.ds(k * count + first, rows)]
        middle = count // 2
        for i, forward in ((0, "x+"), (1, "x-")):

            def onward(i=i, forward=forward):
                dst = place(2, i * middle, middle)
                net.when(net.copy(relay.at[index, i], dst, dst, forward), landed)

            net.when(net.copy(at(2, i * middle, middle), relay.at[index, i], relay.at[index, i], forward), onward)
        for k, forward in ((1, "x+"), (3, "x-")):
            net.when(net.copy(at(k), place(k), place(k), forward), landed)

    flat_rows = math.prod(parts.shape[1:4])

    def expert_up(j):
        fetches[j].wait()

        @pl.loop(0, 2)
        def _(i):
            value = matmul(rows[i].reshape(flat_rows, rows.shape[4]), weights[j % held])
            value = value * (1.0 + lax.erf(value * (0.5**0.5))) * 0.5
            inner[i, :, pl.ds(j * span, span)] = value.astype(inner.dtype)

        fetch()

    def expert_down(i, j):
        t = (2 - i) * tiles + j
        fetches[t].wait()
        value = matmul(inner[i], weights[t % held]).astype(parts.dtype)
        parts[i, :, :, :, pl.ds(j * span, span)] = value.reshape(parts.shape[1:4] + (span,))
        fetch()

    def finish_dense(start, total):
        dense[pl.ds(start, total.shape[0]), :] = total
        if start:
            ready()

    def combine():
        flat = 4 * count
        for index in range(2):
            arrived_rows[index, pl.ds(0, count), :] = packed[index, pl.ds(0, count), :]

        @pl.loop(0, out.shape[1] // 512)
        def _(j):
            columns = pl.ds(pl.multiple_of(j * 512, 512), 512)
            value = hidden[:, columns].astype(jnp.float32) + dense[:, columns]
            for index in range(2):
                value += matmul(pick[:, pl.ds(index * flat, flat)], arrived_rows[index, :, columns])
            out[:, columns] = value.astype(jnp.bfloat16)

    ready = counted(9, combine)
    landed = ready

    def far_landed(d):
        def add():
            total[d] = far[d, :, theirs] + other[d]
            net.spend(0.2)
            arrival = net.copy(total.at[d], found.at[1, d], found.at[1, d], "w")
            net.when(arrival, complete[1])

        net.when(net.copy(far.at[d, :, mine], other.at[d], other.at[d], "z"), add)

    pending = []
    held_back = counted(5, lambda: pending.pop()())

    def gate(action):
        pending.append(action)
        held_back()

    def near_landed(d):
        def add():
            found[0, d] = near[d, :, mine] + partial[d]
            net.spend(0.2)
            complete[0]()

        net.when(net.copy(near.at[d, :, theirs], partial.at[d], partial.at[d], "z"), add)
        held_back()

    complete = [counted(4, functools.partial(send, index)) for index in range(2)]
    far_counts = {d: counted(1 if d == 0 else 2, functools.partial(far_landed, d)) for d in range(4)}
    near_counts = {d: counted(1 if d == 0 else 2, functools.partial(near_landed, d)) for d in range(4)}
    second = y_exchange(net, chunks(parts.at[0]), chunks(near), y_relay.at[0], lambda d: near_counts[d]())
    go = counted(2, lambda: start_all(second))
    first = y_exchange(net, chunks(parts.at[1]), chunks(far), y_relay.at[1], lambda d: far_counts[d](), go)

    def start():
        for j in range(tiles):
            net.work(1.2, functools.partial(expert_up, j))
        for i, after in ((1, lambda: start_all(first)), (0, go)):
            for j in range(tiles):
                net.work(0.6, functools.partial(expert_down, i, j))
            net.work(0.0, after)

    return finish_dense, start, gate


def layer_norm(row_data, gain_vector):
    row_data = row_data.astype(jnp.float32)
    centered = row_data - jnp.mean(row_data, axis=-1, keepdims=True)
    spread = jnp.mean(centered * centered, axis=-1, keepdims=True)
    return centered * lax.rsqrt(spread + 1e-06) * gain_vector


def matmul(a, b):
    return jnp.dot(a, b, preferred_element_type=jnp.float32)


def shards(
    tokens,
    ln1_gain,
    qkv_weight,
    out_weight,
    ln2_gain,
    ffn_in,
    ffn_out,
    expert_ids,
    expert_in,
    expert_out,
):
    tok_count, model_width = tokens.shape
    row_total = lax.axis_size("row")
    col_total = lax.axis_size("col")
    row_index = lax.axis_index("row")
    col_index = lax.axis_index("col")
    expert_count = row_total * col_total // 2
    capacity = max(2, 2 * tok_count // expert_count)
    head_count, head_dim = qkv_weight.shape[1], qkv_weight.shape[3]
    seq_len = tok_count * col_total

    ids = expert_ids[:, 0]
    token = jnp.arange(tok_count, dtype=jnp.int32)
    same = (expert_ids == ids[None, :]) & (token[:, None] < token[None, :])
    codes = ids * capacity + jnp.sum(same.astype(jnp.int32), axis=0)
    image_rows, codes_all, qkv_whole, out_whole = exchange(
        "enter",
        0,
        spreads=(tokens,),
        smalls=(jnp.broadcast_to(codes[None, :], (8, tok_count)),),
        gathers=((qkv_weight.reshape(qkv_weight.shape[0], -1), 0), (out_weight, 1)),
    )
    normed = layer_norm(image_rows, ln1_gain).astype(jnp.bfloat16)
    projected = matmul(normed, qkv_whole).astype(jnp.bfloat16)
    codes_all = codes_all.reshape(col_total, 8, tok_count)[:, 0]
    ids_rows, slot_index = codes_all // capacity, codes_all % capacity
    block = jnp.arange(col_total, dtype=jnp.int32)[:, None]
    plane, place = block // 4, block % 4 * capacity + slot_index
    home_row = 2 * ids_rows // col_total
    mine = (2 * ids_rows % col_total) // 2 == col_index // 2
    other = (home_row // 8 != row_index // 8).astype(jnp.int32)
    chunk = (home_row // 2 - row_index // 2 + 8) % 4 * 2 + home_row % 2
    half = 4 * capacity
    rows = 2 * half
    slot_count = row_total * rows
    position = jnp.where(mine, (other * 8 + chunk) * half + place, -1).reshape(1, seq_len)
    position = jnp.broadcast_to(position, (8, seq_len))
    home = ids // 4
    turn = (home // 2 - row_index // 2 + 8) % 4 * 2 + home % 2
    found = (col_index // 2 - ids % 4 + 4) % 4 * rows + turn * capacity + codes % capacity
    found = jnp.where(home // 8 != row_index // 8, found + 4 * rows, found)
    pick = (found[:, None] == jnp.arange(8 * rows, dtype=jnp.int32)[None, :]).astype(jnp.bfloat16)

    (out,) = whole_block(
        1, head_count, projected, out_whole, tokens, ln2_gain[None, :], ffn_in, ffn_out, position,
        expert_in[0], expert_out[0], pick, rows,
    )
    return out


def solution(mesh):
    in_specs = (
        P(("row", "col"), None),
        P(),
        P("row", "col", None, None),
        P("col", "row"),
        P(),
        P("row", "col"),
        P("col", "row"),
        P(("row", "col"), None),
        P(("row", "col"), None, None),
        P(("row", "col"), None, None),
    )
    out_specs = P(("row", "col"), None)
    return jax.shard_map(shards, mesh=mesh, in_specs=in_specs, out_specs=out_specs, check_vma=False)
```

```python
import functools
import heapq
import math
import jax
import jax.numpy as jnp
from jax import lax
from jax.experimental import pallas as pl
from jax.experimental.pallas import tpu as pltpu
from jax.sharding import PartitionSpec as P

MESH = pl.DeviceIdType.MESH
SPLIT = 32


class Net:
    def __init__(self, send, recv):
        row, col = lax.axis_index("row"), lax.axis_index("col")
        self.row, self.col = row, col
        self.high, self.y, self.core = row // 8, lax.rem(row // 2, 4), lax.rem(row, 2)
        self.x, self.low = col // 2, lax.rem(col, 2)
        self.send, self.recv = send, recv
        self.count = 0
        self.finish = []
        self.queue = []
        self.serial = 0
        self.now = 0.0
        self.free = {}
        self.spare = []

    def row_of(self, high, y, core):
        return high * 8 + lax.rem(y + 8, 4) * 2 + core

    def col_of(self, x, low):
        return lax.rem(x + 8, 4) * 2 + low

    def block_of(self, x, low):
        return low * 4 + lax.rem(x + 8, 4)

    def peer(self, name):
        high, y, core, x, low = self.high, self.y, self.core, self.x, self.low
        at = {
            "x+": (high, y, core, x + 1, low),
            "x-": (high, y, core, x - 1, low),
            "z": (high, y, core, x, 1 - low),
            "y+": (high, y + 1, core, x, low),
            "y-": (high, y - 1, core, x, low),
            "w": (1 - high, y, core, x, 1 - low),
            "c": (high, y, 1 - core, x, low),
            "y+c": (high, y + 1, 1 - core, x, low),
            "y-c": (high, y - 1, 1 - core, x, low),
        }[name]
        return self.row_of(*at[:3]), self.col_of(*at[3:])

    def greet(self, names):
        barrier = pltpu.get_barrier_semaphore()
        for name in names:
            pl.semaphore_signal(barrier, inc=1, device_id=self.peer(name), device_id_type=MESH)
        pl.semaphore_wait(barrier, len(names))

    def copy(self, src, dst, arriving, name):
        k = self.count
        self.count += 1
        make = lambda target: pltpu.make_async_remote_copy(
            src, target, self.send.at[k], self.recv.at[k], device_id=self.peer(name), device_id_type=MESH
        )
        out, arrival = make(dst), make(arriving)
        out.start()
        self.finish.append(out)
        rate, delay = (600e3, 1.0) if name == "c" else (46e3, 2.6)
        begin = max(self.now, self.free.get(name[:2], 0.0))
        self.free[name[:2]] = begin + math.prod(arriving.shape) * arriving.dtype.itemsize / rate
        return arrival, self.free[name[:2]] + delay

    def when(self, pending, action=None):
        arrival, time = pending

        def run():
            arrival.wait_recv()
            if action is not None:
                action()

        heapq.heappush(self.queue, (time, self.serial, run))
        self.serial += 1

    def work(self, time, action):
        self.spare.append((time, action))

    def spend(self, time):
        self.now += time

    def run(self):
        while self.queue or self.spare:
            if self.spare and (not self.queue or self.queue[0][0] > self.now + 0.5 * self.spare[0][0]):
                time, action = self.spare.pop(0)
                action()
                self.now += time
                continue
            time, _, action = heapq.heappop(self.queue)
            self.now = max(self.now, time) + 0.02
            action()
        for out in self.finish:
            out.wait_send()


def rows_of(ref, start, size, step=16):
    return ref.at[pl.ds(pl.multiple_of(start, step), size)]


def counted(count, action):
    left = [count]

    def step():
        left[0] -= 1
        if left[0] == 0:
            action()

    return step


def spread(net, src, out, plane_done=lambda: None, done=lambda: None):
    size = src.shape[0]
    a, half_a, half_b = SPLIT, SPLIT // 2, (size - SPLIT) // 2
    b = size - a
    x, low = net.x, net.low
    mine = counted(8, plane_done)
    theirs = counted(12, done)
    sides = ((-1, "x+", 0), (1, "x-", 1))

    def part(dx, other, start, rows):
        plane = 1 - low if other else low
        return rows_of(out, net.block_of(x + dx, plane) * size + start, rows)

    def own(start, rows):
        return src.at[pl.ds(start, rows)]

    def to_z(dx, start, rows):
        got = part(dx, 0, start, rows)
        net.when(net.copy(got, got, part(dx, 1, start, rows), "z"), theirs)

    def onward(dx, forward, other, start, rows, then):
        got = part(dx, other, start, rows)
        net.when(net.copy(got, got, part(2, other, start, rows), forward), then)

    def from_a(dx, forward, index):
        mine()

        def far():
            mine()
            to_z(2, index * half_a, half_a)

        onward(dx, forward, 0, index * half_a, half_a, far)
        to_z(dx, 0, a)

    def from_b(dx, forward, index):
        mine()
        onward(dx, forward, 0, a + index * half_b, half_b, mine)
        later()

    def partner(index, half, then):
        dx, forward, _ = sides[index]
        got = part(0, 1, a + half * half_b, half_b)
        net.when(net.copy(got, got, part(dx, 1, a + half * half_b, half_b), forward), then)

    def from_z():
        theirs()
        for dx, forward, index in sides:

            def first(dx=dx, forward=forward, index=index):
                theirs()
                onward(dx, forward, 1, a + index * half_b, half_b, theirs)

            partner(index, index, first)
        later()

    def second():
        for _, _, index in sides:
            partner(index, 1 - index, theirs)

    later = counted(3, second)
    net.when(net.copy(own(a, b), part(0, 0, a, b), part(0, 1, a, b), "z"), from_z)
    for start, rows, action in ((0, a, from_a), (a, b, from_b)):
        for dx, forward, index in sides:
            arrival = net.copy(own(start, rows), part(0, 0, start, rows), part(dx, 0, start, rows), forward)
            net.when(arrival, functools.partial(action, dx, forward, index))
    net.when(net.copy(own(0, a), part(0, 0, 0, a), part(0, 1, 0, a), "z"), theirs)
    out[pl.ds(pl.multiple_of(net.block_of(x, low) * size, size), size), :] = src[...]


def spread_small(net, src, out):
    size = src.shape[0]
    x, low = net.x, net.low

    def part(dx, other):
        plane = 1 - low if other else low
        return rows_of(out, net.block_of(x + dx, plane) * size, size, 8)

    def onward(other):
        got = part(-1, other)
        net.when(net.copy(got, got, part(-2, other), "x+"))

    def around(other, got):
        arrival = net.copy(got, part(0, other), part(-1, other), "x+")
        net.when(arrival, lambda: onward(other))
        net.when(net.copy(got, part(0, other), part(1, other), "x-"))

    around(0, src)
    arrival = net.copy(src, part(0, 0), part(0, 1), "z")
    net.when(arrival, lambda: around(1, part(0, 1)))
    out[pl.ds(pl.multiple_of(net.block_of(x, net.low) * size, size), size), :] = src[...]


def gather(net, src, out, relay, axis, done=lambda: None):
    depth, width = src.shape
    high, y, core = net.high, net.y, net.core
    middle = depth // 2
    landed = counted(10, done)

    def part(dy, other, core, half=None):
        index = net.row_of(1 - high if other else high, y + dy, core)
        start, size = (0, depth) if half is None else (half * middle, middle)
        if axis == 0:
            return rows_of(out, index * depth + start, size)
        return out.at[pl.ds(start, size), pl.ds(pl.multiple_of(index * width, width), width)]

    def to_core(dy, other, half=None):
        got = part(dy, other, core, half)
        net.when(net.copy(got, got, part(dy, other, 1 - core, half), "c"), landed)

    def from_y(dy, other):
        got = part(dy, other, core, 0 if dy < 0 else 1)
        forward = "y+" if dy < 0 else "y-"
        half = 0 if dy < 0 else 1
        arrival = net.copy(got, got, part(2, other, core, half), forward)
        net.when(arrival, lambda: to_core(2, other, half))
        to_core(dy, other)

    def around(other, got):
        for dy, forward in ((-1, "y+"), (1, "y-")):
            arrival = net.copy(got, part(0, other, core), part(dy, other, core), forward)
            net.when(arrival, lambda dy=dy: from_y(dy, other))

    around(0, src)
    waiting = [2]

    def arrived():
        waiting[0] -= 1
        if waiting[0] == 0:
            around(1, part(0, 1, core))
            to_core(0, 1)

    for half, first, second in ((0, "z", "w"), (1, "w", "z")):
        arrival = net.copy(src.at[pl.ds(half * middle, middle)], relay.at[half], relay.at[half], first)

        def onward(half=half, second=second):
            got = relay.at[half]
            arrival = net.copy(got, part(0, half, core, half), part(0, 1, core, half), second)
            net.when(arrival, arrived)

        net.when(arrival, onward)
    mine = part(0, 0, core)
    net.when(net.copy(src, mine, part(0, 0, 1 - core), "c"), landed)
    index = net.row
    if axis == 0:
        out[pl.ds(pl.multiple_of(index * depth, depth), depth), :] = src[...]
    else:
        out[:, pl.ds(pl.multiple_of(index * width, width), width)] = src[...]


def reduce_scatter(net, fill, src, scratch, finish, split, step=lambda action: action(), gate=lambda action: action()):
    far_b, near_b, acc_b, plane, last = scratch[:5]
    if split:
        from_z, sums, far_a, near_a, acc_a = scratch[5:]
    size = src.shape[0] // 8
    a = split
    b = size - a
    x, low = net.x, net.low

    def rows(dx, other, start, count):
        index = net.block_of(x + dx, 1 - low if other else low)
        return pl.ds(pl.multiple_of(index * size + start, 16), count)

    def ring(block, count, far, near, acc, done):
        half = count // 2
        halves = {"x+": (0, half), "x-": (half, half)}
        waiting = [4]

        def arrived():
            waiting[0] -= 1
            if waiting[0] == 0:
                done()

        def start_far():
            for index, forward in ((0, "x+"), (1, "x-")):
                first = halves[forward][0]
                arrival = net.copy(block(2, first, half), far.at[index], far.at[index], forward)

                def add(index=index, forward=forward, first=first):
                    need(3)
                    term = block(1 if forward == "x+" else -1, first, half)
                    acc[index] = far[index] + term[...]
                    net.spend(0.1)
                    dst = near.at[index, pl.ds(first, half)]
                    net.when(net.copy(acc.at[index], dst, dst, forward), arrived)

                net.when(arrival, add)

        def start_direct():
            for index, forward in ((0, "x+"), (1, "x-")):
                first = half - halves[forward][0]
                dst = near.at[index, pl.ds(first, half)]
                term = block(1 if forward == "x+" else -1, first, half)
                net.when(net.copy(term, dst, dst, forward), arrived)

        return start_far, start_direct

    def block_b(other):
        return lambda dx, first, count: src.at[rows(dx, other, a + first, count)]

    def block_a(dx, first, count):
        return sums.at[pl.ds((dx % 4) * a + first, count)]

    left = [4]
    both = [3 if a else 2]
    wide = lambda value: value.astype(jnp.float32)

    def from_partner(k):
        need(4)
        sums[pl.ds(k * a, a), :] = from_z[pl.ds(k * a, a), :] + src[rows(k, 0, 0, a), :]
        net.spend(0.1)
        left[0] -= 1
        if left[0] == 0:
            for start in ring(block_a, a, far_a, near_a, acc_a, arrived):
                start()

    def to_partner(k):
        if a == 0:
            return
        landing = from_z.at[pl.ds(k * a, a)]
        net.when(net.copy(src.at[rows(k, 1, 0, a)], landing, landing, "z"), lambda: from_partner(k))

    def plane_done():
        need(4)
        total = wide(near_b[0, 0]) + wide(near_b[0, 1]) + wide(src[rows(0, 1, a, b), :])
        plane[...] = total.astype(plane.dtype)
        net.spend(0.3)
        gate(lambda: net.when(net.copy(plane, last, last, "z"), arrived))

    def arrived():
        both[0] -= 1
        if both[0]:
            return
        if a:
            finish(0, wide(near_a[0]) + wide(near_a[1]) + wide(sums[pl.ds(0, a), :]))
        total = wide(near_b[1, 0]) + wide(near_b[1, 1]) + wide(src[rows(0, 0, a, b), :]) + wide(last[...])
        net.spend(0.5)
        finish(a, total)

    far_other, direct_other = ring(block_b(1), b, far_b.at[0], near_b.at[0], acc_b.at[0], plane_done)
    far_own, direct_own = ring(block_b(0), b, far_b.at[1], near_b.at[1], acc_b.at[1], arrived)
    def first():
        fill(lambda i: net.block_of(x + 2, lax.rem(low + 1 + i, 2)))
        far_other()
        far_own()
        to_partner(2)

    def second():
        fill(lambda i: net.block_of(x + 1 - 2 * i, 1 - low))
        direct_other()
        to_partner(1)
        to_partner(3)

    def third():
        fill(lambda i: net.block_of(x + 1 - 2 * i, low))
        direct_own()

    def fourth():
        fill(lambda i: net.block_of(x, lax.rem(low + 1 + i, 2)))
        to_partner(0)

    actions = [first, second, third, fourth]

    def need(number):
        while len(actions) > 4 - number:
            actions.pop(0)()

    for number in range(1, 5):
        step(lambda number=number: need(number))


def scatter_scratch(size, width, dtype, split):
    a, b = split, size - split
    shapes = [(2, 2, b // 2, width), (2, 2, b, width), (2, 2, b // 2, width), (b, width), (b, width)]
    if a:
        shapes += [(4 * a, width), (4 * a, width), (2, a // 2, width), (2, a, width), (2, a // 2, width)]
    return [pltpu.VMEM(shape, dtype) for shape in shapes]


def comm_body(spreads, smalls, gathers, *refs):
    count = spreads + smalls + len(gathers)
    ins, outs, relays = refs[:count], refs[count : 2 * count], refs[2 * count : -2]
    net = Net(*refs[-2:])
    net.greet(["x+", "x-", "z", "y+", "y-", "w", "c"])
    for k in range(spreads):
        spread(net, ins[k], outs[k])
    for k in range(spreads, spreads + smalls):
        spread_small(net, ins[k], outs[k])
    for i, axis in enumerate(gathers):
        k = spreads + smalls + i
        gather(net, ins[k], outs[k], relays[i], axis)
    net.run()


def communicate(name, body, collective_id, arrays, shapes, scratch, copies, outside=(), spare=6 * 2**20):
    used = sum(math.prod(r.shape) * jnp.dtype(r.dtype).itemsize for r in scratch if r.memory_space == pltpu.VMEM)
    spaces = [pl.ANY if i in outside else pltpu.VMEM for i in range(len(arrays))]
    return pl.pallas_call(
        body,
        out_shape=shapes,
        in_specs=[pl.BlockSpec(memory_space=space) for space in spaces],
        out_specs=[pl.BlockSpec(memory_space=pltpu.VMEM)] * len(shapes),
        scratch_shapes=scratch + [pltpu.SemaphoreType.DMA((copies,)), pltpu.SemaphoreType.DMA((copies,))],
        compiler_params=pltpu.CompilerParams(
            collective_id=collective_id, has_side_effects=True, vmem_limit_bytes=min(used + spare, 62 * 2**20)
        ),
        name=name,
    )(*arrays)


def gathered(array, axis):
    depth, width = array.shape
    total = lax.axis_size("row")
    shape = (depth * total, width) if axis == 0 else (depth, width * total)
    return jax.ShapeDtypeStruct(shape, array.dtype)


def relay_of(array):
    return pltpu.VMEM((2, array.shape[0] // 2, array.shape[1]), array.dtype)


def exchange(name, collective_id, spreads=(), smalls=(), gathers=()):
    whole = [jax.ShapeDtypeStruct((8 * a.shape[0], a.shape[1]), a.dtype) for a in (*spreads, *smalls)]
    return communicate(
        name,
        functools.partial(comm_body, len(spreads), len(smalls), [axis for _, axis in gathers]),
        collective_id,
        [*spreads, *smalls, *(array for array, _ in gathers)],
        whole + [gathered(*pair) for pair in gathers],
        [relay_of(array) for array, _ in gathers],
        22 * len(spreads) + 8 * len(smalls) + 22 * len(gathers),
    )


def block_body(heads, qkv, weight, tokens, gain, up, down, position, expert_in, expert_out, pick, result, *rest):
    terms, mixed, normed, image, up_whole, table, far, y_relay, up_relay, down_relay = rest[:10]
    hidden, down_whole, units, out, pair, weights, fetched = rest[10:17]
    held, _, span = weights.shape
    tiles = expert_in.shape[1] // span
    fetches = []

    def fetch():
        t = len(fetches)
        if t == 3 * tiles:
            return
        source = expert_in if t < tiles else expert_out
        tile = source.at[:, pl.ds(t % tiles * span, span)]
        copy = pltpu.make_async_copy(tile, weights.at[t % held], fetched.at[t])
        copy.start()
        fetches.append(copy)

    for _ in range(held):
        fetch()
    net = Net(*rest[-2:])
    net.greet(["x+", "x-", "z", "y+", "y-", "w", "c", "y+c", "y-c"])
    size = tokens.shape[0]
    dim = qkv.shape[1] // (3 * heads)
    low = net.low
    slots = out.shape[3] // 2
    mine = pl.ds(pl.multiple_of(low * slots, slots), slots)
    theirs = pl.ds(pl.multiple_of((1 - low) * slots, slots), slots)

    def fill(column):
        @pl.loop(0, 2)
        def _(i):
            at = pl.ds(pl.multiple_of(column(i) * size, size), size)

            @pl.loop(0, heads)
            def _(h):
                part = lambda k: pl.ds(pl.multiple_of((3 * h + k) * dim, dim), dim)
                scores = lax.dot_general(
                    qkv[at, part(0)], qkv[:, part(1)], (((1,), (1,)), ((), ())), preferred_element_type=jnp.float32
                )
                scale = dim ** (-0.5) * math.log2(math.e)
                chances = jnp.exp2((scores - jnp.max(scores, axis=-1, keepdims=True)) * scale)
                total = jnp.sum(chances, axis=-1, keepdims=True)
                value = matmul(chances.astype(jnp.bfloat16), qkv[:, part(2)]) / total
                mixed[:, pl.ds(pl.multiple_of(h * dim, dim), dim)] = value.astype(jnp.bfloat16)

            @pl.loop(0, weight.shape[1] // 512)
            def _(j):
                columns = pl.ds(pl.multiple_of(j * 512, 512), 512)
                terms[at, columns] = matmul(mixed[...], weight[:, columns]).astype(jnp.bfloat16)

        net.spend(2.6)

    def fill_dense(column):
        while early:
            early.pop().wait_send()
        at = [pl.ds(pl.multiple_of(column(i) * size, size), size) for i in range(2)]
        for i in range(2):
            pair[pl.ds(i * size, size), :] = units[at[i], :]

        @pl.loop(0, down_whole.shape[1] // 512)
        def _(j):
            columns = pl.ds(pl.multiple_of(j * 512, 512), 512)
            product = matmul(pair[...], down_whole[:, columns]).astype(jnp.bfloat16)
            for i in range(2):
                terms[at[i], columns] = product[i * size : (i + 1) * size]

    def place(index, plane):
        rows = pl.ds(pl.multiple_of(plane * 4 * size, 4 * size), 4 * size)
        flat = math.prod(table.shape[1:5])
        here = lax.broadcasted_iota(jnp.int32, (flat, 4 * size), 0) == position[pl.ds(0, 1), rows]
        placing = jnp.where(here, 1.0, 0.0).astype(jnp.bfloat16)
        span = 512

        @pl.loop(0, image.shape[1] // span)
        def _(j):
            columns = pl.ds(pl.multiple_of(j * span, span), span)
            put = matmul(placing, image[rows, columns]).astype(jnp.bfloat16)
            table[index, :, :, :, :, columns] = put.reshape(table.shape[1:5] + (span,))

        net.spend(1.2)

    def plane_done():
        place(0, low)

        def from_w(d):
            got = far.at[d, :, theirs]
            arrival = net.copy(got, got, far.at[d, :, mine], "z")
            net.when(arrival, last[d])
            first[d]()

        for d in (2, 1, 3, 0):
            arrival = net.copy(table.at[0, 1, d], far.at[d, :, mine], far.at[d, :, theirs], "w")
            net.when(arrival, functools.partial(from_w, d))
        start_all(own)
        ready()

    def image_done():
        place(1, 1 - low)
        start_all(other)
        ready()

    finish_dense, start_expert, gate = returning(
        net, out, pick, hidden, result, weights, fetches, fetch, *rest[17:30]
    )
    dispatched = counted(28, start_expert)
    came = lambda d: dispatched()
    own = y_exchange(net, chunks(table.at[0, 0]), chunks(out.at[0], mine), y_relay.at[0], came)
    first = y_exchange(net, chunks(far, theirs), chunks(out.at[1], theirs), y_relay.at[1], came)
    last = y_exchange(net, chunks(far, mine), chunks(out.at[1], mine), y_relay.at[2], came)
    other = y_exchange(net, chunks(table.at[1, 0]), chunks(out.at[0], theirs), y_relay.at[3], came)
    early = []

    def dense():
        up_tasks(net, image, up_whole, units)
        reduce_scatter(net, fill_dense, terms, rest[30:40], finish_dense, 32, lambda action: net.work(1.4, action), gate)

    ready = counted(4, dense)

    def finish(start, total):
        at = pl.ds(start, total.shape[0])
        state = (tokens[at, :].astype(jnp.float32) + total).astype(jnp.bfloat16)
        hidden[at, :] = state
        normed[at, :] = layer_norm(state, gain[...]).astype(jnp.bfloat16)
        if start == 0:
            return
        early.extend(net.finish)
        net.finish.clear()
        net.spend(0.5)
        spread(net, normed, image, plane_done, image_done)

    gather(net, up, up_whole, up_relay, 0, ready)
    gather(net, down, down_whole, down_relay, 1, ready)
    reduce_scatter(net, fill, terms, rest[40:-2], finish, SPLIT)
    net.run()


def whole_block(collective_id, heads, qkv, weight, tokens, gain, up, down, position, expert_in, expert_out, pick, slots):
    size, width = tokens.shape
    depth, inside = expert_in.shape
    span = min(512, width)
    full, part = (4, 2, slots, width), (4, 2, slots // 2, width)
    sixteen = lambda *shape: pltpu.VMEM(shape, tokens.dtype)
    scratch = [
        sixteen(8 * size, width),
        sixteen(size, weight.shape[0]),
        sixteen(size, width),
        sixteen(8 * size, width),
        sixteen(*gathered(up, 0).shape),
        sixteen(2, 2, *part),
        sixteen(*full),
        sixteen(4, 2, slots // 2, width),
        relay_of(up),
        relay_of(down),
        sixteen(size, width),
        sixteen(*gathered(down, 1).shape),
        sixteen(8 * size, up.shape[1]),
        sixteen(2, *full),
        sixteen(2 * size, up.shape[1]),
        sixteen(3, depth, span),
        pltpu.SemaphoreType.DMA((3 * (width // span),)),
        sixteen(*full),
        sixteen(*part),
        sixteen(*part),
        sixteen(*full),
        sixteen(*part),
        sixteen(2, *part),
        sixteen(2, 4 * slots, width),
        sixteen(2, 2, slots // 2, width),
        sixteen(2, 2, slots, width),
        sixteen(2, 4 * slots, width),
        pltpu.VMEM((size, width), jnp.float32),
        sixteen(2, *full),
        sixteen(2, 8 * slots, inside),
    ]
    scratch += scatter_scratch(size, width, tokens.dtype, 32) + scatter_scratch(size, width, tokens.dtype, SPLIT)
    return communicate(
        "block",
        functools.partial(block_body, heads),
        collective_id,
        (qkv, weight, tokens, gain, up, down, position, expert_in, expert_out, pick),
        [jax.ShapeDtypeStruct(tokens.shape, tokens.dtype)],
        scratch,
        24 + 22 + 2 * 22 + 8 + 4 * 10 + 24 + 2 * 10 + 12 + 12,
        outside=(7, 8),
        spare=7 * 2**20,
    )


def y_exchange(net, src, dst, relay, arrived=lambda d: None, then=lambda: None):
    core = net.core
    forwarded = counted(2, then)

    def opposite():
        for index, c, forward, last in ((0, core, "y+", "y+"), (1, 1 - core, "y-", "y-c")):

            def onward(index=index, c=c, last=last):
                arrival = net.copy(relay.at[index], dst(2, core), dst(2, c), last)
                net.when(arrival, lambda: arrived(2))
                forwarded()

            net.when(net.copy(src(2, c), relay.at[index], relay.at[index], forward), onward)

    def beside(d):
        forward = "y+" if d == 1 else "y-"
        for c, name in ((core, forward), (1 - core, forward + "c")):
            net.when(net.copy(src(d, c), dst(4 - d, core), dst(4 - d, c), name), lambda: arrived(4 - d))

    def here():
        net.when(net.copy(src(0, 1 - core), dst(0, core), dst(0, 1 - core), "c"), lambda: arrived(0))
        dst(0, core)[...] = src(0, core)[...]

    return {2: opposite, 1: lambda: beside(1), 3: lambda: beside(3), 0: here}


def chunks(ref, *rest):
    return lambda d, c: ref.at[(d, c, *rest)]


def start_all(steps):
    for d in (2, 1, 3, 0):
        steps[d]()


def up_tasks(net, x_ref, w_ref, out):
    rows, width = out.shape
    tile = min(256, rows)
    span = min(256, width)

    def piece(j):
        columns = pl.ds(j * span, span)

        @pl.loop(0, rows // tile)
        def _(i):
            at = pl.ds(pl.multiple_of(i * tile, tile), tile)
            inner = jnp.dot(x_ref[at, :], w_ref[:, columns], preferred_element_type=jnp.float32)
            out[at, columns] = (inner * (1.0 + lax.erf(inner * (0.5**0.5))) * 0.5).astype(out.dtype)

    for j in range(width // span):
        net.work(1.6, lambda j=j: piece(j))


def returning(net, rows, pick, hidden, out, weights, fetches, fetch, *rest):
    far, other, total, near, partial, found, packed, relay, y_relay = rest[:9]
    arrived_rows, dense, parts, inner = rest[9:13]
    held, _, span = weights.shape
    tiles = inner.shape[2] // span
    low = net.low
    half = parts.shape[3] // 2
    mine, theirs = pl.ds(pl.multiple_of(low * half, half), half), pl.ds(pl.multiple_of((1 - low) * half, half), half)
    count = packed.shape[1] // 4

    def pack(index):
        flat = math.prod(found.shape[1:4])
        row = lax.broadcasted_iota(jnp.int32, (count, flat), 0)
        slot = lax.broadcasted_iota(jnp.int32, (count, flat), 1)
        each = half // 4
        same = (row // each == slot // half) & (row % each == slot % each)
        for k in range(4):
            chosen = same & (slot % half // each == lax.rem(net.x + k, 4))
            chosen = jnp.where(chosen, 1.0, 0.0).astype(jnp.bfloat16)

            @pl.loop(0, found.shape[4] // 512)
            def _(j):
                columns = pl.ds(pl.multiple_of(j * 512, 512), 512)
                rows = found[index, :, :, :, columns].reshape(flat, 512)
                value = matmul(chosen, rows).astype(jnp.bfloat16)
                packed[index, k * count : (k + 1) * count, columns] = value

        net.spend(0.6)

    def send(index):
        pack(index)
        at = lambda k, first=0, rows=count: packed.at[index, pl.ds(k * count + first, rows)]
        place = lambda k, first=0, rows=count: arrived_rows.at[index, pl.ds(k * count + first, rows)]
        middle = count // 2
        for i, forward in ((0, "x+"), (1, "x-")):

            def onward(i=i, forward=forward):
                dst = place(2, i * middle, middle)
                net.when(net.copy(relay.at[index, i], dst, dst, forward), landed)

            net.when(net.copy(at(2, i * middle, middle), relay.at[index, i], relay.at[index, i], forward), onward)
        for k, forward in ((1, "x+"), (3, "x-")):
            net.when(net.copy(at(k), place(k), place(k), forward), landed)

    flat_rows = math.prod(parts.shape[1:4])

    def expert_up(j):
        fetches[j].wait()

        @pl.loop(0, 2)
        def _(i):
            value = matmul(rows[i].reshape(flat_rows, rows.shape[4]), weights[j % held])
            value = value * (1.0 + lax.erf(value * (0.5**0.5))) * 0.5
            inner[i, :, pl.ds(j * span, span)] = value.astype(inner.dtype)

        fetch()

    def expert_down(i, j):
        t = (2 - i) * tiles + j
        fetches[t].wait()
        value = matmul(inner[i], weights[t % held]).astype(parts.dtype)
        parts[i, :, :, :, pl.ds(j * span, span)] = value.reshape(parts.shape[1:4] + (span,))
        fetch()

    def finish_dense(start, total):
        dense[pl.ds(start, total.shape[0]), :] = total
        if start:
            ready()

    def combine():
        flat = 4 * count
        for index in range(2):
            arrived_rows[index, pl.ds(0, count), :] = packed[index, pl.ds(0, count), :]

        @pl.loop(0, out.shape[1] // 512)
        def _(j):
            columns = pl.ds(pl.multiple_of(j * 512, 512), 512)
            value = hidden[:, columns].astype(jnp.float32) + dense[:, columns]
            for index in range(2):
                value += matmul(pick[:, pl.ds(index * flat, flat)], arrived_rows[index, :, columns])
            out[:, columns] = value.astype(jnp.bfloat16)

    ready = counted(9, combine)
    landed = ready

    def far_landed(d):
        def add():
            total[d] = far[d, :, theirs] + other[d]
            net.spend(0.2)
            arrival = net.copy(total.at[d], found.at[1, d], found.at[1, d], "w")
            net.when(arrival, complete[1])

        net.when(net.copy(far.at[d, :, mine], other.at[d], other.at[d], "z"), add)

    pending = []
    held_back = counted(5, lambda: pending.pop()())

    def gate(action):
        pending.append(action)
        held_back()

    def near_landed(d):
        def add():
            found[0, d] = near[d, :, mine] + partial[d]
            net.spend(0.2)
            complete[0]()

        net.when(net.copy(near.at[d, :, theirs], partial.at[d], partial.at[d], "z"), add)
        held_back()

    complete = [counted(4, functools.partial(send, index)) for index in range(2)]
    far_counts = {d: counted(1 if d == 0 else 2, functools.partial(far_landed, d)) for d in range(4)}
    near_counts = {d: counted(1 if d == 0 else 2, functools.partial(near_landed, d)) for d in range(4)}
    second = y_exchange(net, chunks(parts.at[0]), chunks(near), y_relay.at[0], lambda d: near_counts[d]())
    go = counted(2, lambda: start_all(second))
    first = y_exchange(net, chunks(parts.at[1]), chunks(far), y_relay.at[1], lambda d: far_counts[d](), go)

    def start():
        for j in range(tiles):
            expert_up(j)
            net.spend(1.3)
        for i, after in ((1, lambda: start_all(first)), (0, go)):
            for j in range(tiles):
                expert_down(i, j)
                net.spend(0.7)
            after()

    return finish_dense, start, gate


def layer_norm(row_data, gain_vector):
    row_data = row_data.astype(jnp.float32)
    centered = row_data - jnp.mean(row_data, axis=-1, keepdims=True)
    spread = jnp.mean(centered * centered, axis=-1, keepdims=True)
    return centered * lax.rsqrt(spread + 1e-06) * gain_vector


def matmul(a, b):
    return jnp.dot(a, b, preferred_element_type=jnp.float32)


def shards(
    tokens,
    ln1_gain,
    qkv_weight,
    out_weight,
    ln2_gain,
    ffn_in,
    ffn_out,
    expert_ids,
    expert_in,
    expert_out,
):
    tok_count, model_width = tokens.shape
    row_total = lax.axis_size("row")
    col_total = lax.axis_size("col")
    row_index = lax.axis_index("row")
    col_index = lax.axis_index("col")
    expert_count = row_total * col_total // 2
    capacity = max(2, 2 * tok_count // expert_count)
    head_count, head_dim = qkv_weight.shape[1], qkv_weight.shape[3]
    seq_len = tok_count * col_total

    ids = expert_ids[:, 0]
    token = jnp.arange(tok_count, dtype=jnp.int32)
    same = (expert_ids == ids[None, :]) & (token[:, None] < token[None, :])
    codes = ids * capacity + jnp.sum(same.astype(jnp.int32), axis=0)
    image_rows, codes_all, qkv_whole, out_whole = exchange(
        "enter",
        0,
        spreads=(tokens,),
        smalls=(jnp.broadcast_to(codes[None, :], (8, tok_count)),),
        gathers=((qkv_weight.reshape(qkv_weight.shape[0], -1), 0), (out_weight, 1)),
    )
    normed = layer_norm(image_rows, ln1_gain).astype(jnp.bfloat16)
    projected = matmul(normed, qkv_whole).astype(jnp.bfloat16)
    codes_all = codes_all.reshape(col_total, 8, tok_count)[:, 0]
    ids_rows, slot_index = codes_all // capacity, codes_all % capacity
    block = jnp.arange(col_total, dtype=jnp.int32)[:, None]
    plane, place = block // 4, block % 4 * capacity + slot_index
    home_row = 2 * ids_rows // col_total
    mine = (2 * ids_rows % col_total) // 2 == col_index // 2
    other = (home_row // 8 != row_index // 8).astype(jnp.int32)
    chunk = (home_row // 2 - row_index // 2 + 8) % 4 * 2 + home_row % 2
    half = 4 * capacity
    rows = 2 * half
    slot_count = row_total * rows
    position = jnp.where(mine, (other * 8 + chunk) * half + place, -1).reshape(1, seq_len)
    position = jnp.broadcast_to(position, (8, seq_len))
    home = ids // 4
    turn = (home // 2 - row_index // 2 + 8) % 4 * 2 + home % 2
    found = (col_index // 2 - ids % 4 + 4) % 4 * rows + turn * capacity + codes % capacity
    found = jnp.where(home // 8 != row_index // 8, found + 4 * rows, found)
    pick = (found[:, None] == jnp.arange(8 * rows, dtype=jnp.int32)[None, :]).astype(jnp.bfloat16)

    (out,) = whole_block(
        1, head_count, projected, out_whole, tokens, ln2_gain[None, :], ffn_in, ffn_out, position,
        expert_in[0], expert_out[0], pick, rows,
    )
    return out


def solution(mesh):
    in_specs = (
        P(("row", "col"), None),
        P(),
        P("row", "col", None, None),
        P("col", "row"),
        P(),
        P("row", "col"),
        P("col", "row"),
        P(("row", "col"), None),
        P(("row", "col"), None, None),
        P(("row", "col"), None, None),
    )
    out_specs = P(("row", "col"), None)
    return jax.shard_map(shards, mesh=mesh, in_specs=in_specs, out_specs=out_specs, check_vma=False)
```

```python
import functools
import heapq
import math
import jax
import jax.numpy as jnp
from jax import lax
from jax.experimental import pallas as pl
from jax.experimental.pallas import tpu as pltpu
from jax.sharding import PartitionSpec as P

MESH = pl.DeviceIdType.MESH
SPLIT = 32


class Net:
    def __init__(self, send, recv):
        row, col = lax.axis_index("row"), lax.axis_index("col")
        self.row, self.col = row, col
        self.high, self.y, self.core = row // 8, lax.rem(row // 2, 4), lax.rem(row, 2)
        self.x, self.low = col // 2, lax.rem(col, 2)
        self.send, self.recv = send, recv
        self.count = 0
        self.finish = []
        self.queue = []
        self.serial = 0
        self.now = 0.0
        self.free = {}
        self.spare = []

    def row_of(self, high, y, core):
        return high * 8 + lax.rem(y + 8, 4) * 2 + core

    def col_of(self, x, low):
        return lax.rem(x + 8, 4) * 2 + low

    def block_of(self, x, low):
        return low * 4 + lax.rem(x + 8, 4)

    def peer(self, name):
        high, y, core, x, low = self.high, self.y, self.core, self.x, self.low
        at = {
            "x+": (high, y, core, x + 1, low),
            "x-": (high, y, core, x - 1, low),
            "z": (high, y, core, x, 1 - low),
            "y+": (high, y + 1, core, x, low),
            "y-": (high, y - 1, core, x, low),
            "w": (1 - high, y, core, x, 1 - low),
            "c": (high, y, 1 - core, x, low),
            "y+c": (high, y + 1, 1 - core, x, low),
            "y-c": (high, y - 1, 1 - core, x, low),
        }[name]
        return self.row_of(*at[:3]), self.col_of(*at[3:])

    def greet(self, names):
        barrier = pltpu.get_barrier_semaphore()
        for name in names:
            pl.semaphore_signal(barrier, inc=1, device_id=self.peer(name), device_id_type=MESH)
        pl.semaphore_wait(barrier, len(names))

    def copy(self, src, dst, arriving, name):
        k = self.count
        self.count += 1
        make = lambda target: pltpu.make_async_remote_copy(
            src, target, self.send.at[k], self.recv.at[k], device_id=self.peer(name), device_id_type=MESH
        )
        out, arrival = make(dst), make(arriving)
        out.start()
        self.finish.append(out)
        rate, delay = (600e3, 1.0) if name == "c" else (46e3, 2.6)
        begin = max(self.now, self.free.get(name[:2], 0.0))
        self.free[name[:2]] = begin + math.prod(arriving.shape) * arriving.dtype.itemsize / rate
        return arrival, self.free[name[:2]] + delay

    def when(self, pending, action=None):
        arrival, time = pending

        def run():
            arrival.wait_recv()
            if action is not None:
                action()

        heapq.heappush(self.queue, (time, self.serial, run))
        self.serial += 1

    def work(self, time, action):
        self.spare.append((time, action))

    def spend(self, time):
        self.now += time

    def run(self):
        while self.queue or self.spare:
            if self.spare and (not self.queue or self.queue[0][0] > self.now + 0.5 * self.spare[0][0]):
                time, action = self.spare.pop(0)
                action()
                self.now += time
                continue
            time, _, action = heapq.heappop(self.queue)
            self.now = max(self.now, time) + 0.02
            action()
        for out in self.finish:
            out.wait_send()


def rows_of(ref, start, size, step=16):
    return ref.at[pl.ds(pl.multiple_of(start, step), size)]


def counted(count, action):
    left = [count]

    def step():
        left[0] -= 1
        if left[0] == 0:
            action()

    return step


def spread(net, src, out, plane_done=lambda: None, done=lambda: None):
    size = src.shape[0]
    a, half_a, half_b = SPLIT, SPLIT // 2, (size - SPLIT) // 2
    b = size - a
    x, low = net.x, net.low
    mine = counted(8, plane_done)
    theirs = counted(12, done)
    sides = ((-1, "x+", 0), (1, "x-", 1))

    def part(dx, other, start, rows):
        plane = 1 - low if other else low
        return rows_of(out, net.block_of(x + dx, plane) * size + start, rows)

    def own(start, rows):
        return src.at[pl.ds(start, rows)]

    def to_z(dx, start, rows):
        got = part(dx, 0, start, rows)
        net.when(net.copy(got, got, part(dx, 1, start, rows), "z"), theirs)

    def onward(dx, forward, other, start, rows, then):
        got = part(dx, other, start, rows)
        net.when(net.copy(got, got, part(2, other, start, rows), forward), then)

    def from_a(dx, forward, index):
        mine()

        def far():
            mine()
            to_z(2, index * half_a, half_a)

        onward(dx, forward, 0, index * half_a, half_a, far)
        to_z(dx, 0, a)

    def from_b(dx, forward, index):
        mine()
        onward(dx, forward, 0, a + index * half_b, half_b, mine)
        later()

    def partner(index, half, then):
        dx, forward, _ = sides[index]
        got = part(0, 1, a + half * half_b, half_b)
        net.when(net.copy(got, got, part(dx, 1, a + half * half_b, half_b), forward), then)

    def from_z():
        theirs()
        for dx, forward, index in sides:

            def first(dx=dx, forward=forward, index=index):
                theirs()
                onward(dx, forward, 1, a + index * half_b, half_b, theirs)

            partner(index, index, first)
        later()

    def second():
        for _, _, index in sides:
            partner(index, 1 - index, theirs)

    later = counted(3, second)
    net.when(net.copy(own(a, b), part(0, 0, a, b), part(0, 1, a, b), "z"), from_z)
    for start, rows, action in ((0, a, from_a), (a, b, from_b)):
        for dx, forward, index in sides:
            arrival = net.copy(own(start, rows), part(0, 0, start, rows), part(dx, 0, start, rows), forward)
            net.when(arrival, functools.partial(action, dx, forward, index))
    net.when(net.copy(own(0, a), part(0, 0, 0, a), part(0, 1, 0, a), "z"), theirs)
    out[pl.ds(pl.multiple_of(net.block_of(x, low) * size, size), size), :] = src[...]


def spread_small(net, src, out):
    size = src.shape[0]
    x, low = net.x, net.low

    def part(dx, other):
        plane = 1 - low if other else low
        return rows_of(out, net.block_of(x + dx, plane) * size, size, 8)

    def onward(other):
        got = part(-1, other)
        net.when(net.copy(got, got, part(-2, other), "x+"))

    def around(other, got):
        arrival = net.copy(got, part(0, other), part(-1, other), "x+")
        net.when(arrival, lambda: onward(other))
        net.when(net.copy(got, part(0, other), part(1, other), "x-"))

    around(0, src)
    arrival = net.copy(src, part(0, 0), part(0, 1), "z")
    net.when(arrival, lambda: around(1, part(0, 1)))
    out[pl.ds(pl.multiple_of(net.block_of(x, net.low) * size, size), size), :] = src[...]


def gather(net, src, out, relay, axis, done=lambda: None):
    depth, width = src.shape
    high, y, core = net.high, net.y, net.core
    middle = depth // 2
    landed = counted(10, done)

    def part(dy, other, core, half=None):
        index = net.row_of(1 - high if other else high, y + dy, core)
        start, size = (0, depth) if half is None else (half * middle, middle)
        if axis == 0:
            return rows_of(out, index * depth + start, size)
        return out.at[pl.ds(start, size), pl.ds(pl.multiple_of(index * width, width), width)]

    def to_core(dy, other, half=None):
        got = part(dy, other, core, half)
        net.when(net.copy(got, got, part(dy, other, 1 - core, half), "c"), landed)

    def from_y(dy, other):
        got = part(dy, other, core, 0 if dy < 0 else 1)
        forward = "y+" if dy < 0 else "y-"
        half = 0 if dy < 0 else 1
        arrival = net.copy(got, got, part(2, other, core, half), forward)
        net.when(arrival, lambda: to_core(2, other, half))
        to_core(dy, other)

    def around(other, got):
        for dy, forward in ((-1, "y+"), (1, "y-")):
            arrival = net.copy(got, part(0, other, core), part(dy, other, core), forward)
            net.when(arrival, lambda dy=dy: from_y(dy, other))

    around(0, src)
    waiting = [2]

    def arrived():
        waiting[0] -= 1
        if waiting[0] == 0:
            around(1, part(0, 1, core))
            to_core(0, 1)

    for half, first, second in ((0, "z", "w"), (1, "w", "z")):
        arrival = net.copy(src.at[pl.ds(half * middle, middle)], relay.at[half], relay.at[half], first)

        def onward(half=half, second=second):
            got = relay.at[half]
            arrival = net.copy(got, part(0, half, core, half), part(0, 1, core, half), second)
            net.when(arrival, arrived)

        net.when(arrival, onward)
    mine = part(0, 0, core)
    net.when(net.copy(src, mine, part(0, 0, 1 - core), "c"), landed)
    index = net.row
    if axis == 0:
        out[pl.ds(pl.multiple_of(index * depth, depth), depth), :] = src[...]
    else:
        out[:, pl.ds(pl.multiple_of(index * width, width), width)] = src[...]


def reduce_scatter(net, fill, src, scratch, finish, split, step=lambda action: action(), gate=lambda action: action()):
    far_b, near_b, acc_b, plane, last = scratch[:5]
    if split:
        from_z, sums, far_a, near_a, acc_a = scratch[5:]
    size = src.shape[0] // 8
    a = split
    b = size - a
    x, low = net.x, net.low

    def rows(dx, other, start, count):
        index = net.block_of(x + dx, 1 - low if other else low)
        return pl.ds(pl.multiple_of(index * size + start, 16), count)

    def ring(block, count, far, near, acc, done):
        half = count // 2
        halves = {"x+": (0, half), "x-": (half, half)}
        waiting = [4]

        def arrived():
            waiting[0] -= 1
            if waiting[0] == 0:
                done()

        def start_far():
            for index, forward in ((0, "x+"), (1, "x-")):
                first = halves[forward][0]
                arrival = net.copy(block(2, first, half), far.at[index], far.at[index], forward)

                def add(index=index, forward=forward, first=first):
                    need(3)
                    term = block(1 if forward == "x+" else -1, first, half)
                    acc[index] = far[index] + term[...]
                    net.spend(0.1)
                    dst = near.at[index, pl.ds(first, half)]
                    net.when(net.copy(acc.at[index], dst, dst, forward), arrived)

                net.when(arrival, add)

        def start_direct():
            for index, forward in ((0, "x+"), (1, "x-")):
                first = half - halves[forward][0]
                dst = near.at[index, pl.ds(first, half)]
                term = block(1 if forward == "x+" else -1, first, half)
                net.when(net.copy(term, dst, dst, forward), arrived)

        return start_far, start_direct

    def block_b(other):
        return lambda dx, first, count: src.at[rows(dx, other, a + first, count)]

    def block_a(dx, first, count):
        return sums.at[pl.ds((dx % 4) * a + first, count)]

    left = [4]
    both = [3 if a else 2]
    wide = lambda value: value.astype(jnp.float32)

    def from_partner(k):
        need(4)
        sums[pl.ds(k * a, a), :] = from_z[pl.ds(k * a, a), :] + src[rows(k, 0, 0, a), :]
        net.spend(0.1)
        left[0] -= 1
        if left[0] == 0:
            for start in ring(block_a, a, far_a, near_a, acc_a, arrived):
                start()

    def to_partner(k):
        if a == 0:
            return
        landing = from_z.at[pl.ds(k * a, a)]
        net.when(net.copy(src.at[rows(k, 1, 0, a)], landing, landing, "z"), lambda: from_partner(k))

    def plane_done():
        need(4)
        total = wide(near_b[0, 0]) + wide(near_b[0, 1]) + wide(src[rows(0, 1, a, b), :])
        plane[...] = total.astype(plane.dtype)
        net.spend(0.3)
        gate(lambda: net.when(net.copy(plane, last, last, "z"), arrived))

    def arrived():
        both[0] -= 1
        if both[0]:
            return
        if a:
            finish(0, wide(near_a[0]) + wide(near_a[1]) + wide(sums[pl.ds(0, a), :]))
        total = wide(near_b[1, 0]) + wide(near_b[1, 1]) + wide(src[rows(0, 0, a, b), :]) + wide(last[...])
        net.spend(0.5)
        finish(a, total)

    far_other, direct_other = ring(block_b(1), b, far_b.at[0], near_b.at[0], acc_b.at[0], plane_done)
    far_own, direct_own = ring(block_b(0), b, far_b.at[1], near_b.at[1], acc_b.at[1], arrived)
    def first():
        fill(lambda i: net.block_of(x + 2, lax.rem(low + 1 + i, 2)))
        far_other()
        far_own()
        to_partner(2)

    def second():
        fill(lambda i: net.block_of(x + 1 - 2 * i, 1 - low))
        direct_other()
        to_partner(1)
        to_partner(3)

    def third():
        fill(lambda i: net.block_of(x + 1 - 2 * i, low))
        direct_own()

    def fourth():
        fill(lambda i: net.block_of(x, lax.rem(low + 1 + i, 2)))
        to_partner(0)

    actions = [first, second, third, fourth]

    def need(number):
        while len(actions) > 4 - number:
            actions.pop(0)()

    for number in range(1, 5):
        step(lambda number=number: need(number))


def scatter_scratch(size, width, dtype, split):
    a, b = split, size - split
    shapes = [(2, 2, b // 2, width), (2, 2, b, width), (2, 2, b // 2, width), (b, width), (b, width)]
    if a:
        shapes += [(4 * a, width), (4 * a, width), (2, a // 2, width), (2, a, width), (2, a // 2, width)]
    return [pltpu.VMEM(shape, dtype) for shape in shapes]


def comm_body(spreads, smalls, gathers, *refs):
    count = spreads + smalls + len(gathers)
    ins, outs, relays = refs[:count], refs[count : 2 * count], refs[2 * count : -2]
    net = Net(*refs[-2:])
    net.greet(["x+", "x-", "z", "y+", "y-", "w", "c"])
    for k in range(spreads):
        spread(net, ins[k], outs[k])
    for k in range(spreads, spreads + smalls):
        spread_small(net, ins[k], outs[k])
    for i, axis in enumerate(gathers):
        k = spreads + smalls + i
        gather(net, ins[k], outs[k], relays[i], axis)
    net.run()


def communicate(name, body, collective_id, arrays, shapes, scratch, copies, outside=(), spare=6 * 2**20):
    used = sum(math.prod(r.shape) * jnp.dtype(r.dtype).itemsize for r in scratch if r.memory_space == pltpu.VMEM)
    spaces = [pl.ANY if i in outside else pltpu.VMEM for i in range(len(arrays))]
    return pl.pallas_call(
        body,
        out_shape=shapes,
        in_specs=[pl.BlockSpec(memory_space=space) for space in spaces],
        out_specs=[pl.BlockSpec(memory_space=pltpu.VMEM)] * len(shapes),
        scratch_shapes=scratch + [pltpu.SemaphoreType.DMA((copies,)), pltpu.SemaphoreType.DMA((copies,))],
        compiler_params=pltpu.CompilerParams(
            collective_id=collective_id, has_side_effects=True, vmem_limit_bytes=min(used + spare, 62 * 2**20)
        ),
        name=name,
    )(*arrays)


def gathered(array, axis):
    depth, width = array.shape
    total = lax.axis_size("row")
    shape = (depth * total, width) if axis == 0 else (depth, width * total)
    return jax.ShapeDtypeStruct(shape, array.dtype)


def relay_of(array):
    return pltpu.VMEM((2, array.shape[0] // 2, array.shape[1]), array.dtype)


def exchange(name, collective_id, spreads=(), smalls=(), gathers=()):
    whole = [jax.ShapeDtypeStruct((8 * a.shape[0], a.shape[1]), a.dtype) for a in (*spreads, *smalls)]
    return communicate(
        name,
        functools.partial(comm_body, len(spreads), len(smalls), [axis for _, axis in gathers]),
        collective_id,
        [*spreads, *smalls, *(array for array, _ in gathers)],
        whole + [gathered(*pair) for pair in gathers],
        [relay_of(array) for array, _ in gathers],
        22 * len(spreads) + 8 * len(smalls) + 22 * len(gathers),
    )


def block_body(heads, qkv, weight, tokens, gain, up, down, position, expert_in, expert_out, pick, result, *rest):
    terms, mixed, normed, image, up_whole, table, far, y_relay, up_relay, down_relay = rest[:10]
    hidden, down_whole, units, out, pair, weights, fetched = rest[10:17]
    held, _, span = weights.shape
    tiles = expert_in.shape[1] // span
    fetches = []

    def fetch():
        t = len(fetches)
        if t == 3 * tiles:
            return
        source = expert_in if t < tiles else expert_out
        tile = source.at[:, pl.ds(t % tiles * span, span)]
        copy = pltpu.make_async_copy(tile, weights.at[t % held], fetched.at[t])
        copy.start()
        fetches.append(copy)

    for _ in range(held):
        fetch()
    net = Net(*rest[-2:])
    net.greet(["x+", "x-", "z", "y+", "y-", "w", "c", "y+c", "y-c"])
    size = tokens.shape[0]
    dim = qkv.shape[1] // (3 * heads)
    low = net.low
    slots = out.shape[3] // 2
    mine = pl.ds(pl.multiple_of(low * slots, slots), slots)
    theirs = pl.ds(pl.multiple_of((1 - low) * slots, slots), slots)

    def fill(column):
        @pl.loop(0, 2)
        def _(i):
            at = pl.ds(pl.multiple_of(column(i) * size, size), size)

            for h in range(heads):
                part = lambda k, h=h: pl.ds((3 * h + k) * dim, dim)
                scores = lax.dot_general(
                    qkv[at, part(0)], qkv[:, part(1)], (((1,), (1,)), ((), ())), preferred_element_type=jnp.float32
                )
                scale = dim ** (-0.5) * math.log2(math.e)
                chances = jnp.exp2((scores - jnp.max(scores, axis=-1, keepdims=True)) * scale)
                total = jnp.sum(chances, axis=-1, keepdims=True)
                value = matmul(chances.astype(jnp.bfloat16), qkv[:, part(2)]) / total
                mixed[:, pl.ds(h * dim, dim)] = value.astype(jnp.bfloat16)

            @pl.loop(0, weight.shape[1] // 512)
            def _(j):
                columns = pl.ds(pl.multiple_of(j * 512, 512), 512)
                terms[at, columns] = matmul(mixed[...], weight[:, columns]).astype(jnp.bfloat16)

        net.spend(2.6)

    def fill_dense(column):
        while early:
            early.pop().wait_send()
        at = [pl.ds(pl.multiple_of(column(i) * size, size), size) for i in range(2)]
        for i in range(2):
            pair[pl.ds(i * size, size), :] = units[at[i], :]

        @pl.loop(0, down_whole.shape[1] // 512)
        def _(j):
            columns = pl.ds(pl.multiple_of(j * 512, 512), 512)
            product = matmul(pair[...], down_whole[:, columns]).astype(jnp.bfloat16)
            for i in range(2):
                terms[at[i], columns] = product[i * size : (i + 1) * size]

    def place(index, plane):
        rows = pl.ds(pl.multiple_of(plane * 4 * size, 4 * size), 4 * size)
        flat = math.prod(table.shape[1:5])
        here = lax.broadcasted_iota(jnp.int32, (flat, 4 * size), 0) == position[pl.ds(0, 1), rows]
        placing = jnp.where(here, 1.0, 0.0).astype(jnp.bfloat16)
        span = 512

        @pl.loop(0, image.shape[1] // span)
        def _(j):
            columns = pl.ds(pl.multiple_of(j * span, span), span)
            put = matmul(placing, image[rows, columns]).astype(jnp.bfloat16)
            table[index, :, :, :, :, columns] = put.reshape(table.shape[1:5] + (span,))

        net.spend(1.2)

    def plane_done():
        place(0, low)

        def from_w(d):
            got = far.at[d, :, theirs]
            arrival = net.copy(got, got, far.at[d, :, mine], "z")
            net.when(arrival, last[d])
            first[d]()

        for d in (2, 1, 3, 0):
            arrival = net.copy(table.at[0, 1, d], far.at[d, :, mine], far.at[d, :, theirs], "w")
            net.when(arrival, functools.partial(from_w, d))
        start_all(own)
        ready()

    def image_done():
        place(1, 1 - low)
        start_all(other)
        ready()

    finish_dense, start_expert, gate = returning(
        net, out, pick, hidden, result, weights, fetches, fetch, *rest[17:30]
    )
    dispatched = counted(28, start_expert)
    came = lambda d: dispatched()
    own = y_exchange(net, chunks(table.at[0, 0]), chunks(out.at[0], mine), y_relay.at[0], came)
    first = y_exchange(net, chunks(far, theirs), chunks(out.at[1], theirs), y_relay.at[1], came)
    last = y_exchange(net, chunks(far, mine), chunks(out.at[1], mine), y_relay.at[2], came)
    other = y_exchange(net, chunks(table.at[1, 0]), chunks(out.at[0], theirs), y_relay.at[3], came)
    early = []

    def dense():
        up_tasks(net, image, up_whole, units)
        reduce_scatter(net, fill_dense, terms, rest[30:40], finish_dense, 32, lambda action: net.work(1.4, action), gate)

    ready = counted(4, dense)

    def finish(start, total):
        at = pl.ds(start, total.shape[0])
        state = (tokens[at, :].astype(jnp.float32) + total).astype(jnp.bfloat16)
        hidden[at, :] = state
        normed[at, :] = layer_norm(state, gain[...]).astype(jnp.bfloat16)
        if start == 0:
            return
        early.extend(net.finish)
        net.finish.clear()
        net.spend(0.5)
        spread(net, normed, image, plane_done, image_done)

    gather(net, up, up_whole, up_relay, 0, ready)
    gather(net, down, down_whole, down_relay, 1, ready)
    reduce_scatter(net, fill, terms, rest[40:-2], finish, SPLIT)
    net.run()


def whole_block(collective_id, heads, qkv, weight, tokens, gain, up, down, position, expert_in, expert_out, pick, slots):
    size, width = tokens.shape
    depth, inside = expert_in.shape
    span = min(512, width)
    full, part = (4, 2, slots, width), (4, 2, slots // 2, width)
    sixteen = lambda *shape: pltpu.VMEM(shape, tokens.dtype)
    scratch = [
        sixteen(8 * size, width),
        sixteen(size, weight.shape[0]),
        sixteen(size, width),
        sixteen(8 * size, width),
        sixteen(*gathered(up, 0).shape),
        sixteen(2, 2, *part),
        sixteen(*full),
        sixteen(4, 2, slots // 2, width),
        relay_of(up),
        relay_of(down),
        sixteen(size, width),
        sixteen(*gathered(down, 1).shape),
        sixteen(8 * size, up.shape[1]),
        sixteen(2, *full),
        sixteen(2 * size, up.shape[1]),
        sixteen(3, depth, span),
        pltpu.SemaphoreType.DMA((3 * (width // span),)),
        sixteen(*full),
        sixteen(*part),
        sixteen(*part),
        sixteen(*full),
        sixteen(*part),
        sixteen(2, *part),
        sixteen(2, 4 * slots, width),
        sixteen(2, 2, slots // 2, width),
        sixteen(2, 2, slots, width),
        sixteen(2, 4 * slots, width),
        pltpu.VMEM((size, width), jnp.float32),
        sixteen(2, *full),
        sixteen(2, 8 * slots, inside),
    ]
    scratch += scatter_scratch(size, width, tokens.dtype, 32) + scatter_scratch(size, width, tokens.dtype, SPLIT)
    return communicate(
        "block",
        functools.partial(block_body, heads),
        collective_id,
        (qkv, weight, tokens, gain, up, down, position, expert_in, expert_out, pick),
        [jax.ShapeDtypeStruct(tokens.shape, tokens.dtype)],
        scratch,
        24 + 22 + 2 * 22 + 8 + 4 * 10 + 24 + 2 * 10 + 12 + 12,
        outside=(7, 8),
        spare=7 * 2**20,
    )


def y_exchange(net, src, dst, relay, arrived=lambda d: None, then=lambda: None):
    core = net.core
    forwarded = counted(2, then)

    def opposite():
        for index, c, forward, last in ((0, core, "y+", "y+"), (1, 1 - core, "y-", "y-c")):

            def onward(index=index, c=c, last=last):
                arrival = net.copy(relay.at[index], dst(2, core), dst(2, c), last)
                net.when(arrival, lambda: arrived(2))
                forwarded()

            net.when(net.copy(src(2, c), relay.at[index], relay.at[index], forward), onward)

    def beside(d):
        forward = "y+" if d == 1 else "y-"
        for c, name in ((core, forward), (1 - core, forward + "c")):
            net.when(net.copy(src(d, c), dst(4 - d, core), dst(4 - d, c), name), lambda: arrived(4 - d))

    def here():
        net.when(net.copy(src(0, 1 - core), dst(0, core), dst(0, 1 - core), "c"), lambda: arrived(0))
        dst(0, core)[...] = src(0, core)[...]

    return {2: opposite, 1: lambda: beside(1), 3: lambda: beside(3), 0: here}


def chunks(ref, *rest):
    return lambda d, c: ref.at[(d, c, *rest)]


def start_all(steps):
    for d in (2, 1, 3, 0):
        steps[d]()


def up_tasks(net, x_ref, w_ref, out):
    rows, width = out.shape
    tile = min(256, rows)
    span = min(256, width)

    def piece(j):
        columns = pl.ds(j * span, span)

        @pl.loop(0, rows // tile)
        def _(i):
            at = pl.ds(pl.multiple_of(i * tile, tile), tile)
            inner = jnp.dot(x_ref[at, :], w_ref[:, columns], preferred_element_type=jnp.float32)
            out[at, columns] = (inner * (1.0 + lax.erf(inner * (0.5**0.5))) * 0.5).astype(out.dtype)

    for j in range(width // span):
        net.work(1.6, lambda j=j: piece(j))


def returning(net, rows, pick, hidden, out, weights, fetches, fetch, *rest):
    far, other, total, near, partial, found, packed, relay, y_relay = rest[:9]
    arrived_rows, dense, parts, inner = rest[9:13]
    held, _, span = weights.shape
    tiles = inner.shape[2] // span
    low = net.low
    half = parts.shape[3] // 2
    mine, theirs = pl.ds(pl.multiple_of(low * half, half), half), pl.ds(pl.multiple_of((1 - low) * half, half), half)
    count = packed.shape[1] // 4

    def pack(index):
        flat = math.prod(found.shape[1:4])
        row = lax.broadcasted_iota(jnp.int32, (count, flat), 0)
        slot = lax.broadcasted_iota(jnp.int32, (count, flat), 1)
        each = half // 4
        same = (row // each == slot // half) & (row % each == slot % each)
        for k in range(4):
            chosen = same & (slot % half // each == lax.rem(net.x + k, 4))
            chosen = jnp.where(chosen, 1.0, 0.0).astype(jnp.bfloat16)

            @pl.loop(0, found.shape[4] // 512)
            def _(j):
                columns = pl.ds(pl.multiple_of(j * 512, 512), 512)
                rows = found[index, :, :, :, columns].reshape(flat, 512)
                value = matmul(chosen, rows).astype(jnp.bfloat16)
                packed[index, k * count : (k + 1) * count, columns] = value

        net.spend(0.6)

    def send(index):
        pack(index)
        at = lambda k, first=0, rows=count: packed.at[index, pl.ds(k * count + first, rows)]
        place = lambda k, first=0, rows=count: arrived_rows.at[index, pl.ds(k * count + first, rows)]
        middle = count // 2
        for i, forward in ((0, "x+"), (1, "x-")):

            def onward(i=i, forward=forward):
                dst = place(2, i * middle, middle)
                net.when(net.copy(relay.at[index, i], dst, dst, forward), landed)

            net.when(net.copy(at(2, i * middle, middle), relay.at[index, i], relay.at[index, i], forward), onward)
        for k, forward in ((1, "x+"), (3, "x-")):
            net.when(net.copy(at(k), place(k), place(k), forward), landed)

    flat_rows = math.prod(parts.shape[1:4])

    def expert_up(j):
        fetches[j].wait()

        @pl.loop(0, 2)
        def _(i):
            value = matmul(rows[i].reshape(flat_rows, rows.shape[4]), weights[j % held])
            value = value * (1.0 + lax.erf(value * (0.5**0.5))) * 0.5
            inner[i, :, pl.ds(j * span, span)] = value.astype(inner.dtype)

        fetch()

    def expert_down(i, j):
        t = (2 - i) * tiles + j
        fetches[t].wait()
        value = matmul(inner[i], weights[t % held]).astype(parts.dtype)
        parts[i, :, :, :, pl.ds(j * span, span)] = value.reshape(parts.shape[1:4] + (span,))
        fetch()

    def finish_dense(start, total):
        dense[pl.ds(start, total.shape[0]), :] = total
        if start:
            ready()

    def combine():
        flat = 4 * count
        for index in range(2):
            arrived_rows[index, pl.ds(0, count), :] = packed[index, pl.ds(0, count), :]

        @pl.loop(0, out.shape[1] // 512)
        def _(j):
            columns = pl.ds(pl.multiple_of(j * 512, 512), 512)
            value = hidden[:, columns].astype(jnp.float32) + dense[:, columns]
            for index in range(2):
                value += matmul(pick[:, pl.ds(index * flat, flat)], arrived_rows[index, :, columns])
            out[:, columns] = value.astype(jnp.bfloat16)

    ready = counted(9, combine)
    landed = ready

    def far_landed(d):
        def add():
            total[d] = far[d, :, theirs] + other[d]
            net.spend(0.2)
            arrival = net.copy(total.at[d], found.at[1, d], found.at[1, d], "w")
            net.when(arrival, complete[1])

        net.when(net.copy(far.at[d, :, mine], other.at[d], other.at[d], "z"), add)

    pending = []
    held_back = counted(5, lambda: pending.pop()())

    def gate(action):
        pending.append(action)
        held_back()

    def near_landed(d):
        def add():
            found[0, d] = near[d, :, mine] + partial[d]
            net.spend(0.2)
            complete[0]()

        net.when(net.copy(near.at[d, :, theirs], partial.at[d], partial.at[d], "z"), add)
        held_back()

    complete = [counted(4, functools.partial(send, index)) for index in range(2)]
    far_counts = {d: counted(1 if d == 0 else 2, functools.partial(far_landed, d)) for d in range(4)}
    near_counts = {d: counted(1 if d == 0 else 2, functools.partial(near_landed, d)) for d in range(4)}
    second = y_exchange(net, chunks(parts.at[0]), chunks(near), y_relay.at[0], lambda d: near_counts[d]())
    go = counted(2, lambda: start_all(second))
    first = y_exchange(net, chunks(parts.at[1]), chunks(far), y_relay.at[1], lambda d: far_counts[d](), go)

    def start():
        for j in range(tiles):
            expert_up(j)
            net.spend(1.3)
        for i, after in ((1, lambda: start_all(first)), (0, go)):
            for j in range(tiles):
                expert_down(i, j)
                net.spend(0.7)
            after()

    return finish_dense, start, gate


def layer_norm(row_data, gain_vector):
    row_data = row_data.astype(jnp.float32)
    centered = row_data - jnp.mean(row_data, axis=-1, keepdims=True)
    spread = jnp.mean(centered * centered, axis=-1, keepdims=True)
    return centered * lax.rsqrt(spread + 1e-06) * gain_vector


def matmul(a, b):
    return jnp.dot(a, b, preferred_element_type=jnp.float32)


def shards(
    tokens,
    ln1_gain,
    qkv_weight,
    out_weight,
    ln2_gain,
    ffn_in,
    ffn_out,
    expert_ids,
    expert_in,
    expert_out,
):
    tok_count, model_width = tokens.shape
    row_total = lax.axis_size("row")
    col_total = lax.axis_size("col")
    row_index = lax.axis_index("row")
    col_index = lax.axis_index("col")
    expert_count = row_total * col_total // 2
    capacity = max(2, 2 * tok_count // expert_count)
    head_count, head_dim = qkv_weight.shape[1], qkv_weight.shape[3]
    seq_len = tok_count * col_total

    ids = expert_ids[:, 0]
    token = jnp.arange(tok_count, dtype=jnp.int32)
    same = (expert_ids == ids[None, :]) & (token[:, None] < token[None, :])
    codes = ids * capacity + jnp.sum(same.astype(jnp.int32), axis=0)
    image_rows, codes_all, qkv_whole, out_whole = exchange(
        "enter",
        0,
        spreads=(tokens,),
        smalls=(jnp.broadcast_to(codes[None, :], (8, tok_count)),),
        gathers=((qkv_weight.reshape(qkv_weight.shape[0], -1), 0), (out_weight, 1)),
    )
    normed = layer_norm(image_rows, ln1_gain).astype(jnp.bfloat16)
    projected = matmul(normed, qkv_whole).astype(jnp.bfloat16)
    codes_all = codes_all.reshape(col_total, 8, tok_count)[:, 0]
    ids_rows, slot_index = codes_all // capacity, codes_all % capacity
    block = jnp.arange(col_total, dtype=jnp.int32)[:, None]
    plane, place = block // 4, block % 4 * capacity + slot_index
    home_row = 2 * ids_rows // col_total
    mine = (2 * ids_rows % col_total) // 2 == col_index // 2
    other = (home_row // 8 != row_index // 8).astype(jnp.int32)
    chunk = (home_row // 2 - row_index // 2 + 8) % 4 * 2 + home_row % 2
    half = 4 * capacity
    rows = 2 * half
    slot_count = row_total * rows
    position = jnp.where(mine, (other * 8 + chunk) * half + place, -1).reshape(1, seq_len)
    position = jnp.broadcast_to(position, (8, seq_len))
    home = ids // 4
    turn = (home // 2 - row_index // 2 + 8) % 4 * 2 + home % 2
    found = (col_index // 2 - ids % 4 + 4) % 4 * rows + turn * capacity + codes % capacity
    found = jnp.where(home // 8 != row_index // 8, found + 4 * rows, found)
    pick = (found[:, None] == jnp.arange(8 * rows, dtype=jnp.int32)[None, :]).astype(jnp.bfloat16)

    (out,) = whole_block(
        1, head_count, projected, out_whole, tokens, ln2_gain[None, :], ffn_in, ffn_out, position,
        expert_in[0], expert_out[0], pick, rows,
    )
    return out


def solution(mesh):
    in_specs = (
        P(("row", "col"), None),
        P(),
        P("row", "col", None, None),
        P("col", "row"),
        P(),
        P("row", "col"),
        P("col", "row"),
        P(("row", "col"), None),
        P(("row", "col"), None, None),
        P(("row", "col"), None, None),
    )
    out_specs = P(("row", "col"), None)
    return jax.shard_map(shards, mesh=mesh, in_specs=in_specs, out_specs=out_specs, check_vma=False)
```
